128 devices in a mesh: row: 8 (over z, core), col: 16 (over y, x).
Axes of the slice: x: 4, y: 4, z: 4, core: 2. Of those that a mesh axis runs over, the one named last changes fastest.
Arguments:
- a_matrix: float32 [8192, 8192], P('row', 'col'), may hold values from -14 to 30, as said below
- b_matrix: float32 [4096, 4096], P('row', 'col'), may hold values from -14 to 30, as said below
- c_matrix: float32 [8192, 4096], P('row', 'col'), may hold values from -6 to 6
Outputs:
- a_swept: float32 [8192, 8192], P('row', 'col')
- c_swept: float32 [8192, 4096], P('row', 'col')
- b_next: float32 [4096, 4096], P('row', 'col')
The draws below stay inside these ranges and needn't reach their ends.
Inputs may be any that keep to these rules, and one draw needn't show every extreme that they name: `a_matrix`: symmetric positive definite; its smallest eigenvalue is at least 1. `b_matrix`: symmetric positive definite; its smallest eigenvalue is at least 1.
All inputs are finite; a program needn't handle non-finite values. Where the reference program divides by a largest or mean magnitude, that divisor is 1e-20 or more.
Results may differ from the reference program's by a relative error of at most 0.00012.
Values sent between devices are 32-bit elements; how exact they have to be, the bound alone decides.
A program may use at most 128 MiB of HBM per device.

```python
import math
import jax
import jax.numpy as jnp
from jax import lax

NA = 8192
NB = 4096
PANEL = 256
PIVOT_ITERS = 6
STEPS_A = 2
STEPS_B = 16


def definite(key, order):
    first_key, second_key, third_key = jax.random.split(key, 3)
    inner = order // 4
    limit = math.sqrt(3.0)
    factor = jax.random.uniform(first_key, (order, inner), jnp.float32, -limit, limit)
    spread = math.log(2.0)
    coupling = jnp.dot(factor, factor.T, precision=lax.Precision.HIGHEST, preferred_element_type=jnp.float32) / inner
    block_scale = jnp.exp(jax.random.uniform(second_key, (16,), jnp.float32, 0.0, 0.5 * spread))
    block_scale = jnp.repeat(block_scale, order // 16)
    row_scale = block_scale * jnp.exp(jax.random.uniform(third_key, (order,), jnp.float32, 0.0, 0.5 * spread))
    identity = jnp.eye(order, dtype=jnp.float32)
    core = identity + 0.25 * coupling
    return row_scale[:, None] * core * row_scale[None, :]


def draw_a_matrix(key, part):
    return definite(jax.random.fold_in(key, 11), NA)


def draw_b_matrix(key, part):
    return definite(jax.random.fold_in(key, 23), NB)


def steps_of(key, extent, cuts, low, high):
    loudness = 1.0
    for axis_at, shards_of in cuts:
        steps = jax.random.uniform(jax.random.fold_in(jax.random.fold_in(key, 6), axis_at), (shards_of,), jnp.float32, low / len(cuts), high / len(cuts))
        loudness = loudness * jnp.repeat(jnp.exp(steps), extent[axis_at] // shards_of).reshape((-1,) + (1,) * (len(extent) - 1 - axis_at))
    return loudness


def scatter_about(rng, extent, deviation, bound, pieces=(), held_as=jnp.bfloat16):
    gain = steps_of(rng, extent, pieces, -0.22, 0.18) if pieces else 1.0
    values = jax.random.normal(rng, extent, jnp.float32) * deviation * gain
    return jnp.minimum(jnp.maximum(values, -bound), bound).astype(held_as)


def setup_inputs(seed: int = 0) -> dict:
    keys = jax.random.split(jax.random.key(seed), 4)
    a_matrix = draw_a_matrix(jax.random.fold_in(keys[3], 71), 0)
    b_matrix = draw_b_matrix(jax.random.fold_in(keys[3], 71), 0)
    c_matrix = scatter_about(keys[2], (NA, NB), 1.0, 6.0, ((0, 8), (1, 16)), jnp.float32)
    return dict(a_matrix=a_matrix, b_matrix=b_matrix, c_matrix=c_matrix)


EXACT = lax.Precision.HIGHEST

def pivot_inverse(pivot):
    order = pivot.shape[0]
    scaling = 1.0 / jnp.sqrt(jnp.diagonal(pivot))
    unit = pivot * scaling[:, None] * scaling[None, :]
    ceiling = jnp.max(lax.optimization_barrier(jnp.sum(jnp.abs(unit), axis=1)))
    approx = jnp.eye(order, dtype=jnp.float32) / ceiling
    for turn in range(PIVOT_ITERS):
        product = jnp.dot(unit, approx, precision=EXACT, preferred_element_type=jnp.float32)
        approx = 2.0 * approx - jnp.dot(approx, product, precision=EXACT, preferred_element_type=jnp.float32)
    return approx * scaling[:, None] * scaling[None, :]

def sweep(matrix, other, count):
    order = matrix.shape[0]
    index = jnp.arange(order, dtype=jnp.int32)
    for step in range(count):
        first = step * PANEL
        eye_rows = (index[:, None] == first + jnp.arange(PANEL, dtype=jnp.int32)[None, :]).astype(jnp.float32)
        inverse = pivot_inverse(matrix[first:first + PANEL, first:first + PANEL])
        solved = jnp.dot(matrix[:, first:first + PANEL] - eye_rows, inverse, precision=EXACT, preferred_element_type=jnp.float32)
        rows = matrix[first:first + PANEL, :]
        updated = matrix - jnp.dot(solved, rows, precision=EXACT, preferred_element_type=jnp.float32)
        matrix = updated.at[:, first:first + PANEL].set(eye_rows - solved)
        if other is not None:
            other = other - jnp.dot(solved, other[first:first + PANEL, :], precision=EXACT, preferred_element_type=jnp.float32)
    return (matrix, other)

def reference(a_matrix, b_matrix, c_matrix):
    a_swept, c_swept = sweep(a_matrix, c_matrix, STEPS_A)
    b_inverse, unused = sweep(b_matrix, None, STEPS_B)
    b_squares = jnp.sum(b_matrix * b_matrix)
    inv_squares = jnp.sum(b_inverse * b_inverse)
    scale = jnp.sqrt(jnp.sqrt(inv_squares / b_squares))
    b_next = 0.5 * (scale * b_matrix + b_inverse / scale)
    return (a_swept, c_swept, b_next)
```

```python
import functools

import jax
import jax.numpy as jnp
from jax import lax
from jax.experimental import pallas as pl
from jax.experimental.pallas import tpu as pltpu
from jax.sharding import Mesh
from jax.sharding import PartitionSpec as P

PANEL = 256
SQUARINGS = 5
STEPS_A = 2
STEPS_B = 16
JOINED = 4
AXES = ("z", "core", "y", "x")
ROW = ("z", "core")
COL = ("y", "x")
F32 = jnp.float32
BF16 = jnp.bfloat16


def halves(value):
    high = value.astype(BF16)
    return high, (value - high.astype(F32)).astype(BF16)


def product(left, right):
    return jnp.dot(left, right, preferred_element_type=F32)


def triple(left, right_high, right_low):
    high, low = halves(left)
    return product(high, right_high) + product(high, right_low) + product(low, right_high)


def pivot_inverse(pivot):
    shape = (PANEL, PANEL)
    unit = lax.broadcasted_iota(jnp.int32, shape, 0) == lax.broadcasted_iota(jnp.int32, shape, 1)
    diagonal = jnp.where(unit, pivot, 0.0)
    down = 1.0 / jnp.sqrt(jnp.sum(diagonal, axis=1, keepdims=True))
    across = 1.0 / jnp.sqrt(jnp.sum(diagonal, axis=0, keepdims=True))
    scaled = pivot * down * across
    ceiling = jnp.max(jnp.sum(jnp.abs(scaled), axis=1, keepdims=True), axis=0, keepdims=True)
    eye = jnp.where(unit, 1.0, 0.0)
    power = eye - scaled / ceiling
    total = eye + power
    high, low = halves(power)
    power = product(high, high) + product(high, low) + product(low, high)
    for turn in range(SQUARINGS - 1):
        high, low = halves(jnp.concatenate([power, total], 0))
        both = product(high, high[:PANEL]) + product(high, low[:PANEL]) + product(low, high[:PANEL])
        power = both[:PANEL]
        total = total + both[PANEL:]
    high, low = halves(power)
    total = total + triple(total, high, low)
    return total / ceiling * down * across


def composite(count, table, fresh, fresh_high, fresh_low):
    @pl.loop(0, count)
    def _(p):
        here = pl.ds(pl.multiple_of(p * PANEL, PANEL), PANEL)
        inverse = pivot_inverse(table[here, here])
        high, low = halves(table[here, :])
        fresh[...] = triple(inverse, high, low)
        fresh[:, here] = inverse
        high, low = halves(fresh[...])
        fresh_high[...] = high
        fresh_low[...] = low

        @pl.loop(0, count)
        def _(q):
            @pl.when(q != p)
            def _():
                there = pl.ds(pl.multiple_of(q * PANEL, PANEL), PANEL)
                column = table[there, here]
                table[there, here] = jnp.zeros((PANEL, PANEL), F32)
                table[there, :] = table[there, :] - triple(column, fresh_high[...], fresh_low[...])

        table[here, :] = fresh[...]


def right_side(table, rows, base, right_high, right_low, solved_high, solved_low):
    order, cols = rows.shape
    if base is None:
        value = rows[...]
    else:
        unit = lax.broadcasted_iota(jnp.int32, (order, cols), 0) == base + lax.broadcasted_iota(jnp.int32, (order, cols), 1)
        inside = jnp.logical_and(base >= 0, base < order)
        value = jnp.where(inside, jnp.where(unit, 1.0, 0.0), rows[...])
    high, low = halves(value)
    right_high[:, :cols] = high
    right_low[:, :cols] = low

    @pl.loop(0, order // PANEL)
    def _(q):
        there = pl.ds(pl.multiple_of(q * PANEL, PANEL), PANEL)
        high, low = halves(triple(table[there, :], right_high[:, :cols], right_low[:, :cols]))
        solved_high[there, :cols] = high
        solved_low[there, :cols] = low


def left_side(matrix, result, piece, row_base, col_base, order, solved_high, solved_low):
    rows, cols = matrix.shape

    @pl.loop(0, rows // PANEL)
    def _(r):
        start = pl.multiple_of(r * PANEL, PANEL)
        there = pl.ds(start, PANEL)
        down = row_base + start + lax.broadcasted_iota(jnp.int32, (PANEL, PANEL), 0)
        total = None
        for q in range(order // PANEL):
            unit = down == q * PANEL + lax.broadcasted_iota(jnp.int32, (PANEL, PANEL), 1)
            column = piece(start, q) - jnp.where(unit, 1.0, 0.0)
            among = pl.ds(q * PANEL, PANEL)
            part = triple(column, solved_high[among, :cols], solved_low[among, :cols])
            total = part if total is None else total + part
        base = matrix[there, :]
        if col_base is not None:
            inside = jnp.logical_and(col_base >= 0, col_base < order)
            across = col_base + lax.broadcasted_iota(jnp.int32, (PANEL, cols), 1)
            begin = row_base + start + lax.broadcasted_iota(jnp.int32, (PANEL, cols), 0)
            base = jnp.where(inside, jnp.where(begin == across, 1.0, 0.0), base)
        result[there, :] = base - total


def center_kernel(step, mine, other, matrix, mate, half, table, fresh, fresh_high, fresh_low, right_high, right_low, solved_high, solved_low):
    core = lax.axis_index("core")
    rows = matrix.shape[0]
    order = JOINED * PANEL
    base = (lax.axis_index("y") - step) * order + lax.axis_index("x") * matrix.shape[1]

    @pl.when(lax.axis_index("z") == step)
    def _():
        ours = pl.ds(pl.multiple_of(core * rows, rows), rows)
        theirs = pl.ds(pl.multiple_of((1 - core) * rows, rows), rows)
        for q in range(JOINED):
            table[ours, q * PANEL : (q + 1) * PANEL] = mine[q]
            table[theirs, q * PANEL : (q + 1) * PANEL] = other[q]
        composite(JOINED, table, fresh, fresh_high, fresh_low)
        inside = jnp.logical_and(base >= 0, base < order)
        for there, source in ((ours, matrix), (theirs, mate)):
            shape = source.shape
            down = there.start + lax.broadcasted_iota(jnp.int32, shape, 0)
            unit = down == base + lax.broadcasted_iota(jnp.int32, shape, 1)
            high, low = halves(jnp.where(inside, jnp.where(unit, 1.0, 0.0), source[...]))
            right_high[there, :] = high
            right_low[there, :] = low
        for q in range(rows // PANEL):
            there = pl.ds(pl.multiple_of(core * rows + q * PANEL, PANEL), PANEL)
            half[q * PANEL : (q + 1) * PANEL, :] = triple(table[there, :], right_high[...], right_low[...])


def update_kernel(step, matrix, column, solved, result, solved_high, solved_low):
    order = JOINED * PANEL
    rows = matrix.shape[0]
    row_base = (lax.axis_index("z") - step) * order + lax.axis_index("core") * rows
    col_base = (lax.axis_index("y") - step) * order + lax.axis_index("x") * matrix.shape[1]
    for core in range(2):
        high, low = halves(solved[core])
        solved_high[core * rows : (core + 1) * rows, :] = high
        solved_low[core * rows : (core + 1) * rows, :] = low
    piece = lambda start, q: column[q, pl.ds(start, PANEL), :]
    left_side(matrix, result, piece, row_base, col_base, order, solved_high, solved_low)


def ring(index, by):
    return lax.rem(index + by, 4)


def send(source, target, sent, received, where):
    return pltpu.make_async_remote_copy(
        src_ref=source, dst_ref=target, send_sem=sent, recv_sem=received,
        device_id=where, device_id_type=pl.DeviceIdType.MESH,
    )


def greet(neighbours):
    barrier = pltpu.get_barrier_semaphore()
    for where in neighbours:
        pl.semaphore_signal(barrier, inc=1, device_id=where, device_id_type=pl.DeviceIdType.MESH)
    pl.semaphore_wait(barrier, len(neighbours))


def part(h):
    return pl.ds(h * PANEL, PANEL)


def spread(axis, step, source, landing, sent, received, follow):
    place = lax.axis_index(axis)
    apart = lax.rem(place - step + 4, 4)
    up, down = {axis: ring(place, 1)}, {axis: ring(place, 3)}
    outward = [send(source.at[part(h)], landing.at[part(h)], sent.at[0, h], received.at[h], up) for h in (0, 1)]
    inward = [send(source.at[part(h)], landing.at[part(h)], sent.at[1, h], received.at[h], down) for h in (0, 1)]
    onward = send(landing.at[part(0)], landing.at[part(0)], sent.at[0, 0], received.at[0], up)
    backward = send(landing.at[part(1)], landing.at[part(1)], sent.at[1, 1], received.at[1], down)

    @pl.when(apart == 0)
    def _():
        for copy in (outward[0], inward[1], outward[1], inward[0]):
            copy.start()
        follow(0, source)
        follow(1, source)

    def arrive(h):
        send(landing.at[part(h)], landing.at[part(h)], sent.at[0, h], received.at[h], up).wait_recv()

    @pl.when(apart == 1)
    def _():
        arrive(0)
        onward.start()
        follow(0, landing)
        arrive(1)
        follow(1, landing)

    @pl.when(apart == 3)
    def _():
        arrive(1)
        backward.start()
        follow(1, landing)
        arrive(0)
        follow(0, landing)

    @pl.when(apart == 2)
    def _():
        arrive(0)
        follow(0, landing)
        arrive(1)
        follow(1, landing)

    def finish():
        @pl.when(apart == 0)
        def _():
            for copy in outward + inward:
                copy.wait_send()

        @pl.when(apart == 1)
        def _():
            onward.wait_send()

        @pl.when(apart == 3)
        def _():
            backward.wait_send()

    return apart, finish


def gather_kernel(step, matrix, column, other, mate, y_sent, y_got, x_sent, x_got, far_sent, far_got, core_sent, core_got):
    x, y = lax.axis_index("x"), lax.axis_index("y")
    right, left, far = ring(x, 1), ring(x, 3), ring(x, 2)
    partner = {"core": 1 - lax.axis_index("core")}
    center = lax.axis_index("z") == step
    greet([{"y": ring(y, 1)}, {"y": ring(y, 3)}, {"x": right}, {"x": left}, partner])
    swap = send(matrix, mate, core_sent.at[4], core_got.at[4], partner)

    @pl.when(center)
    def _():
        swap.start()

    def sideways(h, ref):
        return [
            send(ref.at[part(h)], column.at[x, part(h)], x_sent.at[0, h], x_got.at[0, h], {"x": right}),
            send(ref.at[part(h)], column.at[x, part(h)], x_sent.at[1, h], x_got.at[1, h], {"x": left}),
        ]

    def follow(h, ref):
        for copy in sideways(h, ref):
            copy.start()

    apart, finish = spread("y", step, matrix, column.at[x], y_sent, y_got, follow)

    def give(role, place, ref):
        return send(ref, other.at[place], core_sent.at[role], core_got.at[role], partner)

    @pl.when(jnp.logical_and(center, apart == 0))
    def _():
        give(0, x, matrix).start()

    @pl.when(jnp.logical_and(center, apart != 0))
    def _():
        give(0, x, column.at[x]).start()

    @pl.when(apart == 0)
    def _():
        column[x] = matrix[...]

    def arrive(place, h, received):
        ref = column.at[place, part(h)]
        send(ref, ref, x_sent.at[0, h], received, {"x": right}).wait_recv()

    arrive(left, 0, x_got.at[0, 0])
    onward = send(column.at[left, part(0)], column.at[left, part(0)], far_sent.at[0], far_got.at[0], {"x": right})
    onward.start()
    arrive(right, 1, x_got.at[1, 1])
    backward = send(column.at[right, part(1)], column.at[right, part(1)], far_sent.at[1], far_got.at[1], {"x": left})
    backward.start()
    arrive(left, 1, x_got.at[0, 1])
    arrive(right, 0, x_got.at[1, 0])

    @pl.when(center)
    def _():
        give(1, left, column.at[left]).start()
        give(2, right, column.at[right]).start()

    arrive(far, 0, far_got.at[0])
    arrive(far, 1, far_got.at[1])

    @pl.when(center)
    def _():
        give(3, far, column.at[far]).start()

    finish()
    for h in (0, 1):
        for copy in sideways(h, matrix):
            copy.wait_send()
    onward.wait_send()
    backward.wait_send()

    @pl.when(center)
    def _():
        swap.wait()
        for role, place in enumerate((x, left, right, far)):
            give(role, place, column.at[place]).wait()


def share_kernel(step, half, solved, z_sent, z_got, core_sent, core_got):
    z, core = lax.axis_index("z"), lax.axis_index("core")
    partner = {"core": 1 - core}
    greet([{"z": ring(z, 1)}, {"z": ring(z, 3)}, partner])

    def give(h, ref):
        return send(ref.at[part(h)], solved.at[core, part(h)], core_sent.at[h], core_got.at[h], partner)

    def follow(h, ref):
        give(h, ref).start()

    apart, finish = spread("z", step, half, solved.at[core], z_sent, z_got, follow)

    @pl.when(apart == 0)
    def _():
        solved[core] = half[...]

    finish()
    for h in (0, 1):
        give(h, half).wait_send()
        ref = solved.at[1 - core, part(h)]
        send(ref, ref, core_sent.at[h], core_got.at[h], partner).wait_recv()


def sum_kernel(value, total, first, second, between, first_sent, first_got, second_sent, second_got):
    z, core, y, x = (lax.axis_index(axis) for axis in AXES)
    line, plane = z * 2 + core, y * 4 + x

    def of_line(by):
        place = lax.rem(line + by, 8)
        return {"z": place // 2, "core": lax.rem(place, 2)}

    def of_plane(by):
        place = lax.rem(plane + by, 16)
        return {"y": place // 4, "x": lax.rem(place, 4)}

    greet([of_line(by) for by in range(1, 8)] + [of_plane(by) for by in range(1, 16)])
    copies = [send(value, first.at[by - 1], first_sent.at[by - 1], first_got.at[by - 1], of_line(by)) for by in range(1, 8)]
    for copy in copies:
        copy.start()
    for copy in copies:
        copy.wait()
    result = value[...]
    for by in range(7):
        result = result + first[by]
    between[...] = result
    copies = [send(between, second.at[by - 1], second_sent.at[by - 1], second_got.at[by - 1], of_plane(by)) for by in range(1, 16)]
    for copy in copies:
        copy.start()
    for copy in copies:
        copy.wait()
    for by in range(15):
        result = result + second[by]
    total[...] = result


def a_kernel(matrix, other, column, row, other_row, pivot, result, other_result, table, fresh, fresh_high, fresh_low, right_high, right_low, solved_high, solved_low):
    order = STEPS_A * PANEL
    row_base = (lax.axis_index("z") * 2 + lax.axis_index("core")) * matrix.shape[0]
    col_base = (lax.axis_index("y") * 4 + lax.axis_index("x")) * matrix.shape[1]
    table[...] = pivot[...]
    composite(STEPS_A, table, fresh, fresh_high, fresh_low)

    def piece(start, q):
        among = pl.ds(pl.multiple_of(start % order, PANEL), PANEL)
        return column[start // order, pl.ds(q * PANEL, PANEL), among].T

    right_side(table, row, col_base, right_high, right_low, solved_high, solved_low)
    left_side(matrix, result, piece, row_base, col_base, order, solved_high, solved_low)
    right_side(table, other_row, None, right_high, right_low, solved_high, solved_low)
    left_side(other, other_result, piece, row_base, None, order, solved_high, solved_low)


def scratch(order, cols):
    return [
        pltpu.VMEM((order, order), F32),
        pltpu.VMEM((PANEL, order), F32),
        pltpu.VMEM((PANEL, order), BF16),
        pltpu.VMEM((PANEL, order), BF16),
        pltpu.VMEM((order, cols), BF16),
        pltpu.VMEM((order, cols), BF16),
        pltpu.VMEM((order, cols), BF16),
        pltpu.VMEM((order, cols), BF16),
    ]


def call(kernel, outs, scratch_shapes, operands, flops, identity=None):
    space = pl.BlockSpec(memory_space=pltpu.VMEM)
    more = {} if identity is None else dict(collective_id=identity, has_side_effects=True)
    return pl.pallas_call(
        kernel,
        out_shape=[jax.ShapeDtypeStruct(shape, F32) for shape in outs],
        in_specs=[space] * len(operands),
        out_specs=[space] * len(outs),
        scratch_shapes=scratch_shapes,
        compiler_params=pltpu.CompilerParams(vmem_limit_bytes=48 * 1024 * 1024, **more),
        cost_estimate=pl.CostEstimate(flops=flops, bytes_accessed=0, transcendentals=0),
    )(*operands)


def flags(*shape):
    return pltpu.SemaphoreType.DMA(shape)


def b_step(matrix, step):
    rows, cols = matrix.shape
    order = JOINED * PANEL
    column, other, mate = call(
        functools.partial(gather_kernel, step),
        [(4, rows, cols), (4, rows, cols), (rows, cols)],
        [flags(2, 2), flags(2), flags(2, 2), flags(2, 2), flags(2), flags(2), flags(5), flags(5)],
        [matrix], 10**10, 2 * step,
    )
    (half,) = call(
        functools.partial(center_kernel, step), [(rows, cols)], scratch(order, cols),
        [column, other, matrix, mate], 10**10,
    )
    (solved,) = call(
        functools.partial(share_kernel, step), [(2, rows, cols)],
        [flags(2, 2), flags(2), flags(2), flags(2)], [half], 10**10, 2 * step + 1,
    )
    (result,) = call(
        functools.partial(update_kernel, step), [(rows, cols)],
        [pltpu.VMEM((order, cols), BF16), pltpu.VMEM((order, cols), BF16)],
        [matrix, column, solved], 10**9,
    )
    return result


def a_steps(matrix, other):
    order = STEPS_A * PANEL
    cols = matrix.shape[1]
    row = jnp.concatenate([matrix[:order], other[:order]], 1)
    row = lax.all_gather(lax.all_gather(row, "z")[0], "core")[0]
    over = lax.all_gather(row[:, :cols], "y")
    mine = lax.dynamic_index_in_dim(over, lax.axis_index("z"), 0, keepdims=False)
    around = lax.all_gather(jnp.stack([mine, over[0]]), "x")
    column = lax.dynamic_slice_in_dim(around[:, 0], 2 * lax.axis_index("core"), 2, 0)
    return call(
        a_kernel, [matrix.shape, other.shape], scratch(order, cols),
        [matrix, other, column, row[:, :cols], row[:, cols:], around[0, 1]], 10**10,
    )


def squares(value):
    return jnp.sum(value * value)


def total_of(values):
    tile = (8, 128)
    corner = jnp.zeros(tile, F32).at[0, : len(values)].set(jnp.stack(values))
    (total,) = call(
        sum_kernel, [tile],
        [pltpu.VMEM((7, *tile), F32), pltpu.VMEM((15, *tile), F32), pltpu.VMEM(tile, F32), flags(7), flags(7), flags(15), flags(15)],
        [corner], 10**9, 2 * (STEPS_B // JOINED),
    )
    return [total[0, place] for place in range(len(values))]


def body(a_matrix, b_matrix, c_matrix):
    a_swept, c_swept = a_steps(a_matrix, c_matrix)
    b_inverse = b_matrix
    for step in range(STEPS_B // JOINED):
        b_inverse = b_step(b_inverse, step)
    b_squares, inv_squares = total_of([squares(b_matrix), squares(b_inverse)])
    scale = jnp.sqrt(jnp.sqrt(inv_squares / b_squares))
    b_next = 0.5 * (scale * b_matrix + b_inverse / scale)
    return (a_swept, c_swept, b_next)


def solution(mesh):
    finer = Mesh(mesh.devices.reshape(4, 2, 4, 4), AXES)
    placed = (P(ROW, COL), P(ROW, COL), P(ROW, COL))
    return jax.shard_map(body, mesh=finer, in_specs=placed, out_specs=placed, check_vma=False)
```

```python
import functools

import jax
import jax.numpy as jnp
from jax import lax
from jax.experimental import pallas as pl
from jax.experimental.pallas import tpu as pltpu
from jax.sharding import Mesh
from jax.sharding import PartitionSpec as P

PANEL = 256
SQUARINGS = 5
STEPS_A = 2
STEPS_B = 16
JOINED = 4
AXES = ("z", "core", "y", "x")
ROW = ("z", "core")
COL = ("y", "x")
F32 = jnp.float32
BF16 = jnp.bfloat16


def halves(value):
    high = value.astype(BF16)
    return high, (value - high.astype(F32)).astype(BF16)


def product(left, right):
    return jnp.dot(left, right, preferred_element_type=F32)


def triple(left, right_high, right_low):
    high, low = halves(left)
    return product(high, right_high) + product(high, right_low) + product(low, right_high)


def pivot_inverse(pivot):
    shape = (PANEL, PANEL)
    unit = lax.broadcasted_iota(jnp.int32, shape, 0) == lax.broadcasted_iota(jnp.int32, shape, 1)
    diagonal = jnp.where(unit, pivot, 0.0)
    down = 1.0 / jnp.sqrt(jnp.sum(diagonal, axis=1, keepdims=True))
    across = 1.0 / jnp.sqrt(jnp.sum(diagonal, axis=0, keepdims=True))
    scaled = pivot * down * across
    ceiling = jnp.max(jnp.sum(jnp.abs(scaled), axis=1, keepdims=True), axis=0, keepdims=True)
    eye = jnp.where(unit, 1.0, 0.0)
    power = eye - scaled / ceiling
    total = eye + power
    high, low = halves(power)
    power = product(high, high) + product(high, low) + product(low, high)
    for turn in range(SQUARINGS - 1):
        high, low = halves(jnp.concatenate([power, total], 0))
        both = product(high, high[:PANEL]) + product(high, low[:PANEL]) + product(low, high[:PANEL])
        power = both[:PANEL]
        total = total + both[PANEL:]
    high, low = halves(power)
    total = total + triple(total, high, low)
    return total / ceiling * down * across


def composite(count, table, fresh, fresh_high, fresh_low):
    @pl.loop(0, count)
    def _(p):
        here = pl.ds(pl.multiple_of(p * PANEL, PANEL), PANEL)
        inverse = pivot_inverse(table[here, here])
        high, low = halves(table[here, :])
        fresh[...] = triple(inverse, high, low)
        fresh[:, here] = inverse
        high, low = halves(fresh[...])
        fresh_high[...] = high
        fresh_low[...] = low

        @pl.loop(0, count)
        def _(q):
            @pl.when(q != p)
            def _():
                there = pl.ds(pl.multiple_of(q * PANEL, PANEL), PANEL)
                column = table[there, here]
                table[there, here] = jnp.zeros((PANEL, PANEL), F32)
                table[there, :] = table[there, :] - triple(column, fresh_high[...], fresh_low[...])

        table[here, :] = fresh[...]


def left_side(matrix, result, piece, row_base, col_base, order, solved_high, solved_low):
    rows, cols = matrix.shape

    @pl.loop(0, rows // PANEL)
    def _(r):
        start = pl.multiple_of(r * PANEL, PANEL)
        there = pl.ds(start, PANEL)
        down = row_base + start + lax.broadcasted_iota(jnp.int32, (PANEL, PANEL), 0)
        total = None
        for q in range(order // PANEL):
            unit = down == q * PANEL + lax.broadcasted_iota(jnp.int32, (PANEL, PANEL), 1)
            column = piece(start, q) - jnp.where(unit, 1.0, 0.0)
            among = pl.ds(q * PANEL, PANEL)
            part = triple(column, solved_high[among, :cols], solved_low[among, :cols])
            total = part if total is None else total + part
        base = matrix[there, :]
        if col_base is not None:
            inside = jnp.logical_and(col_base >= 0, col_base < order)
            across = col_base + lax.broadcasted_iota(jnp.int32, (PANEL, cols), 1)
            begin = row_base + start + lax.broadcasted_iota(jnp.int32, (PANEL, cols), 0)
            base = jnp.where(inside, jnp.where(begin == across, 1.0, 0.0), base)
        result[there, :] = base - total


def center_kernel(step, mine, other, matrix, mate, half, table, fresh, fresh_high, fresh_low, right_high, right_low):
    core = lax.axis_index("core")
    rows = matrix.shape[0]
    order = JOINED * PANEL
    base = (lax.axis_index("y") - step) * order + lax.axis_index("x") * matrix.shape[1]
    pair = (pl.ds(0, rows), pl.ds(rows, rows))

    @pl.when(lax.axis_index("z") == step)
    def _():
        for at in range(2):

            @pl.when(core == at)
            def _():
                for q in range(JOINED):
                    table[pair[at], q * PANEL : (q + 1) * PANEL] = mine[q]
                for q in range(2):
                    across = 2 * (1 - at) + q
                    table[pair[1 - at], across * PANEL : (across + 1) * PANEL] = other[q]
                    table[across * PANEL : (across + 1) * PANEL, pair[at]] = mine[across].T

        composite(JOINED, table, fresh, fresh_high, fresh_low)
        inside = jnp.logical_and(base >= 0, base < order)
        for first, source in ((core * rows, matrix), ((1 - core) * rows, mate)):
            shape = source.shape
            unit = first + lax.broadcasted_iota(jnp.int32, shape, 0) == base + lax.broadcasted_iota(jnp.int32, shape, 1)
            high, low = halves(jnp.where(inside, jnp.where(unit, 1.0, 0.0), source[...]))
            there = pl.ds(pl.multiple_of(first, rows), rows)
            right_high[there, :] = high
            right_low[there, :] = low
        for q in range(rows // PANEL):
            there = pl.ds(pl.multiple_of(core * rows + q * PANEL, PANEL), PANEL)
            half[q * PANEL : (q + 1) * PANEL, :] = triple(table[there, :], right_high[...], right_low[...])


def center_both_kernel(step, mine, other, matrix, mate, strips, a_top, c_top, half, a_solved, table, fresh, fresh_high, fresh_low, right_high, right_low, *a_scratch):
    center_kernel(step, mine, other, matrix, mate, half, table, fresh, fresh_high, fresh_low, right_high, right_low)
    a_table, a_fresh, a_fresh_high, a_fresh_low, a_right_high, a_right_low = a_scratch

    @pl.when(jnp.logical_and(lax.axis_index("z") == 0, lax.axis_index("core") == 0))
    def _():
        order, cols = a_top.shape
        a_table[...] = strips[0]
        composite(STEPS_A, a_table, a_fresh, a_fresh_high, a_fresh_low)
        base = (lax.axis_index("y") * 4 + lax.axis_index("x")) * cols
        unit = lax.broadcasted_iota(jnp.int32, (order, cols), 0) == base + lax.broadcasted_iota(jnp.int32, (order, cols), 1)
        high, low = halves(jnp.where(base < order, jnp.where(unit, 1.0, 0.0), a_top[...]))
        a_right_high[:, :cols] = high
        a_right_low[:, :cols] = low
        high, low = halves(c_top[...])
        a_right_high[:, cols:] = high
        a_right_low[:, cols:] = low
        for q in range(STEPS_A):
            there = slice(q * PANEL, (q + 1) * PANEL)
            a_solved[there, :] = triple(a_table[there, :], a_right_high[...], a_right_low[...])


def update_kernel(step, matrix, column, solved, result, solved_high, solved_low):
    order = JOINED * PANEL
    rows = matrix.shape[0]
    row_base = (lax.axis_index("z") - step) * order + lax.axis_index("core") * rows
    col_base = (lax.axis_index("y") - step) * order + lax.axis_index("x") * matrix.shape[1]
    for core in range(2):
        high, low = halves(solved[core])
        solved_high[core * rows : (core + 1) * rows, :] = high
        solved_low[core * rows : (core + 1) * rows, :] = low
    piece = lambda start, q: column[q, pl.ds(start, PANEL), :]
    left_side(matrix, result, piece, row_base, col_base, order, solved_high, solved_low)


def a_update_kernel(matrix, other, strips, solved, result, other_result, solved_high, solved_low):
    order = STEPS_A * PANEL
    cols = matrix.shape[1]
    row_base = (lax.axis_index("z") * 2 + lax.axis_index("core")) * matrix.shape[0]
    col_base = (lax.axis_index("y") * 4 + lax.axis_index("x")) * cols
    high, low = halves(solved[...])
    solved_high[...] = high
    solved_low[...] = low

    def piece(start, q):
        among = pl.ds(pl.multiple_of(lax.rem(start, order), PANEL), PANEL)
        return strips[start // order, pl.ds(q * PANEL, PANEL), among].T

    left_side(matrix, result, piece, row_base, col_base, order, solved_high.at[:, :cols], solved_low.at[:, :cols])
    left_side(other, other_result, piece, row_base, None, order, solved_high.at[:, cols:], solved_low.at[:, cols:])


CHUNKS = 4
AHEAD = (0, 1)
BEHIND = (2, 3)


def ring(index, by):
    return lax.rem(index + by, 4)


def send(source, target, sent, received, where):
    return pltpu.make_async_remote_copy(
        src_ref=source, dst_ref=target, send_sem=sent, recv_sem=received,
        device_id=where, device_id_type=pl.DeviceIdType.MESH,
    )


def greet(neighbours, tells=None, teller_of=None, told=None):
    barrier = pltpu.get_barrier_semaphore()
    for where in neighbours:
        pl.semaphore_signal(barrier, inc=1, device_id=where, device_id_type=pl.DeviceIdType.MESH)
    if tells is not None:

        @pl.when(tells)
        def _():
            pl.semaphore_signal(barrier, inc=1, device_id=teller_of, device_id_type=pl.DeviceIdType.MESH)

    if told is None:
        pl.semaphore_wait(barrier, len(neighbours))
    else:

        @pl.when(told)
        def _():
            pl.semaphore_wait(barrier, len(neighbours) + 1)

        @pl.when(jnp.logical_not(told))
        def _():
            pl.semaphore_wait(barrier, len(neighbours))


def chunk(h, rows=512):
    return pl.ds(h * (rows // CHUNKS), rows // CHUNKS)


def both(left, right):
    return left if right is True else jnp.logical_and(left, right)


def spread(axis, step, source, landing, sent, received, follow, active=True):
    place = lax.axis_index(axis)
    apart = lax.rem(place - step + 4, 4)
    up, down = {axis: ring(place, 1)}, {axis: ring(place, 3)}

    def copy(ref, h, side):
        return send(ref.at[chunk(h)], landing.at[chunk(h)], sent.at[side, h], received.at[h], (up, down)[side])

    def begin():
        @pl.when(both(apart == 0, active))
        def _():
            for one, two in zip(AHEAD + BEHIND, BEHIND + AHEAD):
                copy(source, one, 0).start()
                copy(source, two, 1).start()
            for h in range(CHUNKS):
                follow(h, source)

    def relay():
        def take(order, onward, side):
            for h in order:
                copy(landing, h, 0).wait_recv()
                if h in onward:
                    copy(landing, h, side).start()
                follow(h, landing)

        @pl.when(both(apart == 1, active))
        def _():
            take(AHEAD + BEHIND, AHEAD, 0)

        @pl.when(both(apart == 3, active))
        def _():
            take(BEHIND + AHEAD, BEHIND, 1)

        @pl.when(both(apart == 2, active))
        def _():
            take((0, 2, 1, 3), (), 0)

    def finish():
        @pl.when(both(apart == 0, active))
        def _():
            for h in range(CHUNKS):
                copy(source, h, 0).wait_send()
                copy(source, h, 1).wait_send()

        @pl.when(both(apart == 1, active))
        def _():
            for h in AHEAD:
                copy(landing, h, 0).wait_send()

        @pl.when(both(apart == 3, active))
        def _():
            for h in BEHIND:
                copy(landing, h, 1).wait_send()

    return apart, begin, relay, finish


def nothing(h, ref):
    pass


def gather(step, matrix, column, other, mate, y_sent, y_got, x_sent, x_got, far_sent, far_got, core_sent, core_got):
    x = lax.axis_index("x")
    core = lax.axis_index("core")
    right, left, far = ring(x, 1), ring(x, 3), ring(x, 2)
    partner = {"core": 1 - core}
    center = lax.axis_index("z") == step
    swap = send(matrix, mate, core_sent.at[2], core_got.at[2], partner)

    def sideways(h, ref):
        return [
            send(ref.at[chunk(h)], column.at[x, chunk(h)], x_sent.at[0, h], x_got.at[0, h], {"x": right}),
            send(ref.at[chunk(h)], column.at[x, chunk(h)], x_sent.at[1, h], x_got.at[1, h], {"x": left}),
        ]

    def follow(h, ref):
        for copy in sideways(h, ref):
            copy.start()

    apart, begin, relay, finish = spread("y", step, matrix, column.at[x], y_sent, y_got, follow)

    def start():
        begin()

        @pl.when(center)
        def _():
            swap.start()

    def give(place, ref):
        slot = lax.rem(place, 2)
        return send(ref, other.at[slot], core_sent.at[slot], core_got.at[slot], partner)

    def maybe_give(place, ref, also=True):
        @pl.when(both(jnp.logical_and(center, place // 2 == core), also))
        def _():
            give(place, ref).start()

    def arrive(place, h, received):
        ref = column.at[place, chunk(h)]
        send(ref, ref, x_sent.at[0, h], received, {"x": right}).wait_recv()

    def pass_on(h):
        place, where = (left, right) if h in AHEAD else (right, left)
        ref = column.at[place, chunk(h)]
        return send(ref, ref, far_sent.at[h], far_got.at[h], {"x": where})

    def middle():
        relay()
        maybe_give(x, matrix, apart == 0)
        maybe_give(x, column.at[x], apart != 0)

        @pl.when(apart == 0)
        def _():
            column[x] = matrix[...]

        for one, two in zip(AHEAD, BEHIND):
            arrive(left, one, x_got.at[0, one])
            pass_on(one).start()
            arrive(right, two, x_got.at[1, two])
            pass_on(two).start()
        for one, two in zip(AHEAD, BEHIND):
            arrive(right, one, x_got.at[1, one])
            arrive(left, two, x_got.at[0, two])
        maybe_give(left, column.at[left])
        maybe_give(right, column.at[right])
        for h in range(CHUNKS):
            arrive(far, h, far_got.at[h])
        maybe_give(far, column.at[far])

    def end():
        finish()
        for h in range(CHUNKS):
            for copy in sideways(h, matrix):
                copy.wait_send()
            pass_on(h).wait_send()

        @pl.when(center)
        def _():
            swap.wait()
            give(0, matrix).wait()
            give(1, matrix).wait()

    return start, middle, end


def gather_neighbours():
    x, y = lax.axis_index("x"), lax.axis_index("y")
    return [{"y": ring(y, 1)}, {"y": ring(y, 3)}, {"x": ring(x, 1)}, {"x": ring(x, 3)}, {"core": 1 - lax.axis_index("core")}]


def gather_kernel(step, matrix, column, other, mate, *flags_of):
    greet(gather_neighbours())
    for act in gather(step, matrix, column, other, mate, *flags_of):
        act()


def gather_first_kernel(step, matrix, a_top, column, other, mate, seed, *flags_of):
    *flags_of, seed_sent, seed_got = flags_of
    z, core, y, x = (lax.axis_index(axis) for axis in AXES)
    home = jnp.logical_and(z == 0, core == 0)
    goal = jnp.logical_and(z == y, core == x // 2)
    stays = jnp.logical_and(home, goal)
    goes = jnp.logical_and(home, jnp.logical_not(goal))
    comes = jnp.logical_and(goal, jnp.logical_not(home))
    greet(gather_neighbours(), comes, {"z": 0, "core": 0}, goes)
    copy = send(a_top, seed, seed_sent, seed_got, {"z": y, "core": x // 2})

    @pl.when(goes)
    def _():
        copy.start()

    for act in gather(step, matrix, column, other, mate, *flags_of):
        act()

    @pl.when(stays)
    def _():
        seed[...] = a_top[...]

    @pl.when(goes)
    def _():
        copy.wait_send()

    @pl.when(comes)
    def _():
        copy.wait_recv()


def gather_last_kernel(step, matrix, a_solved, column, other, mate, a_shared, *flags_of):
    *flags_of, z_sent, z_got, pass_sent, pass_got = flags_of
    z, core = lax.axis_index("z"), lax.axis_index("core")
    partner = {"core": 1 - core}
    greet(gather_neighbours() + [{"z": ring(z, 1)}, {"z": ring(z, 3)}])

    def give(h, ref):
        return send(ref.at[chunk(h)], a_shared.at[chunk(h)], pass_sent.at[h], pass_got.at[h], partner)

    def follow(h, ref):
        give(h, ref).start()

    apart, begin, relay, finish = spread("z", 0, a_solved, a_shared, z_sent, z_got, follow, core == 0)
    start, middle, end = gather(step, matrix, column, other, mate, *flags_of)
    start()
    begin()
    middle()
    relay()

    @pl.when(jnp.logical_and(apart == 0, core == 0))
    def _():
        a_shared[...] = a_solved[...]

    end()
    finish()

    @pl.when(core == 0)
    def _():
        for h in range(CHUNKS):
            give(h, a_solved).wait_send()

    @pl.when(core == 1)
    def _():
        for h in range(CHUNKS):
            give(h, a_solved).wait_recv()


def share(step, half, solved, z_sent, z_got, core_sent, core_got):
    core = lax.axis_index("core")
    partner = {"core": 1 - core}

    def give(h, ref):
        return send(ref.at[chunk(h)], solved.at[core, chunk(h)], core_sent.at[h], core_got.at[h], partner)

    def follow(h, ref):
        give(h, ref).start()

    apart, begin, relay, finish = spread("z", step, half, solved.at[core], z_sent, z_got, follow)

    def end():
        @pl.when(apart == 0)
        def _():
            solved[core] = half[...]

        finish()
        for h in range(CHUNKS):
            give(h, half).wait_send()
            ref = solved.at[1 - core, chunk(h)]
            send(ref, ref, core_sent.at[h], core_got.at[h], partner).wait_recv()

    return begin, relay, end


def share_neighbours():
    z = lax.axis_index("z")
    return [{"z": ring(z, 1)}, {"z": ring(z, 3)}, {"core": 1 - lax.axis_index("core")}]


def share_kernel(step, half, solved, *flags_of):
    greet(share_neighbours())
    for act in share(step, half, solved, *flags_of):
        act()


def share_first_kernel(step, half, seed, solved, strip, *flags_of):
    *flags_of, y_sent, y_got = flags_of
    y = lax.axis_index("y")
    holds = lax.axis_index("core") == lax.axis_index("x") // 2
    greet(share_neighbours() + [{"y": ring(y, 1)}, {"y": ring(y, 3)}])
    begin, relay, end = share(step, half, solved, *flags_of)
    apart, also_begin, also_relay, also_finish = spread("y", lax.axis_index("z"), seed, strip, y_sent, y_got, nothing, holds)
    begin()
    also_begin()
    relay()
    also_relay()

    @pl.when(jnp.logical_and(holds, apart == 0))
    def _():
        strip[...] = seed[...]

    end()
    also_finish()


def share_second_kernel(step, half, strip, solved, strips, *flags_of):
    *flags_of, x_sent, x_got = flags_of
    x, core = lax.axis_index("x"), lax.axis_index("core")
    greet(share_neighbours() + [{"x": ring(x, 1)}, {"x": ring(x, 3)}])
    begin, relay, end = share(step, half, solved, *flags_of)
    pair = [spread("x", 2 * core + s, strip, strips.at[s], x_sent.at[s], x_got.at[s], nothing) for s in range(2)]
    begin()
    for one in pair:
        one[1]()
    relay()
    for one in pair:
        one[2]()
    for s in range(2):

        @pl.when(pair[s][0] == 0)
        def _():
            strips[s] = strip[...]

    end()
    for one in pair:
        one[3]()


def sum_kernel(value, total, first, second, between, first_sent, first_got, second_sent, second_got):
    z, core, y, x = (lax.axis_index(axis) for axis in AXES)
    line, plane = z * 2 + core, y * 4 + x

    def of_line(by):
        place = lax.rem(line + by, 8)
        return {"z": place // 2, "core": lax.rem(place, 2)}

    def of_plane(by):
        place = lax.rem(plane + by, 16)
        return {"y": place // 4, "x": lax.rem(place, 4)}

    greet([of_line(by) for by in range(1, 8)] + [of_plane(by) for by in range(1, 16)])
    copies = [send(value, first.at[by - 1], first_sent.at[by - 1], first_got.at[by - 1], of_line(by)) for by in range(1, 8)]
    for copy in copies:
        copy.start()
    for copy in copies:
        copy.wait()
    result = value[...]
    for by in range(7):
        result = result + first[by]
    between[...] = result
    copies = [send(between, second.at[by - 1], second_sent.at[by - 1], second_got.at[by - 1], of_plane(by)) for by in range(1, 16)]
    for copy in copies:
        copy.start()
    for copy in copies:
        copy.wait()
    for by in range(15):
        result = result + second[by]
    total[...] = result


def scratch(order, cols):
    return [
        pltpu.VMEM((order, order), F32),
        pltpu.VMEM((PANEL, order), F32),
        pltpu.VMEM((PANEL, order), BF16),
        pltpu.VMEM((PANEL, order), BF16),
        *pair_of(order, cols),
    ]


def pair_of(order, cols):
    return [pltpu.VMEM((order, cols), BF16), pltpu.VMEM((order, cols), BF16)]


def call(kernel, outs, scratch_shapes, operands, flops, identity=None):
    space = pl.BlockSpec(memory_space=pltpu.VMEM)
    more = {} if identity is None else dict(collective_id=identity, has_side_effects=True)
    return pl.pallas_call(
        kernel,
        out_shape=[jax.ShapeDtypeStruct(shape, F32) for shape in outs],
        in_specs=[space] * len(operands),
        out_specs=[space] * len(outs),
        scratch_shapes=scratch_shapes,
        compiler_params=pltpu.CompilerParams(vmem_limit_bytes=48 * 1024 * 1024, **more),
        cost_estimate=pl.CostEstimate(flops=flops, bytes_accessed=0, transcendentals=0),
    )(*operands)


def flags(*shape):
    return pltpu.SemaphoreType.DMA(shape)


def sweeps(a_matrix, b_matrix, c_matrix):
    rows, cols = b_matrix.shape
    order = JOINED * PANEL
    a_order = STEPS_A * PANEL
    a_cols, c_cols = a_matrix.shape[1], c_matrix.shape[1]
    a_top, c_top = a_matrix[:a_order], c_matrix[:a_order]
    side = (a_order, a_cols)
    panel = [(4, rows, cols), (2, rows, cols), (rows, cols)]
    panel_flags = [flags(2, CHUNKS), flags(CHUNKS), flags(2, CHUNKS), flags(2, CHUNKS), flags(CHUNKS), flags(CHUNKS), flags(3), flags(3)]
    shared = [(2, rows, cols)]
    shared_flags = [flags(2, CHUNKS), flags(CHUNKS), flags(CHUNKS), flags(CHUNKS)]
    more_flags = [flags(2, CHUNKS), flags(CHUNKS)]
    matrix = b_matrix
    for step in range(STEPS_B // JOINED):
        last = STEPS_B // JOINED - 1
        bound = lambda kernel: functools.partial(kernel, step)
        if step == 0:
            column, other, mate, seed = call(
                bound(gather_first_kernel), panel + [side], panel_flags + [pltpu.SemaphoreType.DMA, pltpu.SemaphoreType.DMA],
                [matrix, a_top], 10**10, 2 * step,
            )
        elif step == last:
            column, other, mate, a_shared = call(
                bound(gather_last_kernel), panel + [(a_order, a_cols + c_cols)],
                panel_flags + more_flags + [flags(CHUNKS), flags(CHUNKS)], [matrix, a_solved], 10**10, 2 * step,
            )
        else:
            column, other, mate = call(bound(gather_kernel), panel, panel_flags, [matrix], 10**10, 2 * step)
        operands = [column, other, matrix, mate]
        if step == last - 1:
            half, a_solved = call(
                bound(center_both_kernel), [(rows, cols), (a_order, a_cols + c_cols)],
                scratch(order, cols) + scratch(a_order, a_cols + c_cols), operands + [strips, a_top, c_top], 10**10,
            )
        else:
            (half,) = call(bound(center_kernel), [(rows, cols)], scratch(order, cols), operands, 10**10)
        if step == 0:
            solved, strip = call(bound(share_first_kernel), shared + [side], shared_flags + more_flags, [half, seed], 10**10, 2 * step + 1)
        elif step == 1:
            solved, strips = call(
                bound(share_second_kernel), shared + [(2, *side)],
                shared_flags + [flags(2, 2, CHUNKS), flags(2, CHUNKS)], [half, strip], 10**10, 2 * step + 1,
            )
        else:
            (solved,) = call(bound(share_kernel), shared, shared_flags, [half], 10**10, 2 * step + 1)
        (matrix,) = call(bound(update_kernel), [(rows, cols)], pair_of(order, cols), [matrix, column, solved], 10**9)
    a_swept, c_swept = call(
        a_update_kernel, [a_matrix.shape, c_matrix.shape], pair_of(a_order, a_cols + c_cols),
        [a_matrix, c_matrix, strips, a_shared], 10**10,
    )
    return a_swept, c_swept, matrix


def squares(value):
    return jnp.sum(value * value)


def total_of(values):
    tile = (8, 128)
    corner = jnp.zeros(tile, F32).at[0, : len(values)].set(jnp.stack(values))
    (total,) = call(
        sum_kernel, [tile],
        [pltpu.VMEM((7, *tile), F32), pltpu.VMEM((15, *tile), F32), pltpu.VMEM(tile, F32), flags(7), flags(7), flags(15), flags(15)],
        [corner], 10**9, 2 * (STEPS_B // JOINED),
    )
    return [total[0, place] for place in range(len(values))]


def body(a_matrix, b_matrix, c_matrix):
    a_swept, c_swept, b_inverse = sweeps(a_matrix, b_matrix, c_matrix)
    b_squares, inv_squares = total_of([squares(b_matrix), squares(b_inverse)])
    scale = jnp.sqrt(jnp.sqrt(inv_squares / b_squares))
    b_next = 0.5 * (scale * b_matrix + b_inverse / scale)
    return (a_swept, c_swept, b_next)


def solution(mesh):
    finer = Mesh(mesh.devices.reshape(4, 2, 4, 4), AXES)
    placed = (P(ROW, COL), P(ROW, COL), P(ROW, COL))
    return jax.shard_map(body, mesh=finer, in_specs=placed, out_specs=placed, check_vma=False)
```

```python
import functools

import jax
import jax.numpy as jnp
from jax import lax
from jax.experimental import pallas as pl
from jax.experimental.pallas import tpu as pltpu
from jax.sharding import Mesh
from jax.sharding import PartitionSpec as P

PANEL = 256
SQUARINGS = 5
STEPS_A = 2
STEPS_B = 16
JOINED = 4
AXES = ("z", "core", "y", "x")
ROW = ("z", "core")
COL = ("y", "x")
F32 = jnp.float32
BF16 = jnp.bfloat16


def halves(value):
    high = value.astype(BF16)
    return high, (value - high.astype(F32)).astype(BF16)


def product(left, right):
    return jnp.dot(left, right, preferred_element_type=F32)


def triple(left, right_high, right_low):
    high, low = halves(left)
    return product(high, right_high) + product(high, right_low) + product(low, right_high)


def pivot_inverse(pivot):
    shape = (PANEL, PANEL)
    unit = lax.broadcasted_iota(jnp.int32, shape, 0) == lax.broadcasted_iota(jnp.int32, shape, 1)
    diagonal = jnp.where(unit, pivot, 0.0)
    down = 1.0 / jnp.sqrt(jnp.sum(diagonal, axis=1, keepdims=True))
    across = 1.0 / jnp.sqrt(jnp.sum(diagonal, axis=0, keepdims=True))
    scaled = pivot * down * across
    ceiling = jnp.max(jnp.sum(jnp.abs(scaled), axis=1, keepdims=True), axis=0, keepdims=True)
    eye = jnp.where(unit, 1.0, 0.0)
    power = eye - scaled / ceiling
    total = eye + power
    high, low = halves(power)
    power = product(high, high) + product(high, low) + product(low, high)
    for turn in range(SQUARINGS - 1):
        high, low = halves(jnp.concatenate([power, total], 0))
        both = product(high, high[:PANEL]) + product(high, low[:PANEL]) + product(low, high[:PANEL])
        power = both[:PANEL]
        total = total + both[PANEL:]
    high, low = halves(power)
    total = total + triple(total, high, low)
    return total / ceiling * down * across


def composite(count, table, fresh, fresh_high, fresh_low):
    @pl.loop(0, count)
    def _(p):
        here = pl.ds(pl.multiple_of(p * PANEL, PANEL), PANEL)
        inverse = pivot_inverse(table[here, here])
        high, low = halves(table[here, :])
        fresh[...] = triple(inverse, high, low)
        fresh[:, here] = inverse
        high, low = halves(fresh[...])
        fresh_high[...] = high
        fresh_low[...] = low

        @pl.loop(0, count)
        def _(q):
            @pl.when(q != p)
            def _():
                there = pl.ds(pl.multiple_of(q * PANEL, PANEL), PANEL)
                column = table[there, here]
                table[there, here] = jnp.zeros((PANEL, PANEL), F32)
                table[there, :] = table[there, :] - triple(column, fresh_high[...], fresh_low[...])

        table[here, :] = fresh[...]


def left_side(matrix, result, piece, row_base, col_base, order, solved_high, solved_low):
    rows, cols = matrix.shape

    @pl.loop(0, rows // PANEL)
    def _(r):
        start = pl.multiple_of(r * PANEL, PANEL)
        there = pl.ds(start, PANEL)
        down = row_base + start + lax.broadcasted_iota(jnp.int32, (PANEL, PANEL), 0)
        total = None
        for q in range(order // PANEL):
            unit = down == q * PANEL + lax.broadcasted_iota(jnp.int32, (PANEL, PANEL), 1)
            column = piece(start, q) - jnp.where(unit, 1.0, 0.0)
            among = pl.ds(q * PANEL, PANEL)
            part = triple(column, solved_high[among, :cols], solved_low[among, :cols])
            total = part if total is None else total + part
        base = matrix[there, :]
        if col_base is not None:
            inside = jnp.logical_and(col_base >= 0, col_base < order)
            across = col_base + lax.broadcasted_iota(jnp.int32, (PANEL, cols), 1)
            begin = row_base + start + lax.broadcasted_iota(jnp.int32, (PANEL, cols), 0)
            base = jnp.where(inside, jnp.where(begin == across, 1.0, 0.0), base)
        result[there, :] = base - total


def center(step, mine, other, matrix, mate, half, table, fresh, fresh_high, fresh_low, right_high, right_low):
    core = lax.axis_index("core")
    rows = matrix.shape[0]
    order = JOINED * PANEL
    base = (lax.axis_index("y") - step) * order + lax.axis_index("x") * matrix.shape[1]
    pair = (pl.ds(0, rows), pl.ds(rows, rows))
    for at in range(2):

        @pl.when(core == at)
        def _():
            for q in range(JOINED):
                table[pair[at], q * PANEL : (q + 1) * PANEL] = mine[q]
            for q in range(2):
                across = 2 * (1 - at) + q
                table[pair[1 - at], across * PANEL : (across + 1) * PANEL] = other[q]
                table[across * PANEL : (across + 1) * PANEL, pair[at]] = mine[across].T

    composite(JOINED, table, fresh, fresh_high, fresh_low)
    inside = jnp.logical_and(base >= 0, base < order)
    for first, source in ((core * rows, matrix), ((1 - core) * rows, mate)):
        shape = source.shape
        unit = first + lax.broadcasted_iota(jnp.int32, shape, 0) == base + lax.broadcasted_iota(jnp.int32, shape, 1)
        high, low = halves(jnp.where(inside, jnp.where(unit, 1.0, 0.0), source[...]))
        there = pl.ds(pl.multiple_of(first, rows), rows)
        right_high[there, :] = high
        right_low[there, :] = low
    for q in range(rows // PANEL):
        there = pl.ds(pl.multiple_of(core * rows + q * PANEL, PANEL), PANEL)
        half[q * PANEL : (q + 1) * PANEL, :] = triple(table[there, :], right_high[...], right_low[...])


def a_center(strips, a_top, c_top, solved, table, fresh, fresh_high, fresh_low, right_high, right_low):
    order, cols = a_top.shape
    table[...] = strips[0]
    composite(STEPS_A, table, fresh, fresh_high, fresh_low)
    base = (lax.axis_index("y") * 4 + lax.axis_index("x")) * cols
    unit = lax.broadcasted_iota(jnp.int32, (order, cols), 0) == base + lax.broadcasted_iota(jnp.int32, (order, cols), 1)
    high, low = halves(jnp.where(base < order, jnp.where(unit, 1.0, 0.0), a_top[...]))
    right_high[:, :cols] = high
    right_low[:, :cols] = low
    high, low = halves(c_top[...])
    right_high[:, cols:] = high
    right_low[:, cols:] = low
    for q in range(STEPS_A):
        there = slice(q * PANEL, (q + 1) * PANEL)
        solved[there, :] = triple(table[there, :], right_high[...], right_low[...])


def update(step, matrix, column, solved, result, solved_high, solved_low):
    order = JOINED * PANEL
    rows = matrix.shape[0]
    row_base = (lax.axis_index("z") - step) * order + lax.axis_index("core") * rows
    col_base = (lax.axis_index("y") - step) * order + lax.axis_index("x") * matrix.shape[1]
    for core in range(2):
        high, low = halves(solved[core])
        solved_high[core * rows : (core + 1) * rows, :] = high
        solved_low[core * rows : (core + 1) * rows, :] = low
    piece = lambda start, q: column[q, pl.ds(start, PANEL), :]
    left_side(matrix, result, piece, row_base, col_base, order, solved_high, solved_low)


def a_update(matrix, other, strips, solved, solved_high, solved_low):
    order = STEPS_A * PANEL
    cols = matrix.shape[1]
    row_base = (lax.axis_index("z") * 2 + lax.axis_index("core")) * matrix.shape[0]
    col_base = (lax.axis_index("y") * 4 + lax.axis_index("x")) * cols
    high, low = halves(solved[...])
    solved_high[...] = high
    solved_low[...] = low

    def piece(start, q):
        among = pl.ds(pl.multiple_of(lax.rem(start, order), PANEL), PANEL)
        return strips[start // order, pl.ds(q * PANEL, PANEL), among].T

    left_side(matrix, matrix, piece, row_base, col_base, order, solved_high.at[:, :cols], solved_low.at[:, :cols])
    left_side(other, other, piece, row_base, None, order, solved_high.at[:, cols:], solved_low.at[:, cols:])


CHUNKS = 4
AHEAD = (0, 1)
BEHIND = (2, 3)


def ring(index, by):
    return lax.rem(index + by, 4)


def send(source, target, sent, received, where):
    return pltpu.make_async_remote_copy(
        src_ref=source, dst_ref=target, send_sem=sent, recv_sem=received,
        device_id=where, device_id_type=pl.DeviceIdType.MESH,
    )


def greet(neighbours):
    barrier = pltpu.get_barrier_semaphore()
    for where in neighbours:
        pl.semaphore_signal(barrier, inc=1, device_id=where, device_id_type=pl.DeviceIdType.MESH)
    pl.semaphore_wait(barrier, len(neighbours))


def chunk(h, rows=512):
    return pl.ds(h * (rows // CHUNKS), rows // CHUNKS)


def both(left, right):
    return left if right is True else jnp.logical_and(left, right)


def spread(axis, step, source, landing, sent, received, follow, active=True):
    place = lax.axis_index(axis)
    apart = lax.rem(place - step + 4, 4)
    up, down = {axis: ring(place, 1)}, {axis: ring(place, 3)}

    def copy(ref, h, side):
        return send(ref.at[chunk(h)], landing.at[chunk(h)], sent.at[side, h], received.at[h], (up, down)[side])

    def begin():
        @pl.when(both(apart == 0, active))
        def _():
            for one, two in zip(AHEAD + BEHIND, BEHIND + AHEAD):
                copy(source, one, 0).start()
                copy(source, two, 1).start()
            for h in range(CHUNKS):
                follow(h, source)

    def relay():
        def take(order, onward, side):
            for h in order:
                copy(landing, h, 0).wait_recv()
                if h in onward:
                    copy(landing, h, side).start()
                follow(h, landing)

        @pl.when(both(apart == 1, active))
        def _():
            take(AHEAD + BEHIND, AHEAD, 0)

        @pl.when(both(apart == 3, active))
        def _():
            take(BEHIND + AHEAD, BEHIND, 1)

        @pl.when(both(apart == 2, active))
        def _():
            take((0, 2, 1, 3), (), 0)

    def finish():
        @pl.when(both(apart == 0, active))
        def _():
            for h in range(CHUNKS):
                copy(source, h, 0).wait_send()
                copy(source, h, 1).wait_send()

        @pl.when(both(apart == 1, active))
        def _():
            for h in AHEAD:
                copy(landing, h, 0).wait_send()

        @pl.when(both(apart == 3, active))
        def _():
            for h in BEHIND:
                copy(landing, h, 1).wait_send()

    return apart, begin, relay, finish


def nothing(h, ref):
    pass


def gather(step, matrix, column, other, mate, y_sent, y_got, x_sent, x_got, far_sent, far_got, core_sent, core_got):
    x = lax.axis_index("x")
    core = lax.axis_index("core")
    right, left, far = ring(x, 1), ring(x, 3), ring(x, 2)
    partner = {"core": 1 - core}
    centered = lax.axis_index("z") == step
    swap = send(matrix, mate, core_sent.at[2], core_got.at[2], partner)

    def sideways(h, ref):
        return [
            send(ref.at[chunk(h)], column.at[x, chunk(h)], x_sent.at[0, h], x_got.at[0, h], {"x": right}),
            send(ref.at[chunk(h)], column.at[x, chunk(h)], x_sent.at[1, h], x_got.at[1, h], {"x": left}),
        ]

    def follow(h, ref):
        for copy in sideways(h, ref):
            copy.start()

    apart, begin, relay, finish = spread("y", step, matrix, column.at[x], y_sent, y_got, follow)

    def start():
        begin()

        @pl.when(centered)
        def _():
            swap.start()

    def give(place, ref):
        slot = lax.rem(place, 2)
        return send(ref, other.at[slot], core_sent.at[slot], core_got.at[slot], partner)

    def maybe_give(place, ref, also=True):
        @pl.when(both(jnp.logical_and(centered, place // 2 == core), also))
        def _():
            give(place, ref).start()

    def arrive(place, h, received):
        ref = column.at[place, chunk(h)]
        send(ref, ref, x_sent.at[0, h], received, {"x": right}).wait_recv()

    def pass_on(h):
        place, where = (left, right) if h in AHEAD else (right, left)
        ref = column.at[place, chunk(h)]
        return send(ref, ref, far_sent.at[h], far_got.at[h], {"x": where})

    def middle():
        relay()
        maybe_give(x, matrix, apart == 0)
        maybe_give(x, column.at[x], apart != 0)

        @pl.when(apart == 0)
        def _():
            column[x] = matrix[...]

        for one, two in zip(AHEAD, BEHIND):
            arrive(left, one, x_got.at[0, one])
            pass_on(one).start()
            arrive(right, two, x_got.at[1, two])
            pass_on(two).start()
        for one, two in zip(AHEAD, BEHIND):
            arrive(right, one, x_got.at[1, one])
            arrive(left, two, x_got.at[0, two])
        maybe_give(left, column.at[left])
        maybe_give(right, column.at[right])
        for h in range(CHUNKS):
            arrive(far, h, far_got.at[h])
        maybe_give(far, column.at[far])

    def end():
        finish()
        for h in range(CHUNKS):
            for copy in sideways(h, matrix):
                copy.wait_send()
            pass_on(h).wait_send()

        @pl.when(centered)
        def _():
            swap.wait()
            give(0, matrix).wait()
            give(1, matrix).wait()

    return start, middle, end


def share(step, half, solved, z_sent, z_got, core_sent, core_got):
    core = lax.axis_index("core")
    partner = {"core": 1 - core}

    def give(h, ref):
        return send(ref.at[chunk(h)], solved.at[core, chunk(h)], core_sent.at[h], core_got.at[h], partner)

    def follow(h, ref):
        give(h, ref).start()

    apart, begin, relay, finish = spread("z", step, half, solved.at[core], z_sent, z_got, follow)

    def end():
        @pl.when(apart == 0)
        def _():
            solved[core] = half[...]

        finish()
        for h in range(CHUNKS):
            give(h, half).wait_send()
            ref = solved.at[1 - core, chunk(h)]
            send(ref, ref, core_sent.at[h], core_got.at[h], partner).wait_recv()

    return begin, relay, end


def peers():
    z, core, y, x = (lax.axis_index(axis) for axis in AXES)
    line, plane = z * 2 + core, y * 4 + x
    along, among = [], []
    for by in range(1, 8):
        place = lax.rem(line + by, 8)
        along.append({"z": place // 2, "core": lax.rem(place, 2)})
    for by in range(1, 16):
        place = lax.rem(plane + by, 16)
        among.append({"y": place // 4, "x": lax.rem(place, 4)})
    return along, among


def exchange(value, slots, sent, received, partners):
    copies = [send(value, slots.at[at], sent.at[at], received.at[at], where) for at, where in enumerate(partners)]
    for copy in copies:
        copy.start()
    for copy in copies:
        copy.wait()
    result = value[...]
    for at in range(len(partners)):
        result = result + slots[at]
    return result


def squares(value):
    return jnp.sum(jnp.sum(value * value, axis=0, keepdims=True), axis=1, keepdims=True)


def whole_kernel(a_hbm, b, c_hbm, a_out, c_out, b_out, *spaces):
    s = dict(zip(SPACES, spaces))
    z, core, y, x = (lax.axis_index(axis) for axis in AXES)
    a, c = s["a"], s["c"]
    a_order = STEPS_A * PANEL
    a_top, c_top = a.at[:a_order], c.at[:a_order]
    loads = [pltpu.make_async_copy(a_hbm, a, s["load"].at[0]), pltpu.make_async_copy(c_hbm, c, s["load"].at[1])]
    stores = [pltpu.make_async_copy(a, a_out, s["load"].at[0]), pltpu.make_async_copy(c, c_out, s["load"].at[1])]
    for copy in loads:
        copy.start()
    along, among = peers()
    greet(along + among)

    home = jnp.logical_and(z == 0, core == 0)
    holds = core == x // 2
    goal = jnp.logical_and(z == y, holds)
    stays = jnp.logical_and(home, goal)
    goes = jnp.logical_and(home, jnp.logical_not(goal))
    comes = jnp.logical_and(goal, jnp.logical_not(home))
    seeding = send(a_top, s["seed"], s["seed_sent"], s["seed_got"], {"z": y, "core": x // 2})
    partner = {"core": 1 - core}

    def a_give(h, ref):
        return send(ref.at[chunk(h)], s["a_shared"].at[chunk(h)], s["a_pass_sent"].at[h], s["a_pass_got"].at[h], partner)

    def a_follow(h, ref):
        a_give(h, ref).start()

    def along_y(source, active):
        return spread("y", z, source, s["strip"], s["ay_sent"], s["ay_got"], nothing, active)

    def along_x(active):
        return [
            spread("x", 2 * core + at, s["strip"], s["strips"].at[at], s["ax_sent"].at[at], s["ax_got"].at[at], nothing, active)
            for at in range(2)
        ]

    a_share = spread("z", 0, s["a_solved"], s["a_shared"], s["az_sent"], s["az_got"], a_follow, core == 0)

    def finish_a():
        a_update(a, c, s["strips"], s["a_shared"], s["a_solved_high"], s["a_solved_low"])
        for copy in stores:
            copy.start()

    matrix = b
    for step in range(STEPS_B // JOINED):
        column, other, mate, half, solved = (s[name].at[step] for name in ("column", "other", "mate", "half", "solved"))
        here, away = z == step, z != step
        start, middle, end = gather(step, matrix, column, other, mate, *(s[name].at[step] for name in GATHER_FLAGS))
        start()
        if step == 0:
            for copy in loads:
                copy.wait()

            @pl.when(goes)
            def _():
                seeding.start()

        middle()
        if step == 3:
            a_share[2]()
        end()
        if step == 0:

            @pl.when(goes)
            def _():
                seeding.wait_send()

            @pl.when(comes)
            def _():
                seeding.wait_recv()

            along_y(s["seed"], jnp.logical_and(holds, jnp.logical_not(stays)))[1]()
            along_y(a_top, stays)[1]()
        if step == 1:
            for one in along_x(True):
                one[1]()

        @pl.when(here)
        def _():
            center(step, column, other, matrix, mate, half, *(s[name] for name in ("table", "fresh", "fresh_high", "fresh_low", "right_high", "right_low")))

        if step == 0:
            along_y(s["seed"], jnp.logical_and(holds, away))[2]()
        if step == 1:
            for one in along_x(away):
                one[2]()
        if step == 2:

            @pl.when(home)
            def _():
                a_center(s["strips"], a_top, c_top, s["a_solved"], *(s[name] for name in ("a_table", "a_fresh", "a_fresh_high", "a_fresh_low", "a_right_high", "a_right_low")))

        if step == 3:
            @pl.when(jnp.logical_and(home, a_share[0] == 0))
            def _():
                s["a_shared"][...] = s["a_solved"][...]

            @pl.when(core == 1)
            def _():
                for h in range(CHUNKS):
                    a_give(h, s["a_solved"]).wait_recv()

            pl.when(away)(finish_a)

        begin, relay, close = share(step, half, solved, *(s[name].at[step] for name in SHARE_FLAGS))
        begin()
        relay()
        if step == 0:
            along_y(s["seed"], jnp.logical_and(holds, here))[2]()
            across = along_y(s["seed"], holds)

            @pl.when(stays)
            def _():
                s["strip"][...] = a_top[...]

            @pl.when(comes)
            def _():
                s["strip"][...] = s["seed"][...]

        if step == 1:
            for one in along_x(here):
                one[2]()
            for at, one in enumerate(along_x(True)):

                @pl.when(one[0] == 0)
                def _():
                    s["strips"][at] = s["strip"][...]

        if step == 3:
            pl.when(here)(finish_a)
        close()
        if step == 0:
            across[3]()
        if step == 1:
            for one in along_x(True):
                one[3]()
        update(step, matrix, column, solved, s["matrix"].at[step], s["solved_high"], s["solved_low"])
        matrix = s["matrix"].at[step]
        if step == 2:
            a_share[1]()

    lane = lax.broadcasted_iota(jnp.int32, (8, 128), 1)
    s["partial"][0] = jnp.where(lane == 0, squares(b[...]), squares(matrix[...]))
    s["partial"][1] = exchange(s["partial"].at[0], s["line"], s["line_sent"], s["line_got"], along)
    total = exchange(s["partial"].at[1], s["plane"], s["plane_sent"], s["plane_got"], among)
    scale = jnp.sqrt(jnp.sqrt(total[0:1, 1:2] / total[0:1, 0:1]))
    b_out[...] = 0.5 * (scale * b[...] + matrix[...] / scale)
    a_share[3]()

    @pl.when(core == 0)
    def _():
        for h in range(CHUNKS):
            a_give(h, s["a_solved"]).wait_send()

    for copy in stores:
        copy.wait()


GATHER_FLAGS = ("y_sent", "y_got", "x_sent", "x_got", "far_sent", "far_got", "core_sent", "core_got")
SHARE_FLAGS = ("z_sent", "z_got", "pass_sent", "pass_got")


def flags(*shape):
    return pltpu.SemaphoreType.DMA(shape)


def spaces_of(a_shape, b_shape, c_shape):
    steps = STEPS_B // JOINED
    order, a_order = JOINED * PANEL, STEPS_A * PANEL
    rows, cols = b_shape
    wide = a_shape[1] + c_shape[1]
    top = (a_order, a_shape[1])
    full = lambda *shape: pltpu.VMEM(shape, F32)
    short = lambda *shape: pltpu.VMEM(shape, BF16)
    ringed = (2, CHUNKS)
    return dict(
        a=full(*a_shape), c=full(*c_shape), load=flags(2),
        column=full(steps, 4, rows, cols), other=full(steps, 2, rows, cols), mate=full(steps, rows, cols),
        half=full(steps, rows, cols), solved=full(steps, 2, rows, cols), matrix=full(steps, rows, cols),
        table=full(order, order), fresh=full(PANEL, order), fresh_high=short(PANEL, order), fresh_low=short(PANEL, order),
        right_high=short(order, cols), right_low=short(order, cols), solved_high=short(order, cols), solved_low=short(order, cols),
        seed=full(*top), strip=full(*top), strips=full(2, *top), a_solved=full(a_order, wide), a_shared=full(a_order, wide),
        a_table=full(a_order, a_order), a_fresh=full(PANEL, a_order), a_fresh_high=short(PANEL, a_order), a_fresh_low=short(PANEL, a_order),
        a_right_high=short(a_order, wide), a_right_low=short(a_order, wide), a_solved_high=short(a_order, wide), a_solved_low=short(a_order, wide),
        partial=full(2, 8, 128), line=full(7, 8, 128), plane=full(15, 8, 128),
        y_sent=flags(steps, *ringed), y_got=flags(steps, CHUNKS), x_sent=flags(steps, *ringed), x_got=flags(steps, *ringed),
        far_sent=flags(steps, CHUNKS), far_got=flags(steps, CHUNKS), core_sent=flags(steps, 3), core_got=flags(steps, 3),
        z_sent=flags(steps, *ringed), z_got=flags(steps, CHUNKS), pass_sent=flags(steps, CHUNKS), pass_got=flags(steps, CHUNKS),
        seed_sent=pltpu.SemaphoreType.DMA, seed_got=pltpu.SemaphoreType.DMA,
        ay_sent=flags(*ringed), ay_got=flags(CHUNKS), ax_sent=flags(2, *ringed), ax_got=flags(2, CHUNKS),
        az_sent=flags(*ringed), az_got=flags(CHUNKS), a_pass_sent=flags(CHUNKS), a_pass_got=flags(CHUNKS),
        line_sent=flags(7), line_got=flags(7), plane_sent=flags(15), plane_got=flags(15),
    )


SPACES = tuple(spaces_of((1, 1), (1, 1), (1, 1)))


def body(a_matrix, b_matrix, c_matrix):
    held = pl.BlockSpec(memory_space=pltpu.VMEM)
    left = pl.BlockSpec(memory_space=pl.ANY)
    shapes = (a_matrix.shape, b_matrix.shape, c_matrix.shape)
    a_swept, c_swept, b_next = pl.pallas_call(
        whole_kernel,
        out_shape=[jax.ShapeDtypeStruct(shapes[at], F32) for at in (0, 2, 1)],
        in_specs=[left, held, left],
        out_specs=[left, left, held],
        scratch_shapes=list(spaces_of(*shapes).values()),
        compiler_params=pltpu.CompilerParams(vmem_limit_bytes=63 * 1024 * 1024, collective_id=0, has_side_effects=True),
    )(a_matrix, b_matrix, c_matrix)
    return (a_swept, c_swept, b_next)


def solution(mesh):
    finer = Mesh(mesh.devices.reshape(4, 2, 4, 4), AXES)
    placed = (P(ROW, COL), P(ROW, COL), P(ROW, COL))
    return jax.shard_map(body, mesh=finer, in_specs=placed, out_specs=placed, check_vma=False)
```

```python
import functools

import jax
import jax.numpy as jnp
from jax import lax
from jax.experimental import pallas as pl
from jax.experimental.pallas import tpu as pltpu
from jax.sharding import Mesh
from jax.sharding import PartitionSpec as P

PANEL = 256
SQUARINGS = 5
STEPS_A = 2
STEPS_B = 16
JOINED = 4
AXES = ("z", "core", "y", "x")
ROW = ("z", "core")
COL = ("y", "x")
F32 = jnp.float32
BF16 = jnp.bfloat16


def halves(value):
    high = value.astype(BF16)
    return high, (value - high.astype(F32)).astype(BF16)


def product(left, right):
    return jnp.dot(left, right, preferred_element_type=F32)


def summed(high, low, right_high, right_low):
    return product(high, right_high) + product(high, right_low) + product(low, right_high)


def triple(left, right_high, right_low):
    return summed(*halves(left), right_high, right_low)


def by_rows(high, low, right_high, right_low):
    cut = high.shape[0] // 2
    parts = [summed(high[at], low[at], right_high, right_low) for at in (slice(None, cut), slice(cut, None))]
    return jnp.concatenate(parts, 0)


def pivot_inverse(pivot):
    shape = (PANEL, PANEL)
    unit = lax.broadcasted_iota(jnp.int32, shape, 0) == lax.broadcasted_iota(jnp.int32, shape, 1)
    diagonal = jnp.where(unit, pivot, 0.0)
    down = 1.0 / jnp.sqrt(jnp.sum(diagonal, axis=1, keepdims=True))
    across = 1.0 / jnp.sqrt(jnp.sum(diagonal, axis=0, keepdims=True))
    scaled = pivot * down * across
    ceiling = jnp.max(jnp.sum(jnp.abs(scaled), axis=1, keepdims=True), axis=0, keepdims=True)
    eye = jnp.where(unit, 1.0, 0.0)
    power = eye - scaled / ceiling
    total = eye + power
    high, low = halves(power)
    power = by_rows(high, low, high, low)
    for turn in range(SQUARINGS - 1):
        high, low = halves(power)
        total_high, total_low = halves(total)
        pair = summed(high, low, jnp.concatenate([high, total_high], 1), jnp.concatenate([low, total_low], 1))
        power = pair[:, :PANEL]
        total = total + pair[:, PANEL:]
    total = total + by_rows(*halves(total), *halves(power))
    return total / ceiling * down * across


def composite(count, table, fresh, fresh_high, fresh_low):
    width = table.shape[1] // 2

    @pl.loop(0, count)
    def _(p):
        here = pl.ds(pl.multiple_of(p * PANEL, PANEL), PANEL)
        inverse = pivot_inverse(table[here, here])
        fresh[...] = triple(inverse, *halves(table[here, :]))
        fresh[:, here] = inverse
        high, low = halves(fresh[...])
        fresh_high[...] = high
        fresh_low[...] = low
        others = [pl.ds(pl.multiple_of(lax.rem(p + by, count) * PANEL, PANEL), PANEL) for by in range(1, count)]
        high, low = halves(jnp.concatenate([table[there, here] for there in others], 0))
        for there in others:
            table[there, here] = jnp.zeros((PANEL, PANEL), F32)
        for cols in (slice(0, width), slice(width, 2 * width)):
            taken = summed(high, low, fresh_high[:, cols], fresh_low[:, cols])
            for at, there in enumerate(others):
                table[there, cols] = table[there, cols] - taken[at * PANEL : (at + 1) * PANEL]
        table[here, :] = fresh[...]


def left_side(matrix, result, piece, row_base, col_base, order, solved_high, solved_low):
    rows, cols = matrix.shape

    @pl.loop(0, rows // PANEL)
    def _(r):
        start = pl.multiple_of(r * PANEL, PANEL)
        there = pl.ds(start, PANEL)
        down = row_base + start + lax.broadcasted_iota(jnp.int32, (PANEL, PANEL), 0)
        total = None
        for q in range(order // PANEL):
            unit = down == q * PANEL + lax.broadcasted_iota(jnp.int32, (PANEL, PANEL), 1)
            column = piece(start, q) - jnp.where(unit, 1.0, 0.0)
            among = pl.ds(q * PANEL, PANEL)
            part = triple(column, solved_high[among, :cols], solved_low[among, :cols])
            total = part if total is None else total + part
        base = matrix[there, :]
        if col_base is not None:
            inside = jnp.logical_and(col_base >= 0, col_base < order)
            across = col_base + lax.broadcasted_iota(jnp.int32, (PANEL, cols), 1)
            begin = row_base + start + lax.broadcasted_iota(jnp.int32, (PANEL, cols), 0)
            base = jnp.where(inside, jnp.where(begin == across, 1.0, 0.0), base)
        result[there, :] = base - total


def center(step, mine, other, matrix, mate, half, table, fresh, fresh_high, fresh_low, right_high, right_low):
    core = lax.axis_index("core")
    rows = matrix.shape[0]
    order = JOINED * PANEL
    base = (lax.axis_index("y") - step) * order + lax.axis_index("x") * matrix.shape[1]
    pair = (pl.ds(0, rows), pl.ds(rows, rows))
    for at in range(2):

        @pl.when(core == at)
        def _():
            for q in range(JOINED):
                table[pair[at], q * PANEL : (q + 1) * PANEL] = mine[q]
            for q in range(2):
                across = 2 * (1 - at) + q
                table[pair[1 - at], across * PANEL : (across + 1) * PANEL] = other[q]
                table[across * PANEL : (across + 1) * PANEL, pair[at]] = mine[across].T

    composite(JOINED, table, fresh, fresh_high, fresh_low)
    inside = jnp.logical_and(base >= 0, base < order)
    for first, source in ((core * rows, matrix), ((1 - core) * rows, mate)):
        shape = source.shape
        unit = first + lax.broadcasted_iota(jnp.int32, shape, 0) == base + lax.broadcasted_iota(jnp.int32, shape, 1)
        high, low = halves(jnp.where(inside, jnp.where(unit, 1.0, 0.0), source[...]))
        there = pl.ds(pl.multiple_of(first, rows), rows)
        right_high[there, :] = high
        right_low[there, :] = low
    for q in range(rows // PANEL):
        there = pl.ds(pl.multiple_of(core * rows + q * PANEL, PANEL), PANEL)
        half[q * PANEL : (q + 1) * PANEL, :] = triple(table[there, :], right_high[...], right_low[...])


def a_center(strips, a_top, c_top, solved, table, fresh, fresh_high, fresh_low, right_high, right_low):
    order, cols = a_top.shape
    table[...] = strips[0]
    composite(STEPS_A, table, fresh, fresh_high, fresh_low)
    base = (lax.axis_index("y") * 4 + lax.axis_index("x")) * cols
    unit = lax.broadcasted_iota(jnp.int32, (order, cols), 0) == base + lax.broadcasted_iota(jnp.int32, (order, cols), 1)
    high, low = halves(jnp.where(base < order, jnp.where(unit, 1.0, 0.0), a_top[...]))
    right_high[:, :cols] = high
    right_low[:, :cols] = low
    high, low = halves(c_top[...])
    right_high[:, cols:] = high
    right_low[:, cols:] = low
    for q in range(STEPS_A):
        there = slice(q * PANEL, (q + 1) * PANEL)
        solved[there, :] = triple(table[there, :], right_high[...], right_low[...])


def update(step, matrix, column, solved, result, solved_high, solved_low):
    order = JOINED * PANEL
    rows = matrix.shape[0]
    row_base = (lax.axis_index("z") - step) * order + lax.axis_index("core") * rows
    col_base = (lax.axis_index("y") - step) * order + lax.axis_index("x") * matrix.shape[1]
    for core in range(2):
        high, low = halves(solved[core])
        solved_high[core * rows : (core + 1) * rows, :] = high
        solved_low[core * rows : (core + 1) * rows, :] = low
    piece = lambda start, q: column[q, pl.ds(start, PANEL), :]
    left_side(matrix, result, piece, row_base, col_base, order, solved_high, solved_low)


def a_update(matrix, other, strips, solved, solved_high, solved_low):
    order = STEPS_A * PANEL
    cols = matrix.shape[1]
    row_base = (lax.axis_index("z") * 2 + lax.axis_index("core")) * matrix.shape[0]
    col_base = (lax.axis_index("y") * 4 + lax.axis_index("x")) * cols
    high, low = halves(solved[...])
    solved_high[...] = high
    solved_low[...] = low

    def piece(start, q):
        among = pl.ds(pl.multiple_of(lax.rem(start, order), PANEL), PANEL)
        return strips[start // order, pl.ds(q * PANEL, PANEL), among].T

    left_side(matrix, matrix, piece, row_base, col_base, order, solved_high.at[:, :cols], solved_low.at[:, :cols])
    left_side(other, other, piece, row_base, None, order, solved_high.at[:, cols:], solved_low.at[:, cols:])


CHUNKS = 8
AHEAD = tuple(range(CHUNKS // 2))
BEHIND = tuple(range(CHUNKS // 2, CHUNKS))


def ring(index, by):
    return lax.rem(index + by, 4)


def send(source, target, sent, received, where):
    return pltpu.make_async_remote_copy(
        src_ref=source, dst_ref=target, send_sem=sent, recv_sem=received,
        device_id=where, device_id_type=pl.DeviceIdType.MESH,
    )


def greet(neighbours):
    barrier = pltpu.get_barrier_semaphore()
    for where in neighbours:
        pl.semaphore_signal(barrier, inc=1, device_id=where, device_id_type=pl.DeviceIdType.MESH)
    pl.semaphore_wait(barrier, len(neighbours))


def chunk(h, rows=512):
    return pl.ds(h * (rows // CHUNKS), rows // CHUNKS)


def both(left, right):
    return left if right is True else jnp.logical_and(left, right)


def spread(axis, step, source, landing, sent, received, follow, active=True):
    place = lax.axis_index(axis)
    apart = lax.rem(place - step + 4, 4)
    up, down = {axis: ring(place, 1)}, {axis: ring(place, 3)}

    def copy(ref, h, side):
        return send(ref.at[chunk(h)], landing.at[chunk(h)], sent.at[side, h], received.at[h], (up, down)[side])

    def begin():
        @pl.when(both(apart == 0, active))
        def _():
            for one, two in zip(AHEAD + BEHIND, BEHIND + AHEAD):
                copy(source, one, 0).start()
                copy(source, two, 1).start()
            for h in range(CHUNKS):
                follow(h, source)

    def relay():
        def take(order, onward, side):
            for h in order:
                copy(landing, h, 0).wait_recv()
                if h in onward:
                    copy(landing, h, side).start()
                follow(h, landing)

        @pl.when(both(apart == 1, active))
        def _():
            take(AHEAD + BEHIND, AHEAD, 0)

        @pl.when(both(apart == 3, active))
        def _():
            take(BEHIND + AHEAD, BEHIND, 1)

        @pl.when(both(apart == 2, active))
        def _():
            take([h for two in zip(AHEAD, BEHIND) for h in two], (), 0)

    def finish():
        @pl.when(both(apart == 0, active))
        def _():
            for h in range(CHUNKS):
                copy(source, h, 0).wait_send()
                copy(source, h, 1).wait_send()

        @pl.when(both(apart == 1, active))
        def _():
            for h in AHEAD:
                copy(landing, h, 0).wait_send()

        @pl.when(both(apart == 3, active))
        def _():
            for h in BEHIND:
                copy(landing, h, 1).wait_send()

    return apart, begin, relay, finish


def nothing(h, ref):
    pass


def gather(step, matrix, column, other, mate, y_sent, y_got, x_sent, x_got, far_sent, far_got, core_sent, core_got):
    x = lax.axis_index("x")
    core = lax.axis_index("core")
    right, left, far = ring(x, 1), ring(x, 3), ring(x, 2)
    partner = {"core": 1 - core}
    centered = lax.axis_index("z") == step
    swap = send(matrix, mate, core_sent.at[2], core_got.at[2], partner)

    def sideways(h, ref):
        return [
            send(ref.at[chunk(h)], column.at[x, chunk(h)], x_sent.at[0, h], x_got.at[0, h], {"x": right}),
            send(ref.at[chunk(h)], column.at[x, chunk(h)], x_sent.at[1, h], x_got.at[1, h], {"x": left}),
        ]

    def follow(h, ref):
        for copy in sideways(h, ref):
            copy.start()

    apart, begin, relay, finish = spread("y", step, matrix, column.at[x], y_sent, y_got, follow)

    def start():
        begin()

        @pl.when(centered)
        def _():
            swap.start()

    def give(place, ref):
        slot = lax.rem(place, 2)
        return send(ref, other.at[slot], core_sent.at[slot], core_got.at[slot], partner)

    def maybe_give(place, ref, also=True):
        @pl.when(both(jnp.logical_and(centered, place // 2 == core), also))
        def _():
            give(place, ref).start()

    def arrive(place, h, received):
        ref = column.at[place, chunk(h)]
        send(ref, ref, x_sent.at[0, h], received, {"x": right}).wait_recv()

    def pass_on(h):
        place, where = (left, right) if h in AHEAD else (right, left)
        ref = column.at[place, chunk(h)]
        return send(ref, ref, far_sent.at[h], far_got.at[h], {"x": where})

    def middle():
        relay()
        maybe_give(x, matrix, apart == 0)
        maybe_give(x, column.at[x], apart != 0)

        @pl.when(apart == 0)
        def _():
            column[x] = matrix[...]

        for one, two in zip(AHEAD, BEHIND):
            arrive(left, one, x_got.at[0, one])
            pass_on(one).start()
            arrive(right, two, x_got.at[1, two])
            pass_on(two).start()
        for one, two in zip(AHEAD, BEHIND):
            arrive(right, one, x_got.at[1, one])
            arrive(left, two, x_got.at[0, two])
        maybe_give(left, column.at[left])
        maybe_give(right, column.at[right])
        for h in range(CHUNKS):
            arrive(far, h, far_got.at[h])
        maybe_give(far, column.at[far])

    def end():
        finish()
        for h in range(CHUNKS):
            for copy in sideways(h, matrix):
                copy.wait_send()
            pass_on(h).wait_send()

        @pl.when(centered)
        def _():
            swap.wait()
            give(0, matrix).wait()
            give(1, matrix).wait()

    return start, middle, end


def share(step, half, solved, z_sent, z_got, core_sent, core_got):
    core = lax.axis_index("core")
    partner = {"core": 1 - core}

    def give(h, ref):
        return send(ref.at[chunk(h)], solved.at[core, chunk(h)], core_sent.at[h], core_got.at[h], partner)

    def follow(h, ref):
        give(h, ref).start()

    apart, begin, relay, finish = spread("z", step, half, solved.at[core], z_sent, z_got, follow)

    def end():
        @pl.when(apart == 0)
        def _():
            solved[core] = half[...]

        finish()
        for h in range(CHUNKS):
            give(h, half).wait_send()
            ref = solved.at[1 - core, chunk(h)]
            send(ref, ref, core_sent.at[h], core_got.at[h], partner).wait_recv()

    return begin, relay, end


def peers():
    z, core, y, x = (lax.axis_index(axis) for axis in AXES)
    line, plane = z * 2 + core, y * 4 + x
    along, among = [], []
    for by in range(1, 8):
        place = lax.rem(line + by, 8)
        along.append({"z": place // 2, "core": lax.rem(place, 2)})
    for by in range(1, 16):
        place = lax.rem(plane + by, 16)
        among.append({"y": place // 4, "x": lax.rem(place, 4)})
    return along, among


def exchange(value, slots, sent, received, partners):
    copies = [send(value, slots.at[at], sent.at[at], received.at[at], where) for at, where in enumerate(partners)]
    for copy in copies:
        copy.start()
    for copy in copies:
        copy.wait()
    result = value[...]
    for at in range(len(partners)):
        result = result + slots[at]
    return result


def squares(value):
    return jnp.sum(jnp.sum(value * value, axis=0, keepdims=True), axis=1, keepdims=True)


def whole_kernel(a_hbm, b, c_hbm, a_out, c_out, b_out, *spaces):
    s = dict(zip(SPACES, spaces))
    z, core, y, x = (lax.axis_index(axis) for axis in AXES)
    a, c = s["a"], s["c"]
    a_order = STEPS_A * PANEL
    a_top, c_top = a.at[:a_order], c.at[:a_order]
    loads = [pltpu.make_async_copy(a_hbm, a, s["load"].at[0]), pltpu.make_async_copy(c_hbm, c, s["load"].at[1])]
    stores = [pltpu.make_async_copy(a, a_out, s["load"].at[0]), pltpu.make_async_copy(c, c_out, s["load"].at[1])]
    for copy in loads:
        copy.start()
    along, among = peers()
    greet(along + among)

    home = jnp.logical_and(z == 0, core == 0)
    holds = core == x // 2
    goal = jnp.logical_and(z == y, holds)
    stays = jnp.logical_and(home, goal)
    goes = jnp.logical_and(home, jnp.logical_not(goal))
    comes = jnp.logical_and(goal, jnp.logical_not(home))
    seeding = send(a_top, s["seed"], s["seed_sent"], s["seed_got"], {"z": y, "core": x // 2})
    partner = {"core": 1 - core}

    def a_give(h, ref):
        return send(ref.at[chunk(h)], s["a_shared"].at[chunk(h)], s["a_pass_sent"].at[h], s["a_pass_got"].at[h], partner)

    def a_follow(h, ref):
        a_give(h, ref).start()

    def along_y(source, active):
        return spread("y", z, source, s["strip"], s["ay_sent"], s["ay_got"], nothing, active)

    def along_x(active):
        return [
            spread("x", 2 * core + at, s["strip"], s["strips"].at[at], s["ax_sent"].at[at], s["ax_got"].at[at], nothing, active)
            for at in range(2)
        ]

    a_share = spread("z", 0, s["a_solved"], s["a_shared"], s["az_sent"], s["az_got"], a_follow, core == 0)

    def finish_a():
        a_update(a, c, s["strips"], s["a_shared"], s["a_solved_high"], s["a_solved_low"])
        for copy in stores:
            copy.start()

    matrix = b
    for step in range(STEPS_B // JOINED):
        column, other, mate, half, solved = (s[name].at[step] for name in ("column", "other", "mate", "half", "solved"))
        here, away = z == step, z != step
        start, middle, end = gather(step, matrix, column, other, mate, *(s[name].at[step] for name in GATHER_FLAGS))
        start()
        if step == 0:
            for copy in loads:
                copy.wait()

            @pl.when(goes)
            def _():
                seeding.start()

        middle()
        if step == 3:
            a_share[2]()
        end()
        if step == 0:

            @pl.when(goes)
            def _():
                seeding.wait_send()

            @pl.when(comes)
            def _():
                seeding.wait_recv()

            along_y(s["seed"], jnp.logical_and(holds, jnp.logical_not(stays)))[1]()
            along_y(a_top, stays)[1]()
        if step == 1:
            for one in along_x(True):
                one[1]()

        @pl.when(here)
        def _():
            center(step, column, other, matrix, mate, half, *(s[name] for name in ("table", "fresh", "fresh_high", "fresh_low", "right_high", "right_low")))

        if step == 0:
            along_y(s["seed"], jnp.logical_and(holds, away))[2]()
        if step == 1:
            for one in along_x(away):
                one[2]()
        if step == 2:

            @pl.when(home)
            def _():
                a_center(s["strips"], a_top, c_top, s["a_solved"], *(s[name] for name in ("a_table", "a_fresh", "a_fresh_high", "a_fresh_low", "a_right_high", "a_right_low")))

        if step == 3:
            @pl.when(jnp.logical_and(home, a_share[0] == 0))
            def _():
                s["a_shared"][...] = s["a_solved"][...]

            @pl.when(core == 1)
            def _():
                for h in range(CHUNKS):
                    a_give(h, s["a_solved"]).wait_recv()

            pl.when(away)(finish_a)

        begin, relay, close = share(step, half, solved, *(s[name].at[step] for name in SHARE_FLAGS))
        begin()
        relay()
        if step == 0:
            along_y(s["seed"], jnp.logical_and(holds, here))[2]()
            across = along_y(s["seed"], holds)

            @pl.when(stays)
            def _():
                s["strip"][...] = a_top[...]

            @pl.when(comes)
            def _():
                s["strip"][...] = s["seed"][...]

        if step == 1:
            for one in along_x(here):
                one[2]()
            for at, one in enumerate(along_x(True)):

                @pl.when(one[0] == 0)
                def _():
                    s["strips"][at] = s["strip"][...]

        if step == 3:
            pl.when(here)(finish_a)
        close()
        if step == 0:
            across[3]()
        if step == 1:
            for one in along_x(True):
                one[3]()
        update(step, matrix, column, solved, s["matrix"].at[step], s["solved_high"], s["solved_low"])
        matrix = s["matrix"].at[step]
        if step == 2:
            a_share[1]()

    lane = lax.broadcasted_iota(jnp.int32, (8, 128), 1)
    s["partial"][0] = jnp.where(lane == 0, squares(b[...]), squares(matrix[...]))
    s["partial"][1] = exchange(s["partial"].at[0], s["line"], s["line_sent"], s["line_got"], along)
    total = exchange(s["partial"].at[1], s["plane"], s["plane_sent"], s["plane_got"], among)
    scale = jnp.sqrt(jnp.sqrt(total[0:1, 1:2] / total[0:1, 0:1]))
    b_out[...] = 0.5 * (scale * b[...] + matrix[...] / scale)
    a_share[3]()

    @pl.when(core == 0)
    def _():
        for h in range(CHUNKS):
            a_give(h, s["a_solved"]).wait_send()

    for copy in stores:
        copy.wait()


GATHER_FLAGS = ("y_sent", "y_got", "x_sent", "x_got", "far_sent", "far_got", "core_sent", "core_got")
SHARE_FLAGS = ("z_sent", "z_got", "pass_sent", "pass_got")


def flags(*shape):
    return pltpu.SemaphoreType.DMA(shape)


def spaces_of(a_shape, b_shape, c_shape):
    steps = STEPS_B // JOINED
    order, a_order = JOINED * PANEL, STEPS_A * PANEL
    rows, cols = b_shape
    wide = a_shape[1] + c_shape[1]
    top = (a_order, a_shape[1])
    full = lambda *shape: pltpu.VMEM(shape, F32)
    short = lambda *shape: pltpu.VMEM(shape, BF16)
    ringed = (2, CHUNKS)
    return dict(
        a=full(*a_shape), c=full(*c_shape), load=flags(2),
        column=full(steps, 4, rows, cols), other=full(steps, 2, rows, cols), mate=full(steps, rows, cols),
        half=full(steps, rows, cols), solved=full(steps, 2, rows, cols), matrix=full(steps, rows, cols),
        table=full(order, order), fresh=full(PANEL, order), fresh_high=short(PANEL, order), fresh_low=short(PANEL, order),
        right_high=short(order, cols), right_low=short(order, cols), solved_high=short(order, cols), solved_low=short(order, cols),
        seed=full(*top), strip=full(*top), strips=full(2, *top), a_solved=full(a_order, wide), a_shared=full(a_order, wide),
        a_table=full(a_order, a_order), a_fresh=full(PANEL, a_order), a_fresh_high=short(PANEL, a_order), a_fresh_low=short(PANEL, a_order),
        a_right_high=short(a_order, wide), a_right_low=short(a_order, wide), a_solved_high=short(a_order, wide), a_solved_low=short(a_order, wide),
        partial=full(2, 8, 128), line=full(7, 8, 128), plane=full(15, 8, 128),
        y_sent=flags(steps, *ringed), y_got=flags(steps, CHUNKS), x_sent=flags(steps, *ringed), x_got=flags(steps, *ringed),
        far_sent=flags(steps, CHUNKS), far_got=flags(steps, CHUNKS), core_sent=flags(steps, 3), core_got=flags(steps, 3),
        z_sent=flags(steps, *ringed), z_got=flags(steps, CHUNKS), pass_sent=flags(steps, CHUNKS), pass_got=flags(steps, CHUNKS),
        seed_sent=pltpu.SemaphoreType.DMA, seed_got=pltpu.SemaphoreType.DMA,
        ay_sent=flags(*ringed), ay_got=flags(CHUNKS), ax_sent=flags(2, *ringed), ax_got=flags(2, CHUNKS),
        az_sent=flags(*ringed), az_got=flags(CHUNKS), a_pass_sent=flags(CHUNKS), a_pass_got=flags(CHUNKS),
        line_sent=flags(7), line_got=flags(7), plane_sent=flags(15), plane_got=flags(15),
    )


SPACES = tuple(spaces_of((1, 1), (1, 1), (1, 1)))


def body(a_matrix, b_matrix, c_matrix):
    held = pl.BlockSpec(memory_space=pltpu.VMEM)
    left = pl.BlockSpec(memory_space=pl.ANY)
    shapes = (a_matrix.shape, b_matrix.shape, c_matrix.shape)
    a_swept, c_swept, b_next = pl.pallas_call(
        whole_kernel,
        out_shape=[jax.ShapeDtypeStruct(shapes[at], F32) for at in (0, 2, 1)],
        in_specs=[left, held, left],
        out_specs=[left, left, held],
        scratch_shapes=list(spaces_of(*shapes).values()),
        compiler_params=pltpu.CompilerParams(vmem_limit_bytes=63 * 1024 * 1024, collective_id=0, has_side_effects=True),
    )(a_matrix, b_matrix, c_matrix)
    return (a_swept, c_swept, b_next)


def solution(mesh):
    finer = Mesh(mesh.devices.reshape(4, 2, 4, 4), AXES)
    placed = (P(ROW, COL), P(ROW, COL), P(ROW, COL))
    return jax.shard_map(body, mesh=finer, in_specs=placed, out_specs=placed, check_vma=False)
```

```python
import functools

import jax
import jax.numpy as jnp
from jax import lax
from jax.experimental import pallas as pl
from jax.experimental.pallas import tpu as pltpu
from jax.sharding import Mesh
from jax.sharding import PartitionSpec as P

PANEL = 256
SQUARINGS = 5
STEPS_A = 2
STEPS_B = 16
JOINED = 4
AXES = ("z", "core", "y", "x")
ROW = ("z", "core")
COL = ("y", "x")
F32 = jnp.float32
BF16 = jnp.bfloat16


def halves(value):
    high = value.astype(BF16)
    return high, (value - high.astype(F32)).astype(BF16)


def product(left, right):
    return jnp.dot(left, right, preferred_element_type=F32)


def summed(high, low, right_high, right_low):
    return product(high, right_high) + product(high, right_low) + product(low, right_high)


def triple(left, right_high, right_low):
    return summed(*halves(left), right_high, right_low)


def by_rows(high, low, right_high, right_low):
    cut = high.shape[0] // 2
    parts = [summed(high[at], low[at], right_high, right_low) for at in (slice(None, cut), slice(cut, None))]
    return jnp.concatenate(parts, 0)


def pivot_inverse(pivot, between=()):
    parts = iter(between)

    def fill():
        for part in next(parts, ()):
            part()

    shape = (PANEL, PANEL)
    unit = lax.broadcasted_iota(jnp.int32, shape, 0) == lax.broadcasted_iota(jnp.int32, shape, 1)
    diagonal = jnp.where(unit, pivot, 0.0)
    down = 1.0 / jnp.sqrt(jnp.sum(diagonal, axis=1, keepdims=True))
    across = 1.0 / jnp.sqrt(jnp.sum(diagonal, axis=0, keepdims=True))
    scaled = pivot * down * across
    ceiling = jnp.max(jnp.sum(jnp.abs(scaled), axis=1, keepdims=True), axis=0, keepdims=True)
    eye = jnp.where(unit, 1.0, 0.0)
    power = eye - scaled / ceiling
    fill()
    total = eye + power
    high, low = halves(power)
    power = by_rows(high, low, high, low)
    fill()
    for turn in range(SQUARINGS - 1):
        high, low = halves(power)
        total_high, total_low = halves(total)
        pair = summed(high, low, jnp.concatenate([high, total_high], 1), jnp.concatenate([low, total_low], 1))
        fill()
        power = pair[:, :PANEL]
        total = total + pair[:, PANEL:]
    total = total + by_rows(*halves(total), *halves(power))
    return total / ceiling * down * across


def composite(count, table, fresh, fresh_high, fresh_low, inverse_of):
    inverse_of[...] = pivot_inverse(table[:PANEL, :PANEL])

    def panel(p, more):
        here = pl.ds(pl.multiple_of(p * PANEL, PANEL), PANEL)
        others = [pl.ds(pl.multiple_of(lax.rem(p + by, count) * PANEL, PANEL), PANEL) for by in range(1, count)]
        inverse = inverse_of[...]
        inverse_high, inverse_low = halves(inverse)
        high, low = halves(jnp.concatenate([table[there, here] for there in others], 0))

        def row():
            fresh[...] = summed(inverse_high, inverse_low, *halves(table[here, :]))
            fresh[:, here] = inverse
            fresh_high[...], fresh_low[...] = halves(fresh[...])
            for there in others:
                table[there, here] = jnp.zeros((PANEL, PANEL), F32)

        def rest(at):
            cols = slice(at * PANEL, (at + 1) * PANEL)
            taken = summed(high, low, fresh_high[:, cols], fresh_low[:, cols])
            for nth, there in enumerate(others):
                table[there, cols] = table[there, cols] - taken[nth * PANEL : (nth + 1) * PANEL]

        parts = [row] + [functools.partial(rest, at) for at in range(count)]
        if more:
            after = others[0]
            solved = by_rows(inverse_high, inverse_low, *halves(table[here, after]))
            block = table[after, after] - by_rows(high[:PANEL], low[:PANEL], *halves(solved))
            inverse_of[...] = pivot_inverse(block, [(part,) for part in parts])
        else:
            for part in parts:
                part()
        table[here, :] = fresh[...]

    @pl.loop(0, count - 1)
    def _(p):
        panel(p, True)

    panel(count - 1, False)


def left_side(matrix, result, piece, row_base, col_base, order, solved_high, solved_low):
    rows, cols = matrix.shape

    @pl.loop(0, rows // PANEL)
    def _(r):
        start = pl.multiple_of(r * PANEL, PANEL)
        there = pl.ds(start, PANEL)
        down = row_base + start + lax.broadcasted_iota(jnp.int32, (PANEL, PANEL), 0)
        total = None
        for q in range(order // PANEL):
            unit = down == q * PANEL + lax.broadcasted_iota(jnp.int32, (PANEL, PANEL), 1)
            column = piece(start, q) - jnp.where(unit, 1.0, 0.0)
            among = pl.ds(q * PANEL, PANEL)
            part = triple(column, solved_high[among, :cols], solved_low[among, :cols])
            total = part if total is None else total + part
        base = matrix[there, :]
        if col_base is not None:
            inside = jnp.logical_and(col_base >= 0, col_base < order)
            across = col_base + lax.broadcasted_iota(jnp.int32, (PANEL, cols), 1)
            begin = row_base + start + lax.broadcasted_iota(jnp.int32, (PANEL, cols), 0)
            base = jnp.where(inside, jnp.where(begin == across, 1.0, 0.0), base)
        result[there, :] = base - total


def center(step, mine, other, matrix, mate, half, table, fresh, fresh_high, fresh_low, inverse_of, right_high, right_low):
    core = lax.axis_index("core")
    rows = matrix.shape[0]
    order = JOINED * PANEL
    base = (lax.axis_index("y") - step) * order + lax.axis_index("x") * matrix.shape[1]
    pair = (pl.ds(0, rows), pl.ds(rows, rows))
    for at in range(2):

        @pl.when(core == at)
        def _():
            for q in range(JOINED):
                table[pair[at], q * PANEL : (q + 1) * PANEL] = mine[q]
            for q in range(2):
                across = 2 * (1 - at) + q
                table[pair[1 - at], across * PANEL : (across + 1) * PANEL] = other[q]
                table[across * PANEL : (across + 1) * PANEL, pair[at]] = mine[across].T

    composite(JOINED, table, fresh, fresh_high, fresh_low, inverse_of)
    inside = jnp.logical_and(base >= 0, base < order)
    for first, source in ((core * rows, matrix), ((1 - core) * rows, mate)):
        shape = source.shape
        unit = first + lax.broadcasted_iota(jnp.int32, shape, 0) == base + lax.broadcasted_iota(jnp.int32, shape, 1)
        high, low = halves(jnp.where(inside, jnp.where(unit, 1.0, 0.0), source[...]))
        there = pl.ds(pl.multiple_of(first, rows), rows)
        right_high[there, :] = high
        right_low[there, :] = low
    for q in range(rows // PANEL):
        there = pl.ds(pl.multiple_of(core * rows + q * PANEL, PANEL), PANEL)
        half[q * PANEL : (q + 1) * PANEL, :] = triple(table[there, :], right_high[...], right_low[...])


def a_center(strips, a_top, c_top, solved, table, fresh, fresh_high, fresh_low, inverse_of, right_high, right_low):
    order, cols = a_top.shape
    table[...] = strips[0]
    composite(STEPS_A, table, fresh, fresh_high, fresh_low, inverse_of)
    base = (lax.axis_index("y") * 4 + lax.axis_index("x")) * cols
    unit = lax.broadcasted_iota(jnp.int32, (order, cols), 0) == base + lax.broadcasted_iota(jnp.int32, (order, cols), 1)
    high, low = halves(jnp.where(base < order, jnp.where(unit, 1.0, 0.0), a_top[...]))
    right_high[:, :cols] = high
    right_low[:, :cols] = low
    high, low = halves(c_top[...])
    right_high[:, cols:] = high
    right_low[:, cols:] = low
    for q in range(STEPS_A):
        there = slice(q * PANEL, (q + 1) * PANEL)
        solved[there, :] = triple(table[there, :], right_high[...], right_low[...])


def update(step, matrix, column, solved, result, solved_high, solved_low):
    order = JOINED * PANEL
    rows = matrix.shape[0]
    row_base = (lax.axis_index("z") - step) * order + lax.axis_index("core") * rows
    col_base = (lax.axis_index("y") - step) * order + lax.axis_index("x") * matrix.shape[1]
    for core in range(2):
        high, low = halves(solved[core])
        solved_high[core * rows : (core + 1) * rows, :] = high
        solved_low[core * rows : (core + 1) * rows, :] = low
    piece = lambda start, q: column[q, pl.ds(start, PANEL), :]
    left_side(matrix, result, piece, row_base, col_base, order, solved_high, solved_low)


def a_update(matrix, other, strips, solved, solved_high, solved_low):
    order = STEPS_A * PANEL
    cols = matrix.shape[1]
    row_base = (lax.axis_index("z") * 2 + lax.axis_index("core")) * matrix.shape[0]
    col_base = (lax.axis_index("y") * 4 + lax.axis_index("x")) * cols
    high, low = halves(solved[...])
    solved_high[...] = high
    solved_low[...] = low

    def piece(start, q):
        among = pl.ds(pl.multiple_of(lax.rem(start, order), PANEL), PANEL)
        return strips[start // order, pl.ds(q * PANEL, PANEL), among].T

    left_side(matrix, matrix, piece, row_base, col_base, order, solved_high.at[:, :cols], solved_low.at[:, :cols])
    left_side(other, other, piece, row_base, None, order, solved_high.at[:, cols:], solved_low.at[:, cols:])


CHUNKS = 8
AHEAD = tuple(range(CHUNKS // 2))
BEHIND = tuple(range(CHUNKS // 2, CHUNKS))


def ring(index, by):
    return lax.rem(index + by, 4)


def send(source, target, sent, received, where):
    return pltpu.make_async_remote_copy(
        src_ref=source, dst_ref=target, send_sem=sent, recv_sem=received,
        device_id=where, device_id_type=pl.DeviceIdType.MESH,
    )


def greet(neighbours):
    barrier = pltpu.get_barrier_semaphore()
    for where in neighbours:
        pl.semaphore_signal(barrier, inc=1, device_id=where, device_id_type=pl.DeviceIdType.MESH)
    pl.semaphore_wait(barrier, len(neighbours))


def chunk(h, rows=512):
    return pl.ds(h * (rows // CHUNKS), rows // CHUNKS)


def both(left, right):
    return left if right is True else jnp.logical_and(left, right)


def spread(axis, step, source, landing, sent, received, follow, active=True):
    place = lax.axis_index(axis)
    apart = lax.rem(place - step + 4, 4)
    up, down = {axis: ring(place, 1)}, {axis: ring(place, 3)}

    def copy(ref, h, side):
        return send(ref.at[chunk(h)], landing.at[chunk(h)], sent.at[side, h], received.at[h], (up, down)[side])

    def begin():
        @pl.when(both(apart == 0, active))
        def _():
            for one, two in zip(AHEAD + BEHIND, BEHIND + AHEAD):
                copy(source, one, 0).start()
                copy(source, two, 1).start()
            for h in range(CHUNKS):
                follow(h, source)

    def relay():
        def take(order, onward, side):
            for h in order:
                copy(landing, h, 0).wait_recv()
                if h in onward:
                    copy(landing, h, side).start()
                follow(h, landing)

        @pl.when(both(apart == 1, active))
        def _():
            take(AHEAD + BEHIND, AHEAD, 0)

        @pl.when(both(apart == 3, active))
        def _():
            take(BEHIND + AHEAD, BEHIND, 1)

        @pl.when(both(apart == 2, active))
        def _():
            take([h for two in zip(AHEAD, BEHIND) for h in two], (), 0)

    def finish():
        @pl.when(both(apart == 0, active))
        def _():
            for h in range(CHUNKS):
                copy(source, h, 0).wait_send()
                copy(source, h, 1).wait_send()

        @pl.when(both(apart == 1, active))
        def _():
            for h in AHEAD:
                copy(landing, h, 0).wait_send()

        @pl.when(both(apart == 3, active))
        def _():
            for h in BEHIND:
                copy(landing, h, 1).wait_send()

    return apart, begin, relay, finish


def nothing(h, ref):
    pass


def gather(step, matrix, column, other, mate, y_sent, y_got, x_sent, x_got, far_sent, far_got, core_sent, core_got):
    x = lax.axis_index("x")
    core = lax.axis_index("core")
    right, left, far = ring(x, 1), ring(x, 3), ring(x, 2)
    partner = {"core": 1 - core}
    centered = lax.axis_index("z") == step
    swap = send(matrix, mate, core_sent.at[2], core_got.at[2], partner)

    def sideways(h, ref):
        return [
            send(ref.at[chunk(h)], column.at[x, chunk(h)], x_sent.at[0, h], x_got.at[0, h], {"x": right}),
            send(ref.at[chunk(h)], column.at[x, chunk(h)], x_sent.at[1, h], x_got.at[1, h], {"x": left}),
        ]

    def follow(h, ref):
        for copy in sideways(h, ref):
            copy.start()

    apart, begin, relay, finish = spread("y", step, matrix, column.at[x], y_sent, y_got, follow)

    def start():
        begin()

        @pl.when(centered)
        def _():
            swap.start()

    def give(place, ref):
        slot = lax.rem(place, 2)
        return send(ref, other.at[slot], core_sent.at[slot], core_got.at[slot], partner)

    def maybe_give(place, ref, also=True):
        @pl.when(both(jnp.logical_and(centered, place // 2 == core), also))
        def _():
            give(place, ref).start()

    def arrive(place, h, received):
        ref = column.at[place, chunk(h)]
        send(ref, ref, x_sent.at[0, h], received, {"x": right}).wait_recv()

    def pass_on(h):
        place, where = (left, right) if h in AHEAD else (right, left)
        ref = column.at[place, chunk(h)]
        return send(ref, ref, far_sent.at[h], far_got.at[h], {"x": where})

    def middle():
        relay()
        maybe_give(x, matrix, apart == 0)
        maybe_give(x, column.at[x], apart != 0)

        @pl.when(apart == 0)
        def _():
            column[x] = matrix[...]

        for one, two in zip(AHEAD, BEHIND):
            arrive(left, one, x_got.at[0, one])
            pass_on(one).start()
            arrive(right, two, x_got.at[1, two])
            pass_on(two).start()
        for one, two in zip(AHEAD, BEHIND):
            arrive(right, one, x_got.at[1, one])
            arrive(left, two, x_got.at[0, two])
        maybe_give(left, column.at[left])
        maybe_give(right, column.at[right])
        for h in range(CHUNKS):
            arrive(far, h, far_got.at[h])
        maybe_give(far, column.at[far])

    def end():
        finish()
        for h in range(CHUNKS):
            for copy in sideways(h, matrix):
                copy.wait_send()
            pass_on(h).wait_send()

        @pl.when(centered)
        def _():
            swap.wait()
            give(0, matrix).wait()
            give(1, matrix).wait()

    return start, middle, end


def share(step, half, solved, z_sent, z_got, core_sent, core_got):
    core = lax.axis_index("core")
    partner = {"core": 1 - core}

    def give(h, ref):
        return send(ref.at[chunk(h)], solved.at[core, chunk(h)], core_sent.at[h], core_got.at[h], partner)

    def follow(h, ref):
        give(h, ref).start()

    apart, begin, relay, finish = spread("z", step, half, solved.at[core], z_sent, z_got, follow)

    def end():
        @pl.when(apart == 0)
        def _():
            solved[core] = half[...]

        finish()
        for h in range(CHUNKS):
            give(h, half).wait_send()
            ref = solved.at[1 - core, chunk(h)]
            send(ref, ref, core_sent.at[h], core_got.at[h], partner).wait_recv()

    return begin, relay, end


def peers():
    z, core, y, x = (lax.axis_index(axis) for axis in AXES)
    line, plane = z * 2 + core, y * 4 + x
    along, among = [], []
    for by in range(1, 8):
        place = lax.rem(line + by, 8)
        along.append({"z": place // 2, "core": lax.rem(place, 2)})
    for by in range(1, 16):
        place = lax.rem(plane + by, 16)
        among.append({"y": place // 4, "x": lax.rem(place, 4)})
    return along, among


def exchange(value, slots, sent, received, partners):
    copies = [send(value, slots.at[at], sent.at[at], received.at[at], where) for at, where in enumerate(partners)]
    for copy in copies:
        copy.start()
    for copy in copies:
        copy.wait()
    result = value[...]
    for at in range(len(partners)):
        result = result + slots[at]
    return result


def squares(value):
    return jnp.sum(jnp.sum(value * value, axis=0, keepdims=True), axis=1, keepdims=True)


def whole_kernel(a_hbm, b_hbm, c_hbm, a_out, c_out, b_out, *spaces):
    s = dict(zip(SPACES, spaces))
    z, core, y, x = (lax.axis_index(axis) for axis in AXES)
    a, b, c = s["a"], s["matrix"].at[0], s["c"]
    a_order = STEPS_A * PANEL
    a_top, c_top = a.at[:a_order], c.at[:a_order]
    loads = [pltpu.make_async_copy(held, to, s["load"].at[at]) for at, (held, to) in enumerate([(b_hbm, b), (a_hbm, a), (c_hbm, c)])]
    stores = [pltpu.make_async_copy(a, a_out, s["load"].at[1]), pltpu.make_async_copy(c, c_out, s["load"].at[2])]
    for copy in loads:
        copy.start()
    along, among = peers()
    greet(along + among)
    loads[0].wait()

    home = jnp.logical_and(z == 0, core == 0)
    holds = core == x // 2
    goal = jnp.logical_and(z == y, holds)
    stays = jnp.logical_and(home, goal)
    goes = jnp.logical_and(home, jnp.logical_not(goal))
    comes = jnp.logical_and(goal, jnp.logical_not(home))
    seeding = send(a_top, s["seed"], s["seed_sent"], s["seed_got"], {"z": y, "core": x // 2})
    partner = {"core": 1 - core}

    def a_give(h, ref):
        return send(ref.at[chunk(h)], s["a_shared"].at[chunk(h)], s["a_pass_sent"].at[h], s["a_pass_got"].at[h], partner)

    def a_follow(h, ref):
        a_give(h, ref).start()

    def along_y(source, active):
        return spread("y", z, source, s["strip"], s["ay_sent"], s["ay_got"], nothing, active)

    def along_x(active):
        return [
            spread("x", 2 * core + at, s["strip"], s["strips"].at[at], s["ax_sent"].at[at], s["ax_got"].at[at], nothing, active)
            for at in range(2)
        ]

    a_share = spread("z", 0, s["a_solved"], s["a_shared"], s["az_sent"], s["az_got"], a_follow, core == 0)

    def finish_a():
        a_update(a, c, s["strips"], s["a_shared"], s["a_solved_high"], s["a_solved_low"])
        for copy in stores:
            copy.start()

    def both_of(*conditions):
        return functools.reduce(jnp.logical_and, conditions)

    @pl.loop(0, STEPS_B // JOINED)
    def _(step):
        first, second, third, last = (step == at for at in range(4))
        matrix = s["matrix"].at[step]
        column, other, mate, half, solved = (s[name].at[step] for name in ("column", "other", "mate", "half", "solved"))
        here, away = z == step, z != step
        start, middle, end = gather(step, matrix, column, other, mate, *(s[name].at[step] for name in GATHER_FLAGS))
        start()

        @pl.when(first)
        def _():
            loads[1].wait()
            loads[2].wait()
            pl.when(goes)(seeding.start)

        middle()

        @pl.when(last)
        def _():
            a_share[2]()

        end()

        @pl.when(first)
        def _():
            pl.when(goes)(seeding.wait_send)
            pl.when(comes)(seeding.wait_recv)
            along_y(s["seed"], both_of(holds, jnp.logical_not(stays)))[1]()
            along_y(a_top, stays)[1]()

        @pl.when(second)
        def _():
            for one in along_x(True):
                one[1]()

        @pl.when(here)
        def _():
            center(step, column, other, matrix, mate, half, *(s[name] for name in CENTER_SPACES))

        @pl.when(both_of(first, away))
        def _():
            along_y(s["seed"], holds)[2]()

        @pl.when(both_of(second, away))
        def _():
            for one in along_x(True):
                one[2]()

        @pl.when(both_of(third, home))
        def _():
            a_center(s["strips"], a_top, c_top, s["a_solved"], *(s[name] for name in A_CENTER_SPACES))

        @pl.when(last)
        def _():
            @pl.when(home)
            def _():
                s["a_shared"][...] = s["a_solved"][...]

            @pl.when(core == 1)
            def _():
                for h in range(CHUNKS):
                    a_give(h, s["a_solved"]).wait_recv()

        begin, relay, close = share(step, half, solved, *(s[name].at[step] for name in SHARE_FLAGS))
        begin()
        pl.when(last)(finish_a)
        relay()

        @pl.when(first)
        def _():
            @pl.when(here)
            def _():
                along_y(s["seed"], holds)[2]()

            @pl.when(stays)
            def _():
                s["strip"][...] = a_top[...]

            @pl.when(comes)
            def _():
                s["strip"][...] = s["seed"][...]

            along_y(s["seed"], holds)[3]()

        @pl.when(second)
        def _():
            @pl.when(here)
            def _():
                for one in along_x(True):
                    one[2]()

            for at, one in enumerate(along_x(True)):

                @pl.when(one[0] == 0)
                def _():
                    s["strips"][at] = s["strip"][...]

                one[3]()

        close()
        update(step, matrix, column, solved, s["matrix"].at[step + 1], s["solved_high"], s["solved_low"])

        @pl.when(third)
        def _():
            a_share[1]()

    matrix = s["matrix"].at[STEPS_B // JOINED]
    lane = lax.broadcasted_iota(jnp.int32, (8, 128), 1)
    s["partial"][0] = jnp.where(lane == 0, squares(b[...]), squares(matrix[...]))
    s["partial"][1] = exchange(s["partial"].at[0], s["line"], s["line_sent"], s["line_got"], along)
    total = exchange(s["partial"].at[1], s["plane"], s["plane_sent"], s["plane_got"], among)
    scale = jnp.sqrt(jnp.sqrt(total[0:1, 1:2] / total[0:1, 0:1]))
    b_out[...] = 0.5 * (scale * b[...] + matrix[...] / scale)
    a_share[3]()

    @pl.when(core == 0)
    def _():
        for h in range(CHUNKS):
            a_give(h, s["a_solved"]).wait_send()

    for copy in stores:
        copy.wait()


GATHER_FLAGS = ("y_sent", "y_got", "x_sent", "x_got", "far_sent", "far_got", "core_sent", "core_got")
CENTER_SPACES = ("table", "fresh", "fresh_high", "fresh_low", "inverse_of", "right_high", "right_low")
A_CENTER_SPACES = ("a_table", "a_fresh", "a_fresh_high", "a_fresh_low", "inverse_of", "a_right_high", "a_right_low")
SHARE_FLAGS = ("z_sent", "z_got", "pass_sent", "pass_got")


def flags(*shape):
    return pltpu.SemaphoreType.DMA(shape)


def spaces_of(a_shape, b_shape, c_shape):
    steps = STEPS_B // JOINED
    order, a_order = JOINED * PANEL, STEPS_A * PANEL
    rows, cols = b_shape
    wide = a_shape[1] + c_shape[1]
    top = (a_order, a_shape[1])
    full = lambda *shape: pltpu.VMEM(shape, F32)
    short = lambda *shape: pltpu.VMEM(shape, BF16)
    ringed = (2, CHUNKS)
    return dict(
        a=full(*a_shape), c=full(*c_shape), load=flags(3), inverse_of=full(PANEL, PANEL),
        column=full(steps, 4, rows, cols), other=full(steps, 2, rows, cols), mate=full(steps, rows, cols),
        half=full(steps, rows, cols), solved=full(steps, 2, rows, cols), matrix=full(steps + 1, rows, cols),
        table=full(order, order), fresh=full(PANEL, order), fresh_high=short(PANEL, order), fresh_low=short(PANEL, order),
        right_high=short(order, cols), right_low=short(order, cols), solved_high=short(order, cols), solved_low=short(order, cols),
        seed=full(*top), strip=full(*top), strips=full(2, *top), a_solved=full(a_order, wide), a_shared=full(a_order, wide),
        a_table=full(a_order, a_order), a_fresh=full(PANEL, a_order), a_fresh_high=short(PANEL, a_order), a_fresh_low=short(PANEL, a_order),
        a_right_high=short(a_order, wide), a_right_low=short(a_order, wide), a_solved_high=short(a_order, wide), a_solved_low=short(a_order, wide),
        partial=full(2, 8, 128), line=full(7, 8, 128), plane=full(15, 8, 128),
        y_sent=flags(steps, *ringed), y_got=flags(steps, CHUNKS), x_sent=flags(steps, *ringed), x_got=flags(steps, *ringed),
        far_sent=flags(steps, CHUNKS), far_got=flags(steps, CHUNKS), core_sent=flags(steps, 3), core_got=flags(steps, 3),
        z_sent=flags(steps, *ringed), z_got=flags(steps, CHUNKS), pass_sent=flags(steps, CHUNKS), pass_got=flags(steps, CHUNKS),
        seed_sent=pltpu.SemaphoreType.DMA, seed_got=pltpu.SemaphoreType.DMA,
        ay_sent=flags(*ringed), ay_got=flags(CHUNKS), ax_sent=flags(2, *ringed), ax_got=flags(2, CHUNKS),
        az_sent=flags(*ringed), az_got=flags(CHUNKS), a_pass_sent=flags(CHUNKS), a_pass_got=flags(CHUNKS),
        line_sent=flags(7), line_got=flags(7), plane_sent=flags(15), plane_got=flags(15),
    )


SPACES = tuple(spaces_of((1, 1), (1, 1), (1, 1)))


def body(a_matrix, b_matrix, c_matrix):
    held = pl.BlockSpec(memory_space=pltpu.VMEM)
    left = pl.BlockSpec(memory_space=pl.ANY)
    shapes = (a_matrix.shape, b_matrix.shape, c_matrix.shape)
    a_swept, c_swept, b_next = pl.pallas_call(
        whole_kernel,
        out_shape=[jax.ShapeDtypeStruct(shapes[at], F32) for at in (0, 2, 1)],
        in_specs=[left, left, left],
        out_specs=[left, left, held],
        scratch_shapes=list(spaces_of(*shapes).values()),
        compiler_params=pltpu.CompilerParams(vmem_limit_bytes=63 * 1024 * 1024, collective_id=0, has_side_effects=True),
    )(a_matrix, b_matrix, c_matrix)
    return (a_swept, c_swept, b_next)


def solution(mesh):
    finer = Mesh(mesh.devices.reshape(4, 2, 4, 4), AXES)
    placed = (P(ROW, COL), P(ROW, COL), P(ROW, COL))
    return jax.shard_map(body, mesh=finer, in_specs=placed, out_specs=placed, check_vma=False)
```

```python
import functools

import jax
import jax.numpy as jnp
from jax import lax
from jax.experimental import pallas as pl
from jax.experimental.pallas import tpu as pltpu
from jax.sharding import Mesh
from jax.sharding import PartitionSpec as P

PANEL = 256
SQUARINGS = 5
STEPS_A = 2
STEPS_B = 16
JOINED = 4
AXES = ("z", "core", "y", "x")
ROW = ("z", "core")
COL = ("y", "x")
F32 = jnp.float32
BF16 = jnp.bfloat16


def halves(value):
    high = value.astype(BF16)
    return high, (value - high.astype(F32)).astype(BF16)


def product(left, right):
    return jnp.dot(left, right, preferred_element_type=F32)


def summed(high, low, right_high, right_low):
    return product(high, right_high) + product(high, right_low) + product(low, right_high)


def triple(left, right_high, right_low):
    return summed(*halves(left), right_high, right_low)


def by_rows(high, low, right_high, right_low):
    cut = high.shape[0] // 2
    parts = [summed(high[at], low[at], right_high, right_low) for at in (slice(None, cut), slice(cut, None))]
    return jnp.concatenate(parts, 0)


def pivot_inverse(pivot, between=()):
    parts = iter(between)

    def fill():
        for part in next(parts, ()):
            part()

    shape = (PANEL, PANEL)
    unit = lax.broadcasted_iota(jnp.int32, shape, 0) == lax.broadcasted_iota(jnp.int32, shape, 1)
    diagonal = jnp.where(unit, pivot, 0.0)
    down = 1.0 / jnp.sqrt(jnp.sum(diagonal, axis=1, keepdims=True))
    across = 1.0 / jnp.sqrt(jnp.sum(diagonal, axis=0, keepdims=True))
    scaled = pivot * down * across
    ceiling = jnp.max(jnp.sum(jnp.abs(scaled), axis=0, keepdims=True), axis=1, keepdims=True)
    eye = jnp.where(unit, 1.0, 0.0)
    power = eye - scaled / ceiling
    fill()
    total = eye + power
    high, low = halves(power)
    power = by_rows(high, low, high, low)
    fill()
    for turn in range(SQUARINGS - 1):
        high, low = halves(power)
        total_high, total_low = halves(total)
        pair = summed(high, low, jnp.concatenate([high, total_high], 1), jnp.concatenate([low, total_low], 1))
        fill()
        power = pair[:, :PANEL]
        total = total + pair[:, PANEL:]
    total = total + by_rows(*halves(total), *halves(power))
    return total / ceiling * down * across


def composite(count, table, fresh, fresh_high, fresh_low, inverse_of):
    inverse_of[...] = pivot_inverse(table[:PANEL, :PANEL])

    def panel(p, more):
        here = pl.ds(pl.multiple_of(p * PANEL, PANEL), PANEL)
        others = [pl.ds(pl.multiple_of(lax.rem(p + by, count) * PANEL, PANEL), PANEL) for by in range(1, count)]
        inverse = inverse_of[...]
        inverse_high, inverse_low = halves(inverse)
        high, low = halves(jnp.concatenate([table[there, here] for there in others], 0))

        def row():
            fresh[...] = summed(inverse_high, inverse_low, *halves(table[here, :]))
            fresh[:, here] = inverse
            fresh_high[...], fresh_low[...] = halves(fresh[...])
            for there in others:
                table[there, here] = jnp.zeros((PANEL, PANEL), F32)

        def rest(at):
            cols = slice(at * PANEL, (at + 1) * PANEL)
            taken = summed(high, low, fresh_high[:, cols], fresh_low[:, cols])
            for nth, there in enumerate(others):
                table[there, cols] = table[there, cols] - taken[nth * PANEL : (nth + 1) * PANEL]

        parts = [row] + [functools.partial(rest, at) for at in range(count)]
        if more:
            after = others[0]
            solved = by_rows(inverse_high, inverse_low, *halves(table[here, after]))
            block = table[after, after] - by_rows(high[:PANEL], low[:PANEL], *halves(solved))
            inverse_of[...] = pivot_inverse(block, [(part,) for part in parts])
        else:
            for part in parts:
                part()
        table[here, :] = fresh[...]

    @pl.loop(0, count - 1)
    def _(p):
        panel(p, True)

    panel(count - 1, False)


def left_side(matrix, result, piece, row_base, col_base, order, solved_high, solved_low):
    rows, cols = matrix.shape

    @pl.loop(0, rows // PANEL)
    def _(r):
        start = pl.multiple_of(r * PANEL, PANEL)
        there = pl.ds(start, PANEL)
        down = row_base + start + lax.broadcasted_iota(jnp.int32, (PANEL, PANEL), 0)
        total = None
        for q in range(order // PANEL):
            unit = down == q * PANEL + lax.broadcasted_iota(jnp.int32, (PANEL, PANEL), 1)
            column = piece(start, q) - jnp.where(unit, 1.0, 0.0)
            among = pl.ds(q * PANEL, PANEL)
            part = triple(column, solved_high[among, :cols], solved_low[among, :cols])
            total = part if total is None else total + part
        base = matrix[there, :]
        if col_base is not None:
            inside = jnp.logical_and(col_base >= 0, col_base < order)
            across = col_base + lax.broadcasted_iota(jnp.int32, (PANEL, cols), 1)
            begin = row_base + start + lax.broadcasted_iota(jnp.int32, (PANEL, cols), 0)
            base = jnp.where(inside, jnp.where(begin == across, 1.0, 0.0), base)
        result[there, :] = base - total


def center(step, mine, other, matrix, mate, half, table, fresh, fresh_high, fresh_low, inverse_of, right_high, right_low):
    core = lax.axis_index("core")
    rows = matrix.shape[0]
    order = JOINED * PANEL
    base = (lax.axis_index("y") - step) * order + lax.axis_index("x") * matrix.shape[1]
    pair = (pl.ds(0, rows), pl.ds(rows, rows))
    for at in range(2):

        @pl.when(core == at)
        def _():
            for q in range(JOINED):
                table[pair[at], q * PANEL : (q + 1) * PANEL] = mine[q]
            for q in range(2):
                across = 2 * (1 - at) + q
                table[pair[1 - at], across * PANEL : (across + 1) * PANEL] = other[q]
                table[across * PANEL : (across + 1) * PANEL, pair[at]] = mine[across].T

    composite(JOINED, table, fresh, fresh_high, fresh_low, inverse_of)
    inside = jnp.logical_and(base >= 0, base < order)
    for first, source in ((core * rows, matrix), ((1 - core) * rows, mate)):
        shape = source.shape
        unit = first + lax.broadcasted_iota(jnp.int32, shape, 0) == base + lax.broadcasted_iota(jnp.int32, shape, 1)
        high, low = halves(jnp.where(inside, jnp.where(unit, 1.0, 0.0), source[...]))
        there = pl.ds(pl.multiple_of(first, rows), rows)
        right_high[there, :] = high
        right_low[there, :] = low
    for q in range(rows // PANEL):
        there = pl.ds(pl.multiple_of(core * rows + q * PANEL, PANEL), PANEL)
        half[q * PANEL : (q + 1) * PANEL, :] = triple(table[there, :], right_high[...], right_low[...])


def a_center(strips, a_top, c_top, solved, table, fresh, fresh_high, fresh_low, inverse_of, right_high, right_low):
    order, cols = a_top.shape
    table[...] = strips[0]
    composite(STEPS_A, table, fresh, fresh_high, fresh_low, inverse_of)
    base = (lax.axis_index("y") * 4 + lax.axis_index("x")) * cols
    unit = lax.broadcasted_iota(jnp.int32, (order, cols), 0) == base + lax.broadcasted_iota(jnp.int32, (order, cols), 1)
    high, low = halves(jnp.where(base < order, jnp.where(unit, 1.0, 0.0), a_top[...]))
    right_high[:, :cols] = high
    right_low[:, :cols] = low
    high, low = halves(c_top[...])
    right_high[:, cols:] = high
    right_low[:, cols:] = low
    for q in range(STEPS_A):
        there = slice(q * PANEL, (q + 1) * PANEL)
        solved[there, :] = triple(table[there, :], right_high[...], right_low[...])


def update(step, matrix, column, solved, result, solved_high, solved_low):
    order = JOINED * PANEL
    rows = matrix.shape[0]
    row_base = (lax.axis_index("z") - step) * order + lax.axis_index("core") * rows
    col_base = (lax.axis_index("y") - step) * order + lax.axis_index("x") * matrix.shape[1]
    for core in range(2):
        high, low = halves(solved[core])
        solved_high[core * rows : (core + 1) * rows, :] = high
        solved_low[core * rows : (core + 1) * rows, :] = low
    piece = lambda start, q: column[q, pl.ds(start, PANEL), :]
    left_side(matrix, result, piece, row_base, col_base, order, solved_high, solved_low)


def a_update(matrix, other, strips, solved, solved_high, solved_low):
    order = STEPS_A * PANEL
    cols = matrix.shape[1]
    row_base = (lax.axis_index("z") * 2 + lax.axis_index("core")) * matrix.shape[0]
    col_base = (lax.axis_index("y") * 4 + lax.axis_index("x")) * cols
    high, low = halves(solved[...])
    solved_high[...] = high
    solved_low[...] = low

    def piece(start, q):
        among = pl.ds(pl.multiple_of(lax.rem(start, order), PANEL), PANEL)
        return strips[start // order, pl.ds(q * PANEL, PANEL), among].T

    left_side(matrix, matrix, piece, row_base, col_base, order, solved_high.at[:, :cols], solved_low.at[:, :cols])
    left_side(other, other, piece, row_base, None, order, solved_high.at[:, cols:], solved_low.at[:, cols:])


CHUNKS = 8
AHEAD = tuple(range(CHUNKS // 2))
BEHIND = tuple(range(CHUNKS // 2, CHUNKS))


def ring(index, by):
    return lax.rem(index + by, 4)


def send(source, target, sent, received, where):
    return pltpu.make_async_remote_copy(
        src_ref=source, dst_ref=target, send_sem=sent, recv_sem=received,
        device_id=where, device_id_type=pl.DeviceIdType.MESH,
    )


def greet(neighbours):
    barrier = pltpu.get_barrier_semaphore()
    for where in neighbours:
        pl.semaphore_signal(barrier, inc=1, device_id=where, device_id_type=pl.DeviceIdType.MESH)
    pl.semaphore_wait(barrier, len(neighbours))


def chunk(h, rows=512):
    return pl.ds(h * (rows // CHUNKS), rows // CHUNKS)


def both(left, right):
    return left if right is True else jnp.logical_and(left, right)


def spread(axis, step, source, landing, sent, received, follow, active=True, around=()):
    place = lax.axis_index(axis)
    apart = lax.rem(place - step + 4, 4)
    up, down = {axis: ring(place, 1)}, {axis: ring(place, 3)}

    def copy(ref, h, side):
        return send(ref.at[chunk(h)], landing.at[chunk(h)], sent.at[side, h], received.at[h], (up, down)[side])

    def begin():
        @pl.when(both(apart == 0, active))
        def _():
            for one, two in zip(AHEAD + BEHIND, BEHIND + AHEAD):
                if one not in around:
                    copy(source, one, 0).start()
                copy(source, two, 1).start()
            for h in range(CHUNKS):
                follow(h, source)

    def relay():
        def take(order, onward, side):
            for h in order:
                copy(landing, h, 0).wait_recv()
                if h in onward:
                    copy(landing, h, side).start()
                follow(h, landing)

        @pl.when(both(apart == 1, active))
        def _():
            take([h for h in AHEAD + BEHIND if h not in around] + list(around), AHEAD, 0)

        @pl.when(both(apart == 3, active))
        def _():
            take(BEHIND + AHEAD, BEHIND, 1)

        @pl.when(both(apart == 2, active))
        def _():
            take([h for two in zip(AHEAD, BEHIND) for h in two], around, 1)

    def finish():
        @pl.when(both(apart == 0, active))
        def _():
            for h in range(CHUNKS):
                if h not in around:
                    copy(source, h, 0).wait_send()
                copy(source, h, 1).wait_send()

        @pl.when(both(apart == 1, active))
        def _():
            for h in AHEAD:
                copy(landing, h, 0).wait_send()

        @pl.when(both(apart == 3, active))
        def _():
            for h in BEHIND:
                copy(landing, h, 1).wait_send()

        if around:

            @pl.when(both(apart == 2, active))
            def _():
                for h in around:
                    copy(landing, h, 1).wait_send()

    return apart, begin, relay, finish


def nothing(h, ref):
    pass


def gather(step, matrix, column, other, mate, y_sent, y_got, x_sent, x_got, far_sent, far_got, core_sent, core_got):
    x = lax.axis_index("x")
    core = lax.axis_index("core")
    right, left, far = ring(x, 1), ring(x, 3), ring(x, 2)
    partner = {"core": 1 - core}
    centered = lax.axis_index("z") == step
    swap = send(matrix, mate, core_sent.at[2], core_got.at[2], partner)

    def sideways(h, ref):
        return [
            send(ref.at[chunk(h)], column.at[x, chunk(h)], x_sent.at[0, h], x_got.at[0, h], {"x": right}),
            send(ref.at[chunk(h)], column.at[x, chunk(h)], x_sent.at[1, h], x_got.at[1, h], {"x": left}),
        ]

    def follow(h, ref):
        for copy in sideways(h, ref):
            copy.start()

    apart, begin, relay, finish = spread("y", step, matrix, column.at[x], y_sent, y_got, follow)

    def start():
        begin()

        @pl.when(centered)
        def _():
            swap.start()

    def give(place, ref):
        slot = lax.rem(place, 2)
        return send(ref, other.at[slot], core_sent.at[slot], core_got.at[slot], partner)

    def maybe_give(place, ref, also=True):
        @pl.when(both(jnp.logical_and(centered, place // 2 == core), also))
        def _():
            give(place, ref).start()

    def arrive(place, h, received):
        ref = column.at[place, chunk(h)]
        send(ref, ref, x_sent.at[0, h], received, {"x": right}).wait_recv()

    def pass_on(h):
        place, where = (left, right) if h in AHEAD else (right, left)
        ref = column.at[place, chunk(h)]
        return send(ref, ref, far_sent.at[h], far_got.at[h], {"x": where})

    def middle():
        relay()
        maybe_give(x, matrix, apart == 0)
        maybe_give(x, column.at[x], apart != 0)

        @pl.when(apart == 0)
        def _():
            column[x] = matrix[...]

        for one, two in zip(AHEAD, BEHIND):
            arrive(left, one, x_got.at[0, one])
            pass_on(one).start()
            arrive(right, two, x_got.at[1, two])
            pass_on(two).start()
        for one, two in zip(AHEAD, BEHIND):
            arrive(right, one, x_got.at[1, one])
            arrive(left, two, x_got.at[0, two])
        maybe_give(left, column.at[left])
        maybe_give(right, column.at[right])
        for h in range(CHUNKS):
            arrive(far, h, far_got.at[h])
        maybe_give(far, column.at[far])

    def end():
        @pl.when(centered)
        def _():
            swap.wait_recv()
            give(0, matrix).wait_recv()
            give(1, matrix).wait_recv()

    def drain():
        finish()
        for h in range(CHUNKS):
            for copy in sideways(h, matrix):
                copy.wait_send()
            pass_on(h).wait_send()

        @pl.when(centered)
        def _():
            swap.wait_send()
            give(0, matrix).wait_send()
            give(1, matrix).wait_send()

    return start, middle, end, drain


def share(step, half, solved, z_sent, z_got, core_sent, core_got):
    core = lax.axis_index("core")
    partner = {"core": 1 - core}

    def give(h, ref):
        return send(ref.at[chunk(h)], solved.at[core, chunk(h)], core_sent.at[h], core_got.at[h], partner)

    def follow(h, ref):
        give(h, ref).start()

    apart, begin, relay, finish = spread("z", step, half, solved.at[core], z_sent, z_got, follow, around=BEHIND[:2])

    def end():
        @pl.when(apart == 0)
        def _():
            solved[core] = half[...]

        for h in range(CHUNKS):
            ref = solved.at[1 - core, chunk(h)]
            send(ref, ref, core_sent.at[h], core_got.at[h], partner).wait_recv()

    def drain():
        finish()
        for h in range(CHUNKS):
            give(h, half).wait_send()

    return begin, relay, end, drain


def peers():
    z, core, y, x = (lax.axis_index(axis) for axis in AXES)
    line, plane = z * 2 + core, y * 4 + x
    along, among = [], []
    for by in range(1, 8):
        place = lax.rem(line + by, 8)
        along.append({"z": place // 2, "core": lax.rem(place, 2)})
    for by in range(1, 16):
        place = lax.rem(plane + by, 16)
        among.append({"y": place // 4, "x": lax.rem(place, 4)})
    return along, among


def exchange(value, slots, sent, received, partners):
    copies = [send(value, slots.at[at], sent.at[at], received.at[at], where) for at, where in enumerate(partners)]
    for copy in copies:
        copy.start()
    for copy in copies:
        copy.wait()
    result = value[...]
    for at in range(len(partners)):
        result = result + slots[at]
    return result


def squares(value):
    return jnp.sum(jnp.sum(value * value, axis=0, keepdims=True), axis=1, keepdims=True)


def whole_kernel(a_hbm, b_hbm, c_hbm, a_out, c_out, b_out, *spaces):
    s = dict(zip(SPACES, spaces))
    z, core, y, x = (lax.axis_index(axis) for axis in AXES)
    a, b, c = s["a"], s["matrix"].at[0], s["c"]
    a_order = STEPS_A * PANEL
    a_top, c_top = a.at[:a_order], c.at[:a_order]
    loads = [pltpu.make_async_copy(held, to, s["load"].at[at]) for at, (held, to) in enumerate([(b_hbm, b), (a_hbm, a), (c_hbm, c)])]
    stores = [pltpu.make_async_copy(a, a_out, s["load"].at[1]), pltpu.make_async_copy(c, c_out, s["load"].at[2])]
    for copy in loads:
        copy.start()
    along, among = peers()
    greet(along + among)
    loads[0].wait()

    home = jnp.logical_and(z == 0, core == 0)
    holds = core == x // 2
    goal = jnp.logical_and(z == y, holds)
    stays = jnp.logical_and(home, goal)
    goes = jnp.logical_and(home, jnp.logical_not(goal))
    comes = jnp.logical_and(goal, jnp.logical_not(home))
    seeding = send(a_top, s["seed"], s["seed_sent"], s["seed_got"], {"z": y, "core": x // 2})
    partner = {"core": 1 - core}

    def a_give(h, ref):
        return send(ref.at[chunk(h)], s["a_shared"].at[chunk(h)], s["a_pass_sent"].at[h], s["a_pass_got"].at[h], partner)

    def a_follow(h, ref):
        a_give(h, ref).start()

    def along_y(source, active):
        return spread("y", z, source, s["strip"], s["ay_sent"], s["ay_got"], nothing, active)

    def along_x(active):
        return [
            spread("x", 2 * core + at, s["strip"], s["strips"].at[at], s["ax_sent"].at[at], s["ax_got"].at[at], nothing, active)
            for at in range(2)
        ]

    a_share = spread("z", 0, s["a_solved"], s["a_shared"], s["az_sent"], s["az_got"], a_follow, core == 0)

    def finish_a():
        a_update(a, c, s["strips"], s["a_shared"], s["a_solved_high"], s["a_solved_low"])
        for copy in stores:
            copy.start()

    def both_of(*conditions):
        return functools.reduce(jnp.logical_and, conditions)

    @pl.loop(0, STEPS_B // JOINED)
    def _(step):
        first, second, third, last = (step == at for at in range(4))
        matrix = s["matrix"].at[step]
        column, other, mate, half, solved = (s[name].at[step] for name in ("column", "other", "mate", "half", "solved"))
        here, away = z == step, z != step
        start, middle, end, gathered = gather(step, matrix, column, other, mate, *(s[name].at[step] for name in GATHER_FLAGS))
        start()

        @pl.when(first)
        def _():
            loads[1].wait()
            loads[2].wait()
            pl.when(goes)(seeding.start)

        middle()

        @pl.when(last)
        def _():
            a_share[2]()

        end()

        @pl.when(first)
        def _():
            pl.when(goes)(seeding.wait_send)
            pl.when(comes)(seeding.wait_recv)
            along_y(s["seed"], both_of(holds, jnp.logical_not(stays)))[1]()
            along_y(a_top, stays)[1]()

        @pl.when(second)
        def _():
            for one in along_x(True):
                one[1]()

        @pl.when(here)
        def _():
            center(step, column, other, matrix, mate, half, *(s[name] for name in CENTER_SPACES))

        @pl.when(both_of(first, away))
        def _():
            along_y(s["seed"], holds)[2]()

        @pl.when(both_of(second, away))
        def _():
            for one in along_x(True):
                one[2]()

        @pl.when(both_of(third, home))
        def _():
            a_center(s["strips"], a_top, c_top, s["a_solved"], *(s[name] for name in A_CENTER_SPACES))

        @pl.when(last)
        def _():
            @pl.when(home)
            def _():
                s["a_shared"][...] = s["a_solved"][...]

            @pl.when(core == 1)
            def _():
                for h in range(CHUNKS):
                    a_give(h, s["a_solved"]).wait_recv()

        begin, relay, close, shared = share(step, half, solved, *(s[name].at[step] for name in SHARE_FLAGS))
        begin()
        pl.when(last)(finish_a)
        relay()

        @pl.when(first)
        def _():
            @pl.when(here)
            def _():
                along_y(s["seed"], holds)[2]()

            @pl.when(stays)
            def _():
                s["strip"][...] = a_top[...]

            @pl.when(comes)
            def _():
                s["strip"][...] = s["seed"][...]

        @pl.when(second)
        def _():
            @pl.when(here)
            def _():
                for one in along_x(True):
                    one[2]()

            for at, one in enumerate(along_x(True)):

                @pl.when(one[0] == 0)
                def _():
                    s["strips"][at] = s["strip"][...]

        close()
        update(step, matrix, column, solved, s["matrix"].at[step + 1], s["solved_high"], s["solved_low"])
        gathered()
        shared()

        @pl.when(first)
        def _():
            along_y(s["seed"], holds)[3]()

        @pl.when(second)
        def _():
            for one in along_x(True):
                one[3]()

        @pl.when(third)
        def _():
            a_share[1]()

    matrix = s["matrix"].at[STEPS_B // JOINED]
    lane = lax.broadcasted_iota(jnp.int32, (8, 128), 1)
    s["partial"][0] = jnp.where(lane == 0, squares(b[...]), squares(matrix[...]))
    s["partial"][1] = exchange(s["partial"].at[0], s["line"], s["line_sent"], s["line_got"], along)
    total = exchange(s["partial"].at[1], s["plane"], s["plane_sent"], s["plane_got"], among)
    scale = jnp.sqrt(jnp.sqrt(total[0:1, 1:2] / total[0:1, 0:1]))
    b_out[...] = 0.5 * (scale * b[...] + matrix[...] / scale)
    a_share[3]()

    @pl.when(core == 0)
    def _():
        for h in range(CHUNKS):
            a_give(h, s["a_solved"]).wait_send()

    for copy in stores:
        copy.wait()


GATHER_FLAGS = ("y_sent", "y_got", "x_sent", "x_got", "far_sent", "far_got", "core_sent", "core_got")
CENTER_SPACES = ("table", "fresh", "fresh_high", "fresh_low", "inverse_of", "right_high", "right_low")
A_CENTER_SPACES = ("a_table", "a_fresh", "a_fresh_high", "a_fresh_low", "inverse_of", "a_right_high", "a_right_low")
SHARE_FLAGS = ("z_sent", "z_got", "pass_sent", "pass_got")


def flags(*shape):
    return pltpu.SemaphoreType.DMA(shape)


def spaces_of(a_shape, b_shape, c_shape):
    steps = STEPS_B // JOINED
    order, a_order = JOINED * PANEL, STEPS_A * PANEL
    rows, cols = b_shape
    wide = a_shape[1] + c_shape[1]
    top = (a_order, a_shape[1])
    full = lambda *shape: pltpu.VMEM(shape, F32)
    short = lambda *shape: pltpu.VMEM(shape, BF16)
    ringed = (2, CHUNKS)
    return dict(
        a=full(*a_shape), c=full(*c_shape), load=flags(3), inverse_of=full(PANEL, PANEL),
        column=full(steps, 4, rows, cols), other=full(steps, 2, rows, cols), mate=full(steps, rows, cols),
        half=full(steps, rows, cols), solved=full(steps, 2, rows, cols), matrix=full(steps + 1, rows, cols),
        table=full(order, order), fresh=full(PANEL, order), fresh_high=short(PANEL, order), fresh_low=short(PANEL, order),
        right_high=short(order, cols), right_low=short(order, cols), solved_high=short(order, cols), solved_low=short(order, cols),
        seed=full(*top), strip=full(*top), strips=full(2, *top), a_solved=full(a_order, wide), a_shared=full(a_order, wide),
        a_table=full(a_order, a_order), a_fresh=full(PANEL, a_order), a_fresh_high=short(PANEL, a_order), a_fresh_low=short(PANEL, a_order),
        a_right_high=short(a_order, wide), a_right_low=short(a_order, wide), a_solved_high=short(a_order, wide), a_solved_low=short(a_order, wide),
        partial=full(2, 8, 128), line=full(7, 8, 128), plane=full(15, 8, 128),
        y_sent=flags(steps, *ringed), y_got=flags(steps, CHUNKS), x_sent=flags(steps, *ringed), x_got=flags(steps, *ringed),
        far_sent=flags(steps, CHUNKS), far_got=flags(steps, CHUNKS), core_sent=flags(steps, 3), core_got=flags(steps, 3),
        z_sent=flags(steps, *ringed), z_got=flags(steps, CHUNKS), pass_sent=flags(steps, CHUNKS), pass_got=flags(steps, CHUNKS),
        seed_sent=pltpu.SemaphoreType.DMA, seed_got=pltpu.SemaphoreType.DMA,
        ay_sent=flags(*ringed), ay_got=flags(CHUNKS), ax_sent=flags(2, *ringed), ax_got=flags(2, CHUNKS),
        az_sent=flags(*ringed), az_got=flags(CHUNKS), a_pass_sent=flags(CHUNKS), a_pass_got=flags(CHUNKS),
        line_sent=flags(7), line_got=flags(7), plane_sent=flags(15), plane_got=flags(15),
    )


SPACES = tuple(spaces_of((1, 1), (1, 1), (1, 1)))


def body(a_matrix, b_matrix, c_matrix):
    held = pl.BlockSpec(memory_space=pltpu.VMEM)
    left = pl.BlockSpec(memory_space=pl.ANY)
    shapes = (a_matrix.shape, b_matrix.shape, c_matrix.shape)
    a_swept, c_swept, b_next = pl.pallas_call(
        whole_kernel,
        out_shape=[jax.ShapeDtypeStruct(shapes[at], F32) for at in (0, 2, 1)],
        in_specs=[left, left, left],
        out_specs=[left, left, held],
        scratch_shapes=list(spaces_of(*shapes).values()),
        compiler_params=pltpu.CompilerParams(vmem_limit_bytes=63 * 1024 * 1024, collective_id=0, has_side_effects=True),
    )(a_matrix, b_matrix, c_matrix)
    return (a_swept, c_swept, b_next)


def solution(mesh):
    finer = Mesh(mesh.devices.reshape(4, 2, 4, 4), AXES)
    placed = (P(ROW, COL), P(ROW, COL), P(ROW, COL))
    return jax.shard_map(body, mesh=finer, in_specs=placed, out_specs=placed, check_vma=False)
```

```python
import functools

import jax
import jax.numpy as jnp
from jax import lax
from jax.experimental import pallas as pl
from jax.experimental.pallas import tpu as pltpu
from jax.sharding import Mesh
from jax.sharding import PartitionSpec as P

PANEL = 256
SQUARINGS = 5
STEPS_A = 2
STEPS_B = 16
JOINED = 4
AXES = ("z", "core", "y", "x")
ROW = ("z", "core")
COL = ("y", "x")
F32 = jnp.float32
BF16 = jnp.bfloat16


def halves(value):
    high = value.astype(BF16)
    return high, (value - high.astype(F32)).astype(BF16)


def product(left, right):
    return jnp.dot(left, right, preferred_element_type=F32)


def summed(high, low, right_high, right_low):
    return product(high, right_high) + product(high, right_low) + product(low, right_high)


def triple(left, right_high, right_low):
    return summed(*halves(left), right_high, right_low)


def by_rows(high, low, right_high, right_low):
    cut = high.shape[0] // 2
    parts = [summed(high[at], low[at], right_high, right_low) for at in (slice(None, cut), slice(cut, None))]
    return jnp.concatenate(parts, 0)


def pivot_inverse(pivot, between=()):
    parts = iter(between)

    def fill():
        for part in next(parts, ()):
            part()

    shape = (PANEL, PANEL)
    unit = lax.broadcasted_iota(jnp.int32, shape, 0) == lax.broadcasted_iota(jnp.int32, shape, 1)
    diagonal = jnp.where(unit, pivot, 0.0)
    down = 1.0 / jnp.sqrt(jnp.sum(diagonal, axis=1, keepdims=True))
    across = 1.0 / jnp.sqrt(jnp.sum(diagonal, axis=0, keepdims=True))
    scaled = pivot * down * across
    ceiling = jnp.max(jnp.sum(jnp.abs(scaled), axis=0, keepdims=True), axis=1, keepdims=True)
    eye = jnp.where(unit, 1.0, 0.0)
    power = eye - scaled / ceiling
    fill()
    total = eye + power
    high, low = halves(power)
    power = by_rows(high, low, high, low)
    fill()
    for turn in range(SQUARINGS - 1):
        high, low = halves(power)
        total_high, total_low = halves(total)
        pair = summed(high, low, jnp.concatenate([high, total_high], 1), jnp.concatenate([low, total_low], 1))
        fill()
        power = pair[:, :PANEL]
        total = total + pair[:, PANEL:]
    total = total + by_rows(*halves(total), *halves(power))
    return total / ceiling * down * across


def composite(count, table, fresh, fresh_high, fresh_low, inverse_of):
    inverse_of[...] = pivot_inverse(table[:PANEL, :PANEL])

    def panel(p, more):
        here = pl.ds(pl.multiple_of(p * PANEL, PANEL), PANEL)
        others = [pl.ds(pl.multiple_of(lax.rem(p + by, count) * PANEL, PANEL), PANEL) for by in range(1, count)]
        inverse = inverse_of[...]
        inverse_high, inverse_low = halves(inverse)
        high, low = halves(jnp.concatenate([table[there, here] for there in others], 0))

        def row():
            fresh[...] = summed(inverse_high, inverse_low, *halves(table[here, :]))
            fresh[:, here] = inverse
            fresh_high[...], fresh_low[...] = halves(fresh[...])
            for there in others:
                table[there, here] = jnp.zeros((PANEL, PANEL), F32)

        def rest(at):
            cols = slice(at * PANEL, (at + 1) * PANEL)
            taken = summed(high, low, fresh_high[:, cols], fresh_low[:, cols])
            for nth, there in enumerate(others):
                table[there, cols] = table[there, cols] - taken[nth * PANEL : (nth + 1) * PANEL]

        parts = [row] + [functools.partial(rest, at) for at in range(count)]
        if more:
            after = others[0]
            solved = by_rows(inverse_high, inverse_low, *halves(table[here, after]))
            block = table[after, after] - by_rows(high[:PANEL], low[:PANEL], *halves(solved))
            inverse_of[...] = pivot_inverse(block, [(part,) for part in parts])
        else:
            for part in parts:
                part()
        table[here, :] = fresh[...]

    @pl.loop(0, count - 1)
    def _(p):
        panel(p, True)

    panel(count - 1, False)


def left_side(matrix, result, piece, row_base, col_base, order, solved_high, solved_low):
    rows, cols = matrix.shape

    @pl.loop(0, rows // PANEL)
    def _(r):
        start = pl.multiple_of(r * PANEL, PANEL)
        there = pl.ds(start, PANEL)
        down = row_base + start + lax.broadcasted_iota(jnp.int32, (PANEL, PANEL), 0)
        total = None
        for q in range(order // PANEL):
            unit = down == q * PANEL + lax.broadcasted_iota(jnp.int32, (PANEL, PANEL), 1)
            column = piece(start, q) - jnp.where(unit, 1.0, 0.0)
            among = pl.ds(q * PANEL, PANEL)
            part = triple(column, solved_high[among, :cols], solved_low[among, :cols])
            total = part if total is None else total + part
        base = matrix[there, :]
        if col_base is not None:
            inside = jnp.logical_and(col_base >= 0, col_base < order)
            across = col_base + lax.broadcasted_iota(jnp.int32, (PANEL, cols), 1)
            begin = row_base + start + lax.broadcasted_iota(jnp.int32, (PANEL, cols), 0)
            base = jnp.where(inside, jnp.where(begin == across, 1.0, 0.0), base)
        result[there, :] = base - total


def center(step, mine, other, matrix, mate, half, table, fresh, fresh_high, fresh_low, inverse_of, right_high, right_low):
    core = lax.axis_index("core")
    rows = matrix.shape[0]
    order = JOINED * PANEL
    base = (lax.axis_index("y") - step) * order + lax.axis_index("x") * matrix.shape[1]
    pair = (pl.ds(0, rows), pl.ds(rows, rows))
    for at in range(2):

        @pl.when(core == at)
        def _():
            for q in range(JOINED):
                table[pair[at], q * PANEL : (q + 1) * PANEL] = mine[q]
            for q in range(2):
                across = 2 * (1 - at) + q
                table[pair[1 - at], across * PANEL : (across + 1) * PANEL] = other[q]
                table[across * PANEL : (across + 1) * PANEL, pair[at]] = mine[across].T

    composite(JOINED, table, fresh, fresh_high, fresh_low, inverse_of)
    inside = jnp.logical_and(base >= 0, base < order)
    for first, source in ((core * rows, matrix), ((1 - core) * rows, mate)):
        shape = source.shape
        unit = first + lax.broadcasted_iota(jnp.int32, shape, 0) == base + lax.broadcasted_iota(jnp.int32, shape, 1)
        high, low = halves(jnp.where(inside, jnp.where(unit, 1.0, 0.0), source[...]))
        there = pl.ds(pl.multiple_of(first, rows), rows)
        right_high[there, :] = high
        right_low[there, :] = low
    for q in range(rows // PANEL):
        there = pl.ds(pl.multiple_of(core * rows + q * PANEL, PANEL), PANEL)
        half[q * PANEL : (q + 1) * PANEL, :] = triple(table[there, :], right_high[...], right_low[...])


def a_center(strips, a_top, c_top, solved, table, fresh, fresh_high, fresh_low, inverse_of, right_high, right_low):
    order, cols = a_top.shape
    table[...] = strips[0]
    composite(STEPS_A, table, fresh, fresh_high, fresh_low, inverse_of)
    base = (lax.axis_index("y") * 4 + lax.axis_index("x")) * cols
    unit = lax.broadcasted_iota(jnp.int32, (order, cols), 0) == base + lax.broadcasted_iota(jnp.int32, (order, cols), 1)
    high, low = halves(jnp.where(base < order, jnp.where(unit, 1.0, 0.0), a_top[...]))
    right_high[:, :cols] = high
    right_low[:, :cols] = low
    high, low = halves(c_top[...])
    right_high[:, cols:] = high
    right_low[:, cols:] = low
    for q in range(STEPS_A):
        there = slice(q * PANEL, (q + 1) * PANEL)
        solved[there, :] = triple(table[there, :], right_high[...], right_low[...])


def update(step, matrix, column, solved, result, solved_high, solved_low):
    order = JOINED * PANEL
    rows = matrix.shape[0]
    row_base = (lax.axis_index("z") - step) * order + lax.axis_index("core") * rows
    col_base = (lax.axis_index("y") - step) * order + lax.axis_index("x") * matrix.shape[1]
    for core in range(2):
        high, low = halves(solved[core])
        solved_high[core * rows : (core + 1) * rows, :] = high
        solved_low[core * rows : (core + 1) * rows, :] = low
    piece = lambda start, q: column[q, pl.ds(start, PANEL), :]
    left_side(matrix, result, piece, row_base, col_base, order, solved_high, solved_low)


def a_update(matrix, other, strips, solved, solved_high, solved_low):
    order = STEPS_A * PANEL
    cols = matrix.shape[1]
    row_base = (lax.axis_index("z") * 2 + lax.axis_index("core")) * matrix.shape[0]
    col_base = (lax.axis_index("y") * 4 + lax.axis_index("x")) * cols
    high, low = halves(solved[...])
    solved_high[...] = high
    solved_low[...] = low

    def piece(start, q):
        among = pl.ds(pl.multiple_of(lax.rem(start, order), PANEL), PANEL)
        return strips[start // order, pl.ds(q * PANEL, PANEL), among].T

    left_side(matrix, matrix, piece, row_base, col_base, order, solved_high.at[:, :cols], solved_low.at[:, :cols])
    left_side(other, other, piece, row_base, None, order, solved_high.at[:, cols:], solved_low.at[:, cols:])


CHUNKS = 8
AHEAD = tuple(range(CHUNKS // 2))
BEHIND = tuple(range(CHUNKS // 2, CHUNKS))


def ring(index, by):
    return lax.rem(index + by, 4)


def send(source, target, sent, received, where):
    return pltpu.make_async_remote_copy(
        src_ref=source, dst_ref=target, send_sem=sent, recv_sem=received,
        device_id=where, device_id_type=pl.DeviceIdType.MESH,
    )


def greet(neighbours):
    barrier = pltpu.get_barrier_semaphore()
    for where in neighbours:
        pl.semaphore_signal(barrier, inc=1, device_id=where, device_id_type=pl.DeviceIdType.MESH)
    pl.semaphore_wait(barrier, len(neighbours))


def chunk(h, rows=512):
    return pl.ds(h * (rows // CHUNKS), rows // CHUNKS)


def both(left, right):
    return left if right is True else jnp.logical_and(left, right)


def spread(axis, step, source, landing, sent, received, follow, active=True, around=()):
    place = lax.axis_index(axis)
    apart = lax.rem(place - step + 4, 4)
    up, down = {axis: ring(place, 1)}, {axis: ring(place, 3)}

    def copy(ref, h, side):
        return send(ref.at[chunk(h)], landing.at[chunk(h)], sent.at[side, h], received.at[h], (up, down)[side])

    def begin():
        @pl.when(both(apart == 0, active))
        def _():
            for one, two in zip(AHEAD + BEHIND, BEHIND + AHEAD):
                if one not in around:
                    copy(source, one, 0).start()
                copy(source, two, 1).start()
            for h in range(CHUNKS):
                follow(h, source)

    def relay():
        def take(order, onward, side):
            for h in order:
                copy(landing, h, 0).wait_recv()
                if h in onward:
                    copy(landing, h, side).start()
                follow(h, landing)

        @pl.when(both(apart == 1, active))
        def _():
            take([h for h in AHEAD + BEHIND if h not in around] + list(around), AHEAD, 0)

        @pl.when(both(apart == 3, active))
        def _():
            take(BEHIND + AHEAD, BEHIND, 1)

        @pl.when(both(apart == 2, active))
        def _():
            take([h for two in zip(AHEAD, BEHIND) for h in two], around, 1)

    def finish():
        @pl.when(both(apart == 0, active))
        def _():
            for h in range(CHUNKS):
                if h not in around:
                    copy(source, h, 0).wait_send()
                copy(source, h, 1).wait_send()

        @pl.when(both(apart == 1, active))
        def _():
            for h in AHEAD:
                copy(landing, h, 0).wait_send()

        @pl.when(both(apart == 3, active))
        def _():
            for h in BEHIND:
                copy(landing, h, 1).wait_send()

        if around:

            @pl.when(both(apart == 2, active))
            def _():
                for h in around:
                    copy(landing, h, 1).wait_send()

    return apart, begin, relay, finish


def nothing(h, ref):
    pass


def gather(step, matrix, column, other, mate, y_sent, y_got, x_sent, x_got, far_sent, far_got, core_sent, core_got):
    x = lax.axis_index("x")
    core = lax.axis_index("core")
    right, left, far = ring(x, 1), ring(x, 3), ring(x, 2)
    partner = {"core": 1 - core}
    centered = lax.axis_index("z") == step
    swap = send(matrix, mate, core_sent.at[2], core_got.at[2], partner)

    def sideways(h, ref):
        return [
            send(ref.at[chunk(h)], column.at[x, chunk(h)], x_sent.at[0, h], x_got.at[0, h], {"x": right}),
            send(ref.at[chunk(h)], column.at[x, chunk(h)], x_sent.at[1, h], x_got.at[1, h], {"x": left}),
        ]

    def follow(h, ref):
        for copy in sideways(h, ref):
            copy.start()

    apart, begin, relay, finish = spread("y", step, matrix, column.at[x], y_sent, y_got, follow)

    def start():
        begin()

        @pl.when(centered)
        def _():
            swap.start()

    def give(place, ref):
        slot = lax.rem(place, 2)
        return send(ref, other.at[slot], core_sent.at[slot], core_got.at[slot], partner)

    def maybe_give(place, ref, also=True):
        @pl.when(both(jnp.logical_and(centered, place // 2 == core), also))
        def _():
            give(place, ref).start()

    def arrive(place, h, received):
        ref = column.at[place, chunk(h)]
        send(ref, ref, x_sent.at[0, h], received, {"x": right}).wait_recv()

    def pass_on(h):
        place, where = (left, right) if h in AHEAD else (right, left)
        ref = column.at[place, chunk(h)]
        return send(ref, ref, far_sent.at[h], far_got.at[h], {"x": where})

    def middle():
        relay()
        maybe_give(x, matrix, apart == 0)
        maybe_give(x, column.at[x], apart != 0)

        @pl.when(apart == 0)
        def _():
            column[x] = matrix[...]

        for one, two in zip(AHEAD, BEHIND):
            arrive(left, one, x_got.at[0, one])
            pass_on(one).start()
            arrive(right, two, x_got.at[1, two])
            pass_on(two).start()
        for one, two in zip(AHEAD, BEHIND):
            arrive(right, one, x_got.at[1, one])
            arrive(left, two, x_got.at[0, two])
        maybe_give(left, column.at[left])
        maybe_give(right, column.at[right])
        slot = lax.rem(far, 2)
        ours = jnp.logical_and(centered, far // 2 == core)
        for h in [h for two in zip(AHEAD, BEHIND) for h in two]:
            arrive(far, h, far_got.at[h])
            late = send(column.at[far, chunk(h)], other.at[slot, chunk(h)], core_sent.at[slot], core_got.at[slot], partner)
            pl.when(ours)(late.start)

    def end():
        @pl.when(centered)
        def _():
            swap.wait_recv()
            give(0, matrix).wait_recv()
            give(1, matrix).wait_recv()

    def drain():
        finish()
        for h in range(CHUNKS):
            for copy in sideways(h, matrix):
                copy.wait_send()
            pass_on(h).wait_send()

        @pl.when(centered)
        def _():
            swap.wait_send()
            give(0, matrix).wait_send()
            give(1, matrix).wait_send()

    return start, middle, end, drain


def share(step, half, solved, z_sent, z_got, core_sent, core_got):
    core = lax.axis_index("core")
    partner = {"core": 1 - core}

    def give(h, ref):
        return send(ref.at[chunk(h)], solved.at[core, chunk(h)], core_sent.at[h], core_got.at[h], partner)

    def follow(h, ref):
        give(h, ref).start()

    apart, begin, relay, finish = spread("z", step, half, solved.at[core], z_sent, z_got, follow, around=BEHIND[:1])

    def end():
        @pl.when(apart == 0)
        def _():
            solved[core] = half[...]

        for h in range(CHUNKS):
            ref = solved.at[1 - core, chunk(h)]
            send(ref, ref, core_sent.at[h], core_got.at[h], partner).wait_recv()

    def drain():
        finish()
        for h in range(CHUNKS):
            give(h, half).wait_send()

    return begin, relay, end, drain


def peers():
    z, core, y, x = (lax.axis_index(axis) for axis in AXES)
    line, plane = z * 2 + core, y * 4 + x
    along, among = [], []
    for by in range(1, 8):
        place = lax.rem(line + by, 8)
        along.append({"z": place // 2, "core": lax.rem(place, 2)})
    for by in range(1, 16):
        place = lax.rem(plane + by, 16)
        among.append({"y": place // 4, "x": lax.rem(place, 4)})
    return along, among


def exchange(value, slots, sent, received, partners):
    copies = [send(value, slots.at[at], sent.at[at], received.at[at], where) for at, where in enumerate(partners)]
    for copy in copies:
        copy.start()
    for copy in copies:
        copy.wait()
    result = value[...]
    for at in range(len(partners)):
        result = result + slots[at]
    return result


def squares(value):
    return jnp.sum(jnp.sum(value * value, axis=0, keepdims=True), axis=1, keepdims=True)


def whole_kernel(a_hbm, b_hbm, c_hbm, a_out, c_out, b_out, *spaces):
    s = dict(zip(SPACES, spaces))
    z, core, y, x = (lax.axis_index(axis) for axis in AXES)
    a, b, c = s["a"], s["matrix"].at[0], s["c"]
    a_order = STEPS_A * PANEL
    a_top, c_top = a.at[:a_order], c.at[:a_order]
    loads = [pltpu.make_async_copy(held, to, s["load"].at[at]) for at, (held, to) in enumerate([(b_hbm, b), (a_hbm, a), (c_hbm, c)])]
    stores = [pltpu.make_async_copy(a, a_out, s["load"].at[1]), pltpu.make_async_copy(c, c_out, s["load"].at[2])]
    for copy in loads:
        copy.start()
    along, among = peers()
    greet(along + among)
    loads[0].wait()

    home = jnp.logical_and(z == 0, core == 0)
    holds = core == x // 2
    goal = jnp.logical_and(z == y, holds)
    stays = jnp.logical_and(home, goal)
    goes = jnp.logical_and(home, jnp.logical_not(goal))
    comes = jnp.logical_and(goal, jnp.logical_not(home))
    seeding = send(a_top, s["seed"], s["seed_sent"], s["seed_got"], {"z": y, "core": x // 2})
    partner = {"core": 1 - core}

    def a_give(h, ref):
        return send(ref.at[chunk(h)], s["a_shared"].at[chunk(h)], s["a_pass_sent"].at[h], s["a_pass_got"].at[h], partner)

    def a_follow(h, ref):
        a_give(h, ref).start()

    def along_y(source, active):
        return spread("y", z, source, s["strip"], s["ay_sent"], s["ay_got"], nothing, active)

    def along_x(active):
        return [
            spread("x", 2 * core + at, s["strip"], s["strips"].at[at], s["ax_sent"].at[at], s["ax_got"].at[at], nothing, active)
            for at in range(2)
        ]

    a_share = spread("z", 0, s["a_solved"], s["a_shared"], s["az_sent"], s["az_got"], a_follow, core == 0)

    def finish_a():
        a_update(a, c, s["strips"], s["a_shared"], s["a_solved_high"], s["a_solved_low"])
        for copy in stores:
            copy.start()

    def both_of(*conditions):
        return functools.reduce(jnp.logical_and, conditions)

    @pl.loop(0, STEPS_B // JOINED)
    def _(step):
        first, second, third, last = (step == at for at in range(4))
        matrix = s["matrix"].at[step]
        column, other, mate, half, solved = (s[name].at[step] for name in ("column", "other", "mate", "half", "solved"))
        here, away = z == step, z != step
        start, middle, end, gathered = gather(step, matrix, column, other, mate, *(s[name].at[step] for name in GATHER_FLAGS))
        start()

        @pl.when(first)
        def _():
            loads[1].wait()
            loads[2].wait()
            pl.when(goes)(seeding.start)

        middle()

        @pl.when(last)
        def _():
            a_share[2]()

        end()

        @pl.when(first)
        def _():
            pl.when(goes)(seeding.wait_send)
            pl.when(comes)(seeding.wait_recv)
            along_y(s["seed"], both_of(holds, jnp.logical_not(stays)))[1]()
            along_y(a_top, stays)[1]()

        @pl.when(second)
        def _():
            for one in along_x(True):
                one[1]()

        @pl.when(here)
        def _():
            center(step, column, other, matrix, mate, half, *(s[name] for name in CENTER_SPACES))

        @pl.when(both_of(first, away))
        def _():
            along_y(s["seed"], holds)[2]()

        @pl.when(both_of(second, away))
        def _():
            for one in along_x(True):
                one[2]()

        @pl.when(both_of(third, home))
        def _():
            a_center(s["strips"], a_top, c_top, s["a_solved"], *(s[name] for name in A_CENTER_SPACES))

        @pl.when(last)
        def _():
            @pl.when(home)
            def _():
                s["a_shared"][...] = s["a_solved"][...]

            @pl.when(core == 1)
            def _():
                for h in range(CHUNKS):
                    a_give(h, s["a_solved"]).wait_recv()

        begin, relay, close, shared = share(step, half, solved, *(s[name].at[step] for name in SHARE_FLAGS))
        begin()
        pl.when(last)(finish_a)
        relay()

        @pl.when(first)
        def _():
            @pl.when(here)
            def _():
                along_y(s["seed"], holds)[2]()

            @pl.when(stays)
            def _():
                s["strip"][...] = a_top[...]

            @pl.when(comes)
            def _():
                s["strip"][...] = s["seed"][...]

        @pl.when(second)
        def _():
            @pl.when(here)
            def _():
                for one in along_x(True):
                    one[2]()

            for at, one in enumerate(along_x(True)):

                @pl.when(one[0] == 0)
                def _():
                    s["strips"][at] = s["strip"][...]

        close()
        update(step, matrix, column, solved, s["matrix"].at[step + 1], s["solved_high"], s["solved_low"])
        gathered()
        shared()

        @pl.when(first)
        def _():
            along_y(s["seed"], holds)[3]()

        @pl.when(second)
        def _():
            for one in along_x(True):
                one[3]()

        @pl.when(third)
        def _():
            a_share[1]()

    matrix = s["matrix"].at[STEPS_B // JOINED]
    lane = lax.broadcasted_iota(jnp.int32, (8, 128), 1)
    s["partial"][0] = jnp.where(lane == 0, squares(b[...]), squares(matrix[...]))
    s["partial"][1] = exchange(s["partial"].at[0], s["line"], s["line_sent"], s["line_got"], along)
    total = exchange(s["partial"].at[1], s["plane"], s["plane_sent"], s["plane_got"], among)
    scale = jnp.sqrt(jnp.sqrt(total[0:1, 1:2] / total[0:1, 0:1]))
    b_out[...] = 0.5 * (scale * b[...] + matrix[...] / scale)
    a_share[3]()

    @pl.when(core == 0)
    def _():
        for h in range(CHUNKS):
            a_give(h, s["a_solved"]).wait_send()

    for copy in stores:
        copy.wait()


GATHER_FLAGS = ("y_sent", "y_got", "x_sent", "x_got", "far_sent", "far_got", "core_sent", "core_got")
CENTER_SPACES = ("table", "fresh", "fresh_high", "fresh_low", "inverse_of", "right_high", "right_low")
A_CENTER_SPACES = ("a_table", "a_fresh", "a_fresh_high", "a_fresh_low", "inverse_of", "a_right_high", "a_right_low")
SHARE_FLAGS = ("z_sent", "z_got", "pass_sent", "pass_got")


def flags(*shape):
    return pltpu.SemaphoreType.DMA(shape)


def spaces_of(a_shape, b_shape, c_shape):
    steps = STEPS_B // JOINED
    order, a_order = JOINED * PANEL, STEPS_A * PANEL
    rows, cols = b_shape
    wide = a_shape[1] + c_shape[1]
    top = (a_order, a_shape[1])
    full = lambda *shape: pltpu.VMEM(shape, F32)
    short = lambda *shape: pltpu.VMEM(shape, BF16)
    ringed = (2, CHUNKS)
    return dict(
        a=full(*a_shape), c=full(*c_shape), load=flags(3), inverse_of=full(PANEL, PANEL),
        column=full(steps, 4, rows, cols), other=full(steps, 2, rows, cols), mate=full(steps, rows, cols),
        half=full(steps, rows, cols), solved=full(steps, 2, rows, cols), matrix=full(steps + 1, rows, cols),
        table=full(order, order), fresh=full(PANEL, order), fresh_high=short(PANEL, order), fresh_low=short(PANEL, order),
        right_high=short(order, cols), right_low=short(order, cols), solved_high=short(order, cols), solved_low=short(order, cols),
        seed=full(*top), strip=full(*top), strips=full(2, *top), a_solved=full(a_order, wide), a_shared=full(a_order, wide),
        a_table=full(a_order, a_order), a_fresh=full(PANEL, a_order), a_fresh_high=short(PANEL, a_order), a_fresh_low=short(PANEL, a_order),
        a_right_high=short(a_order, wide), a_right_low=short(a_order, wide), a_solved_high=short(a_order, wide), a_solved_low=short(a_order, wide),
        partial=full(2, 8, 128), line=full(7, 8, 128), plane=full(15, 8, 128),
        y_sent=flags(steps, *ringed), y_got=flags(steps, CHUNKS), x_sent=flags(steps, *ringed), x_got=flags(steps, *ringed),
        far_sent=flags(steps, CHUNKS), far_got=flags(steps, CHUNKS), core_sent=flags(steps, 3), core_got=flags(steps, 3),
        z_sent=flags(steps, *ringed), z_got=flags(steps, CHUNKS), pass_sent=flags(steps, CHUNKS), pass_got=flags(steps, CHUNKS),
        seed_sent=pltpu.SemaphoreType.DMA, seed_got=pltpu.SemaphoreType.DMA,
        ay_sent=flags(*ringed), ay_got=flags(CHUNKS), ax_sent=flags(2, *ringed), ax_got=flags(2, CHUNKS),
        az_sent=flags(*ringed), az_got=flags(CHUNKS), a_pass_sent=flags(CHUNKS), a_pass_got=flags(CHUNKS),
        line_sent=flags(7), line_got=flags(7), plane_sent=flags(15), plane_got=flags(15),
    )


SPACES = tuple(spaces_of((1, 1), (1, 1), (1, 1)))


def body(a_matrix, b_matrix, c_matrix):
    held = pl.BlockSpec(memory_space=pltpu.VMEM)
    left = pl.BlockSpec(memory_space=pl.ANY)
    shapes = (a_matrix.shape, b_matrix.shape, c_matrix.shape)
    a_swept, c_swept, b_next = pl.pallas_call(
        whole_kernel,
        out_shape=[jax.ShapeDtypeStruct(shapes[at], F32) for at in (0, 2, 1)],
        in_specs=[left, left, left],
        out_specs=[left, left, held],
        scratch_shapes=list(spaces_of(*shapes).values()),
        compiler_params=pltpu.CompilerParams(vmem_limit_bytes=63 * 1024 * 1024, collective_id=0, has_side_effects=True),
    )(a_matrix, b_matrix, c_matrix)
    return (a_swept, c_swept, b_next)


def solution(mesh):
    finer = Mesh(mesh.devices.reshape(4, 2, 4, 4), AXES)
    placed = (P(ROW, COL), P(ROW, COL), P(ROW, COL))
    return jax.shard_map(body, mesh=finer, in_specs=placed, out_specs=placed, check_vma=False)
```

```python
import functools

import jax
import jax.numpy as jnp
from jax import lax
from jax.experimental import pallas as pl
from jax.experimental.pallas import tpu as pltpu
from jax.sharding import Mesh
from jax.sharding import PartitionSpec as P

PANEL = 256
SQUARINGS = 5
STEPS_A = 2
STEPS_B = 16
JOINED = 4
AXES = ("z", "core", "y", "x")
ROW = ("z", "core")
COL = ("y", "x")
F32 = jnp.float32
BF16 = jnp.bfloat16


def halves(value):
    high = value.astype(BF16)
    return high, (value - high.astype(F32)).astype(BF16)


def product(left, right):
    return jnp.dot(left, right, preferred_element_type=F32)


def summed(high, low, right_high, right_low):
    return product(high, right_high) + product(high, right_low) + product(low, right_high)


def triple(left, right_high, right_low):
    return summed(*halves(left), right_high, right_low)


def by_rows(high, low, right_high, right_low):
    cut = high.shape[0] // 2
    parts = [summed(high[at], low[at], right_high, right_low) for at in (slice(None, cut), slice(cut, None))]
    return jnp.concatenate(parts, 0)


def pivot_inverse(pivot, between=()):
    parts = iter(between)

    def fill():
        for part in next(parts, ()):
            part()

    shape = (PANEL, PANEL)
    unit = lax.broadcasted_iota(jnp.int32, shape, 0) == lax.broadcasted_iota(jnp.int32, shape, 1)
    diagonal = jnp.where(unit, pivot, 0.0)
    down = 1.0 / jnp.sqrt(jnp.sum(diagonal, axis=1, keepdims=True))
    across = 1.0 / jnp.sqrt(jnp.sum(diagonal, axis=0, keepdims=True))
    scaled = pivot * down * across
    ceiling = jnp.max(jnp.sum(jnp.abs(scaled), axis=0, keepdims=True), axis=1, keepdims=True)
    eye = jnp.where(unit, 1.0, 0.0)
    power = eye - scaled / ceiling
    fill()
    total = eye + power
    high, low = halves(power)
    power = by_rows(high, low, high, low)
    fill()
    for turn in range(SQUARINGS - 1):
        high, low = halves(power)
        total_high, total_low = halves(total)
        pair = summed(high, low, jnp.concatenate([high, total_high], 1), jnp.concatenate([low, total_low], 1))
        fill()
        power = pair[:, :PANEL]
        total = total + pair[:, PANEL:]
    total = total + by_rows(*halves(total), *halves(power))
    return total / ceiling * down * across


def composite(count, table, fresh, fresh_high, fresh_low, inverse_of):
    inverse_of[...] = pivot_inverse(table[:PANEL, :PANEL])

    def panel(p, more):
        here = pl.ds(pl.multiple_of(p * PANEL, PANEL), PANEL)
        others = [pl.ds(pl.multiple_of(lax.rem(p + by, count) * PANEL, PANEL), PANEL) for by in range(1, count)]
        inverse = inverse_of[...]
        inverse_high, inverse_low = halves(inverse)
        high, low = halves(jnp.concatenate([table[there, here] for there in others], 0))

        def row():
            fresh[...] = summed(inverse_high, inverse_low, *halves(table[here, :]))
            fresh[:, here] = inverse
            fresh_high[...], fresh_low[...] = halves(fresh[...])
            for there in others:
                table[there, here] = jnp.zeros((PANEL, PANEL), F32)

        def rest(at):
            cols = slice(at * PANEL, (at + 1) * PANEL)
            taken = summed(high, low, fresh_high[:, cols], fresh_low[:, cols])
            for nth, there in enumerate(others):
                table[there, cols] = table[there, cols] - taken[nth * PANEL : (nth + 1) * PANEL]

        parts = [row] + [functools.partial(rest, at) for at in range(count)]
        if more:
            after = others[0]
            solved = by_rows(inverse_high, inverse_low, *halves(table[here, after]))
            block = table[after, after] - by_rows(high[:PANEL], low[:PANEL], *halves(solved))
            inverse_of[...] = pivot_inverse(block, [(part,) for part in parts])
        else:
            for part in parts:
                part()
        table[here, :] = fresh[...]

    @pl.loop(0, count - 1)
    def _(p):
        panel(p, True)

    panel(count - 1, False)


def left_side(matrix, result, piece, row_base, col_base, order, solved_high, solved_low):
    rows, cols = matrix.shape

    @pl.loop(0, rows // PANEL)
    def _(r):
        start = pl.multiple_of(r * PANEL, PANEL)
        there = pl.ds(start, PANEL)
        down = row_base + start + lax.broadcasted_iota(jnp.int32, (PANEL, PANEL), 0)
        total = None
        for q in range(order // PANEL):
            unit = down == q * PANEL + lax.broadcasted_iota(jnp.int32, (PANEL, PANEL), 1)
            column = piece(start, q) - jnp.where(unit, 1.0, 0.0)
            among = pl.ds(q * PANEL, PANEL)
            part = triple(column, solved_high[among, :cols], solved_low[among, :cols])
            total = part if total is None else total + part
        base = matrix[there, :]
        if col_base is not None:
            inside = jnp.logical_and(col_base >= 0, col_base < order)
            across = col_base + lax.broadcasted_iota(jnp.int32, (PANEL, cols), 1)
            begin = row_base + start + lax.broadcasted_iota(jnp.int32, (PANEL, cols), 0)
            base = jnp.where(inside, jnp.where(begin == across, 1.0, 0.0), base)
        result[there, :] = base - total


def center(step, mine, other, matrix, mate, half, table, fresh, fresh_high, fresh_low, inverse_of, right_high, right_low):
    core = lax.axis_index("core")
    rows = matrix.shape[0]
    order = JOINED * PANEL
    base = (lax.axis_index("y") - step) * order + lax.axis_index("x") * matrix.shape[1]
    pair = (pl.ds(0, rows), pl.ds(rows, rows))
    for at in range(2):

        @pl.when(core == at)
        def _():
            far = ring(lax.axis_index("x"), 2)
            table[pair[at], pl.ds(pl.multiple_of(far * PANEL, PANEL), PANEL)] = mine[far]
            for q in range(2):
                across = 2 * (1 - at) + q
                table[pair[1 - at], across * PANEL : (across + 1) * PANEL] = other[q]
                table[across * PANEL : (across + 1) * PANEL, pair[at]] = mine[across].T

    composite(JOINED, table, fresh, fresh_high, fresh_low, inverse_of)
    inside = jnp.logical_and(base >= 0, base < order)
    for first, source in ((core * rows, matrix), ((1 - core) * rows, mate)):
        shape = source.shape
        unit = first + lax.broadcasted_iota(jnp.int32, shape, 0) == base + lax.broadcasted_iota(jnp.int32, shape, 1)
        high, low = halves(jnp.where(inside, jnp.where(unit, 1.0, 0.0), source[...]))
        there = pl.ds(pl.multiple_of(first, rows), rows)
        right_high[there, :] = high
        right_low[there, :] = low
    for q in range(rows // PANEL):
        there = pl.ds(pl.multiple_of(core * rows + q * PANEL, PANEL), PANEL)
        half[q * PANEL : (q + 1) * PANEL, :] = triple(table[there, :], right_high[...], right_low[...])


def a_center(strips, a_top, c_top, solved, table, fresh, fresh_high, fresh_low, inverse_of, right_high, right_low):
    order, cols = a_top.shape
    table[...] = strips[0]
    composite(STEPS_A, table, fresh, fresh_high, fresh_low, inverse_of)
    base = (lax.axis_index("y") * 4 + lax.axis_index("x")) * cols
    unit = lax.broadcasted_iota(jnp.int32, (order, cols), 0) == base + lax.broadcasted_iota(jnp.int32, (order, cols), 1)
    high, low = halves(jnp.where(base < order, jnp.where(unit, 1.0, 0.0), a_top[...]))
    right_high[:, :cols] = high
    right_low[:, :cols] = low
    high, low = halves(c_top[...])
    right_high[:, cols:] = high
    right_low[:, cols:] = low
    for q in range(STEPS_A):
        there = slice(q * PANEL, (q + 1) * PANEL)
        solved[there, :] = triple(table[there, :], right_high[...], right_low[...])


def update(step, matrix, column, solved, result, solved_high, solved_low):
    order = JOINED * PANEL
    rows = matrix.shape[0]
    row_base = (lax.axis_index("z") - step) * order + lax.axis_index("core") * rows
    col_base = (lax.axis_index("y") - step) * order + lax.axis_index("x") * matrix.shape[1]
    for core in range(2):
        high, low = halves(solved[core])
        solved_high[core * rows : (core + 1) * rows, :] = high
        solved_low[core * rows : (core + 1) * rows, :] = low
    piece = lambda start, q: column[q, pl.ds(start, PANEL), :]
    left_side(matrix, result, piece, row_base, col_base, order, solved_high, solved_low)


def a_update(matrix, other, strips, solved, solved_high, solved_low):
    order = STEPS_A * PANEL
    cols = matrix.shape[1]
    row_base = (lax.axis_index("z") * 2 + lax.axis_index("core")) * matrix.shape[0]
    col_base = (lax.axis_index("y") * 4 + lax.axis_index("x")) * cols
    high, low = halves(solved[...])
    solved_high[...] = high
    solved_low[...] = low

    def piece(start, q):
        among = pl.ds(pl.multiple_of(lax.rem(start, order), PANEL), PANEL)
        return strips[start // order, pl.ds(q * PANEL, PANEL), among].T

    left_side(matrix, matrix, piece, row_base, col_base, order, solved_high.at[:, :cols], solved_low.at[:, :cols])
    left_side(other, other, piece, row_base, None, order, solved_high.at[:, cols:], solved_low.at[:, cols:])


CHUNKS = 8
AHEAD = tuple(range(CHUNKS // 2))
BEHIND = tuple(range(CHUNKS // 2, CHUNKS))


def ring(index, by):
    return lax.rem(index + by, 4)


def send(source, target, sent, received, where):
    return pltpu.make_async_remote_copy(
        src_ref=source, dst_ref=target, send_sem=sent, recv_sem=received,
        device_id=where, device_id_type=pl.DeviceIdType.MESH,
    )


def greet(neighbours):
    barrier = pltpu.get_barrier_semaphore()
    for where in neighbours:
        pl.semaphore_signal(barrier, inc=1, device_id=where, device_id_type=pl.DeviceIdType.MESH)
    pl.semaphore_wait(barrier, len(neighbours))


def chunk(h, rows=512):
    return pl.ds(h * (rows // CHUNKS), rows // CHUNKS)


def both(left, right):
    return left if right is True else jnp.logical_and(left, right)


def spread(axis, step, source, landing, sent, received, follow, active=True, around=()):
    place = lax.axis_index(axis)
    apart = lax.rem(place - step + 4, 4)
    up, down = {axis: ring(place, 1)}, {axis: ring(place, 3)}

    def copy(ref, h, side):
        return send(ref.at[chunk(h)], landing.at[chunk(h)], sent.at[side, h], received.at[h], (up, down)[side])

    def begin():
        @pl.when(both(apart == 0, active))
        def _():
            for one, two in zip(AHEAD + BEHIND, BEHIND + AHEAD):
                if one not in around:
                    copy(source, one, 0).start()
                copy(source, two, 1).start()
            for h in range(CHUNKS):
                follow(h, source)

    def relay():
        def take(order, onward, side):
            for h in order:
                copy(landing, h, 0).wait_recv()
                if h in onward:
                    copy(landing, h, side).start()
                follow(h, landing)

        @pl.when(both(apart == 1, active))
        def _():
            take([h for h in AHEAD + BEHIND if h not in around] + list(around), AHEAD, 0)

        @pl.when(both(apart == 3, active))
        def _():
            take(BEHIND + AHEAD, BEHIND, 1)

        @pl.when(both(apart == 2, active))
        def _():
            take([h for two in zip(AHEAD, BEHIND) for h in two], around, 1)

    def finish():
        @pl.when(both(apart == 0, active))
        def _():
            for h in range(CHUNKS):
                if h not in around:
                    copy(source, h, 0).wait_send()
                copy(source, h, 1).wait_send()

        @pl.when(both(apart == 1, active))
        def _():
            for h in AHEAD:
                copy(landing, h, 0).wait_send()

        @pl.when(both(apart == 3, active))
        def _():
            for h in BEHIND:
                copy(landing, h, 1).wait_send()

        if around:

            @pl.when(both(apart == 2, active))
            def _():
                for h in around:
                    copy(landing, h, 1).wait_send()

    return apart, begin, relay, finish


def nothing(h, ref):
    pass


def gather(early, step, matrix, column, other, mate, y_sent, y_got, x_sent, x_got, far_sent, far_got, core_sent, core_got):
    x = lax.axis_index("x")
    core = lax.axis_index("core")
    right, left, far = ring(x, 1), ring(x, 3), ring(x, 2)
    partner = {"core": 1 - core}
    centered = lax.axis_index("z") == step
    swap = send(matrix, mate, core_sent.at[2], core_got.at[2], partner)

    def sideways(h, ref):
        return [
            send(ref.at[chunk(h)], column.at[x, chunk(h)], x_sent.at[0, h], x_got.at[0, h], {"x": right}),
            send(ref.at[chunk(h)], column.at[x, chunk(h)], x_sent.at[1, h], x_got.at[1, h], {"x": left}),
        ]

    def follow(h, ref):
        for copy in sideways(h, ref):
            copy.start()

    apart, begin, relay, finish = spread("y", step, matrix, column.at[x], y_sent, y_got, follow)

    def start():
        begin()

        @pl.when(centered)
        def _():
            swap.start()

    def give(place, ref):
        slot = lax.rem(place, 2)
        return send(ref, other.at[slot], core_sent.at[slot], core_got.at[slot], partner)

    def maybe_give(place, ref, also=True):
        @pl.when(both(jnp.logical_and(centered, place // 2 == core), also))
        def _():
            give(place, ref).start()

    def arrive(place, h, received):
        ref = column.at[place, chunk(h)]
        send(ref, ref, x_sent.at[0, h], received, {"x": right}).wait_recv()

    def pass_on(h):
        place, where = (left, right) if h in AHEAD else (right, left)
        ref = column.at[place, chunk(h)]
        return send(ref, ref, far_sent.at[h], far_got.at[h], {"x": where})

    def middle():
        relay()
        maybe_give(x, matrix, apart == 0)
        maybe_give(x, column.at[x], apart != 0)

        @pl.when(apart == 0)
        def _():
            column[x] = matrix[...]

        for one, two in zip(AHEAD, BEHIND):
            arrive(left, one, x_got.at[0, one])
            pass_on(one).start()
            arrive(right, two, x_got.at[1, two])
            pass_on(two).start()
        for one, two in zip(AHEAD, BEHIND):
            arrive(right, one, x_got.at[1, one])
            arrive(left, two, x_got.at[0, two])
        maybe_give(left, column.at[left])
        maybe_give(right, column.at[right])
        for place in (x, left, right):
            early(place)
        slot = lax.rem(far, 2)
        ours = jnp.logical_and(centered, far // 2 == core)
        for h in [h for two in zip(AHEAD, BEHIND) for h in two]:
            arrive(far, h, far_got.at[h])
            late = send(column.at[far, chunk(h)], other.at[slot, chunk(h)], core_sent.at[slot], core_got.at[slot], partner)
            pl.when(ours)(late.start)

    def end():
        @pl.when(centered)
        def _():
            swap.wait_recv()
            give(0, matrix).wait_recv()
            give(1, matrix).wait_recv()

    def drain():
        finish()
        for h in range(CHUNKS):
            for copy in sideways(h, matrix):
                copy.wait_send()
            pass_on(h).wait_send()

        @pl.when(centered)
        def _():
            swap.wait_send()
            give(0, matrix).wait_send()
            give(1, matrix).wait_send()

    return start, middle, end, drain


def share(step, half, solved, z_sent, z_got, core_sent, core_got):
    core = lax.axis_index("core")
    partner = {"core": 1 - core}

    def give(h, ref):
        return send(ref.at[chunk(h)], solved.at[core, chunk(h)], core_sent.at[h], core_got.at[h], partner)

    def follow(h, ref):
        give(h, ref).start()

    apart, begin, relay, finish = spread("z", step, half, solved.at[core], z_sent, z_got, follow, around=BEHIND[:1])

    def end():
        @pl.when(apart == 0)
        def _():
            solved[core] = half[...]

        for h in range(CHUNKS):
            ref = solved.at[1 - core, chunk(h)]
            send(ref, ref, core_sent.at[h], core_got.at[h], partner).wait_recv()

    def drain():
        finish()
        for h in range(CHUNKS):
            give(h, half).wait_send()

    return begin, relay, end, drain


def peers():
    z, core, y, x = (lax.axis_index(axis) for axis in AXES)
    line, plane = z * 2 + core, y * 4 + x
    along, among = [], []
    for by in range(1, 8):
        place = lax.rem(line + by, 8)
        along.append({"z": place // 2, "core": lax.rem(place, 2)})
    for by in range(1, 16):
        place = lax.rem(plane + by, 16)
        among.append({"y": place // 4, "x": lax.rem(place, 4)})
    return along, among


def exchange(value, slots, sent, received, partners):
    copies = [send(value, slots.at[at], sent.at[at], received.at[at], where) for at, where in enumerate(partners)]
    for copy in copies:
        copy.start()
    for copy in copies:
        copy.wait()
    result = value[...]
    for at in range(len(partners)):
        result = result + slots[at]
    return result


def squares(value):
    return jnp.sum(jnp.sum(value * value, axis=0, keepdims=True), axis=1, keepdims=True)


def whole_kernel(a_hbm, b_hbm, c_hbm, a_out, c_out, b_out, *spaces):
    s = dict(zip(SPACES, spaces))
    z, core, y, x = (lax.axis_index(axis) for axis in AXES)
    a, b, c = s["a"], s["matrix"].at[0], s["c"]
    a_order = STEPS_A * PANEL
    a_top, c_top = a.at[:a_order], c.at[:a_order]
    loads = [pltpu.make_async_copy(held, to, s["load"].at[at]) for at, (held, to) in enumerate([(b_hbm, b), (a_hbm, a), (c_hbm, c)])]
    stores = [pltpu.make_async_copy(a, a_out, s["load"].at[1]), pltpu.make_async_copy(c, c_out, s["load"].at[2])]
    for copy in loads:
        copy.start()
    along, among = peers()
    greet(along + among)
    loads[0].wait()

    home = jnp.logical_and(z == 0, core == 0)
    holds = core == x // 2
    goal = jnp.logical_and(z == y, holds)
    stays = jnp.logical_and(home, goal)
    goes = jnp.logical_and(home, jnp.logical_not(goal))
    comes = jnp.logical_and(goal, jnp.logical_not(home))
    seeding = send(a_top, s["seed"], s["seed_sent"], s["seed_got"], {"z": y, "core": x // 2})
    partner = {"core": 1 - core}

    def a_give(h, ref):
        return send(ref.at[chunk(h)], s["a_shared"].at[chunk(h)], s["a_pass_sent"].at[h], s["a_pass_got"].at[h], partner)

    def a_follow(h, ref):
        a_give(h, ref).start()

    def along_y(source, active):
        return spread("y", z, source, s["strip"], s["ay_sent"], s["ay_got"], nothing, active)

    def along_x(active):
        return [
            spread("x", 2 * core + at, s["strip"], s["strips"].at[at], s["ax_sent"].at[at], s["ax_got"].at[at], nothing, active)
            for at in range(2)
        ]

    a_share = spread("z", 0, s["a_solved"], s["a_shared"], s["az_sent"], s["az_got"], a_follow, core == 0)

    def finish_a():
        a_update(a, c, s["strips"], s["a_shared"], s["a_solved_high"], s["a_solved_low"])
        for copy in stores:
            copy.start()

    def both_of(*conditions):
        return functools.reduce(jnp.logical_and, conditions)

    @pl.loop(0, STEPS_B // JOINED)
    def _(step):
        first, second, third, last = (step == at for at in range(4))
        matrix = s["matrix"].at[step]
        column, other, mate, half, solved = (s[name].at[step] for name in ("column", "other", "mate", "half", "solved"))
        here, away = z == step, z != step

        def early(place):
            @pl.when(here)
            def _():
                rows = pl.ds(pl.multiple_of(core * matrix.shape[0], PANEL), matrix.shape[0])
                s["table"][rows, pl.ds(pl.multiple_of(place * PANEL, PANEL), PANEL)] = column[place]

        start, middle, end, gathered = gather(early, step, matrix, column, other, mate, *(s[name].at[step] for name in GATHER_FLAGS))
        start()

        @pl.when(first)
        def _():
            loads[1].wait()
            loads[2].wait()
            pl.when(goes)(seeding.start)

        middle()

        @pl.when(last)
        def _():
            a_share[2]()

        end()

        @pl.when(first)
        def _():
            pl.when(goes)(seeding.wait_send)
            pl.when(comes)(seeding.wait_recv)
            along_y(s["seed"], both_of(holds, jnp.logical_not(stays)))[1]()
            along_y(a_top, stays)[1]()

        @pl.when(second)
        def _():
            for one in along_x(True):
                one[1]()

        @pl.when(here)
        def _():
            center(step, column, other, matrix, mate, half, *(s[name] for name in CENTER_SPACES))

        @pl.when(both_of(first, away))
        def _():
            along_y(s["seed"], holds)[2]()

        @pl.when(both_of(second, away))
        def _():
            for one in along_x(True):
                one[2]()

        @pl.when(both_of(third, home))
        def _():
            a_center(s["strips"], a_top, c_top, s["a_solved"], *(s[name] for name in A_CENTER_SPACES))

        @pl.when(last)
        def _():
            @pl.when(home)
            def _():
                s["a_shared"][...] = s["a_solved"][...]

            @pl.when(core == 1)
            def _():
                for h in range(CHUNKS):
                    a_give(h, s["a_solved"]).wait_recv()

        begin, relay, close, shared = share(step, half, solved, *(s[name].at[step] for name in SHARE_FLAGS))
        begin()
        pl.when(last)(finish_a)
        relay()

        @pl.when(first)
        def _():
            @pl.when(here)
            def _():
                along_y(s["seed"], holds)[2]()

            @pl.when(stays)
            def _():
                s["strip"][...] = a_top[...]

            @pl.when(comes)
            def _():
                s["strip"][...] = s["seed"][...]

        @pl.when(second)
        def _():
            @pl.when(here)
            def _():
                for one in along_x(True):
                    one[2]()

            for at, one in enumerate(along_x(True)):

                @pl.when(one[0] == 0)
                def _():
                    s["strips"][at] = s["strip"][...]

        close()
        update(step, matrix, column, solved, s["matrix"].at[step + 1], s["solved_high"], s["solved_low"])
        gathered()
        shared()

        @pl.when(first)
        def _():
            along_y(s["seed"], holds)[3]()

        @pl.when(second)
        def _():
            for one in along_x(True):
                one[3]()

        @pl.when(third)
        def _():
            a_share[1]()

    matrix = s["matrix"].at[STEPS_B // JOINED]
    lane = lax.broadcasted_iota(jnp.int32, (8, 128), 1)
    s["partial"][0] = jnp.where(lane == 0, squares(b[...]), squares(matrix[...]))
    s["partial"][1] = exchange(s["partial"].at[0], s["line"], s["line_sent"], s["line_got"], along)
    total = exchange(s["partial"].at[1], s["plane"], s["plane_sent"], s["plane_got"], among)
    scale = jnp.sqrt(jnp.sqrt(total[0:1, 1:2] / total[0:1, 0:1]))
    b_out[...] = 0.5 * (scale * b[...] + matrix[...] / scale)
    a_share[3]()

    @pl.when(core == 0)
    def _():
        for h in range(CHUNKS):
            a_give(h, s["a_solved"]).wait_send()

    for copy in stores:
        copy.wait()


GATHER_FLAGS = ("y_sent", "y_got", "x_sent", "x_got", "far_sent", "far_got", "core_sent", "core_got")
CENTER_SPACES = ("table", "fresh", "fresh_high", "fresh_low", "inverse_of", "right_high", "right_low")
A_CENTER_SPACES = ("a_table", "a_fresh", "a_fresh_high", "a_fresh_low", "inverse_of", "a_right_high", "a_right_low")
SHARE_FLAGS = ("z_sent", "z_got", "pass_sent", "pass_got")


def flags(*shape):
    return pltpu.SemaphoreType.DMA(shape)


def spaces_of(a_shape, b_shape, c_shape):
    steps = STEPS_B // JOINED
    order, a_order = JOINED * PANEL, STEPS_A * PANEL
    rows, cols = b_shape
    wide = a_shape[1] + c_shape[1]
    top = (a_order, a_shape[1])
    full = lambda *shape: pltpu.VMEM(shape, F32)
    short = lambda *shape: pltpu.VMEM(shape, BF16)
    ringed = (2, CHUNKS)
    return dict(
        a=full(*a_shape), c=full(*c_shape), load=flags(3), inverse_of=full(PANEL, PANEL),
        column=full(steps, 4, rows, cols), other=full(steps, 2, rows, cols), mate=full(steps, rows, cols),
        half=full(steps, rows, cols), solved=full(steps, 2, rows, cols), matrix=full(steps + 1, rows, cols),
        table=full(order, order), fresh=full(PANEL, order), fresh_high=short(PANEL, order), fresh_low=short(PANEL, order),
        right_high=short(order, cols), right_low=short(order, cols), solved_high=short(order, cols), solved_low=short(order, cols),
        seed=full(*top), strip=full(*top), strips=full(2, *top), a_solved=full(a_order, wide), a_shared=full(a_order, wide),
        a_table=full(a_order, a_order), a_fresh=full(PANEL, a_order), a_fresh_high=short(PANEL, a_order), a_fresh_low=short(PANEL, a_order),
        a_right_high=short(a_order, wide), a_right_low=short(a_order, wide), a_solved_high=short(a_order, wide), a_solved_low=short(a_order, wide),
        partial=full(2, 8, 128), line=full(7, 8, 128), plane=full(15, 8, 128),
        y_sent=flags(steps, *ringed), y_got=flags(steps, CHUNKS), x_sent=flags(steps, *ringed), x_got=flags(steps, *ringed),
        far_sent=flags(steps, CHUNKS), far_got=flags(steps, CHUNKS), core_sent=flags(steps, 3), core_got=flags(steps, 3),
        z_sent=flags(steps, *ringed), z_got=flags(steps, CHUNKS), pass_sent=flags(steps, CHUNKS), pass_got=flags(steps, CHUNKS),
        seed_sent=pltpu.SemaphoreType.DMA, seed_got=pltpu.SemaphoreType.DMA,
        ay_sent=flags(*ringed), ay_got=flags(CHUNKS), ax_sent=flags(2, *ringed), ax_got=flags(2, CHUNKS),
        az_sent=flags(*ringed), az_got=flags(CHUNKS), a_pass_sent=flags(CHUNKS), a_pass_got=flags(CHUNKS),
        line_sent=flags(7), line_got=flags(7), plane_sent=flags(15), plane_got=flags(15),
    )


SPACES = tuple(spaces_of((1, 1), (1, 1), (1, 1)))


def body(a_matrix, b_matrix, c_matrix):
    held = pl.BlockSpec(memory_space=pltpu.VMEM)
    left = pl.BlockSpec(memory_space=pl.ANY)
    shapes = (a_matrix.shape, b_matrix.shape, c_matrix.shape)
    a_swept, c_swept, b_next = pl.pallas_call(
        whole_kernel,
        out_shape=[jax.ShapeDtypeStruct(shapes[at], F32) for at in (0, 2, 1)],
        in_specs=[left, left, left],
        out_specs=[left, left, held],
        scratch_shapes=list(spaces_of(*shapes).values()),
        compiler_params=pltpu.CompilerParams(vmem_limit_bytes=63 * 1024 * 1024, collective_id=0, has_side_effects=True),
    )(a_matrix, b_matrix, c_matrix)
    return (a_swept, c_swept, b_next)


def solution(mesh):
    finer = Mesh(mesh.devices.reshape(4, 2, 4, 4), AXES)
    placed = (P(ROW, COL), P(ROW, COL), P(ROW, COL))
    return jax.shard_map(body, mesh=finer, in_specs=placed, out_specs=placed, check_vma=False)
```
